8 devices in a mesh: batch: 1 (over z), z: 2 (over y), y: 2 (over x), x: 2 (over core).
Axes of the slice: x: 2, y: 2, z: 1, core: 2. Of those that a mesh axis runs over, the one named last changes fastest.
Arguments:
- source: float32 [192, 192, 192], P(('batch', 'z'), 'y', 'x')
- initial_guess: float32 [192, 192, 192], P(('batch', 'z'), 'y', 'x')
Outputs:
- output: float32 [192, 192, 192], P(('batch', 'z'), 'y', 'x')
All inputs are finite; a program needn't handle non-finite values.
Results may differ from the reference program's by a relative error of at most 0.001.
Values sent between devices are 32-bit elements.
A program may use at most 1 GiB of HBM per device.

```python
import math
import jax
import jax.numpy as jnp
from jax import lax

N = 192
CYCLES = 2
PRE = 2
POST = 2
COARSE_SWEEPS = 24


def level_count(fine_edge):
    count = 0
    edge_now = fine_edge
    for step_index in range(16):
        if edge_now % 2 == 0 and edge_now // 2 >= 4:
            edge_now = edge_now // 2
            count = count + 1
    return count


LEVELS = level_count(N)


def sine_table(modes, edge):
    centres = (jnp.arange(edge, dtype=jnp.float32) + 0.5) / edge
    waves = jnp.arange(1, modes + 1, dtype=jnp.float32)
    return jnp.sin(math.pi * waves[:, None] * centres[None, :])


def mode_field(coeffs, table):
    stage = jnp.einsum('abc,ck->abk', coeffs, table)
    stage = jnp.einsum('abk,bj->ajk', stage, table)
    return jnp.einsum('ajk,ai->ijk', stage, table)


def setup_inputs(seed: int = 0, part: int = 0) -> dict:
    base_key = jax.random.fold_in(jax.random.key(seed), part)
    key_sol, key_noise, key_init, key_rough = jax.random.split(base_key, 4)
    waves = jnp.arange(1, 9, dtype=jnp.float32)
    wave_sq = waves[:, None, None] ** 2 + waves[None, :, None] ** 2 + waves[None, None, :] ** 2
    pi_sq = math.pi * math.pi
    sol_coeffs = 2.0 * jax.random.normal(key_sol, (8, 8, 8), jnp.float32) / jnp.sqrt(wave_sq)
    table = sine_table(8, N)
    smooth_source = mode_field(pi_sq * sol_coeffs * wave_sq, table)
    rough_source = 2.0 * N * N * jax.random.normal(key_noise, (N, N, N), jnp.float32)
    init_coeffs = 3.5 * jax.random.normal(key_init, (4, 4, 4), jnp.float32)
    smooth_guess = mode_field(init_coeffs, table[:4])
    rough_guess = jax.random.normal(key_rough, (N, N, N), jnp.float32)
    return {'source': smooth_source + rough_source, 'initial_guess': smooth_guess + rough_guess}


def shifted(grid, axis):
    extent = grid.shape[axis]
    first = lax.slice_in_dim(grid, 0, 1, axis=axis)
    last = lax.slice_in_dim(grid, extent - 1, extent, axis=axis)
    below = jnp.concatenate([-first, lax.slice_in_dim(grid, 0, extent - 1, axis=axis)], axis=axis)
    above = jnp.concatenate([lax.slice_in_dim(grid, 1, extent, axis=axis), -last], axis=axis)
    return below, above


def neighbour_sum(grid):
    total = jnp.zeros_like(grid)
    for axis in range(3):
        below, above = shifted(grid, axis)
        total = total + below + above
    return total


def red_mask(edge):
    coords = jnp.arange(edge)
    return (coords[:, None, None] + coords[None, :, None] + coords[None, None, :]) % 2 == 0


def gs_sweep(iterate, source, step_sq, red_cells):
    scaled = step_sq * source
    updated = (scaled + neighbour_sum(iterate)) / 6.0
    iterate = jnp.where(red_cells, updated, iterate)
    updated = (scaled + neighbour_sum(iterate)) / 6.0
    return jnp.where(red_cells, iterate, updated)


def residual(iterate, source, step_sq):
    return source - (6.0 * iterate - neighbour_sum(iterate)) / step_sq


def restrict(grid):
    grid_shape = grid.shape
    folded = grid.reshape(grid_shape[0] // 2, 2, grid_shape[1] // 2, 2, grid_shape[2] // 2, 2)
    return folded.mean(axis=(1, 3, 5))


def prolong(coarse):
    fine = coarse
    for axis in range(3):
        below, above = shifted(fine, axis)
        even_cells = 0.75 * fine + 0.25 * below
        odd_cells = 0.75 * fine + 0.25 * above
        new_shape = list(fine.shape)
        new_shape[axis] = 2 * new_shape[axis]
        fine = jnp.stack([even_cells, odd_cells], axis=axis + 1).reshape(new_shape)
    return fine


def vcycle(iterate, source, level):
    step_sq = (1.0 / (N >> level)) ** 2
    red_cells = red_mask(N >> level)
    if level == LEVELS:
        return lax.fori_loop(0, COARSE_SWEEPS, lambda sweep_index, current: gs_sweep(current, source, step_sq, red_cells), iterate)
    for sweep_index in range(PRE):
        iterate = gs_sweep(iterate, source, step_sq, red_cells)
    coarse_source = restrict(residual(iterate, source, step_sq))
    correction = vcycle(jnp.zeros_like(coarse_source), coarse_source, level + 1)
    iterate = iterate + prolong(correction)
    for sweep_index in range(POST):
        iterate = gs_sweep(iterate, source, step_sq, red_cells)
    return iterate


def reference(source, initial_guess):
    iterate = initial_guess
    for cycle_index in range(CYCLES):
        iterate = vcycle(iterate, source, 0)
    return iterate
```

```python
import jax
import jax.numpy as jnp
from jax import lax
from jax.experimental import pallas as pl
from jax.experimental.pallas import tpu as pltpu
from jax.sharding import PartitionSpec as P

N = 192
CYCLES = 2
COARSE_SWEEPS = 24
F32 = jnp.float32
MESH = pl.DeviceIdType.MESH

PAIRS = (48, 24, 24, 12, 6, 3)
ROWS = (96, 48, 48, 24, 12, 6)
LANES = (96, 48, 48, 24, 12, 6)
ZO = (9, 7, 1, 1, 1, 1)
NZ = (66, 38, 26, 14, 8, 5)
YO = (24, 24, 8, 8, 8, 8)
NY = (144, 96, 64, 40, 32, 24)
ZHALO = (8, 6, 0, 0, 0, 0)
YHALO = (16, 16, 0, 0, 0, 0)
WINDOW = (112, 64, 48, 24, 16, 8)
UNROLL = (8, 10, 12, 12, 6, 3)
CHUNK = 16
SLOTS = 4
WIDTH = 128
TILE = 8
BRICK = 96
BOX = 24


def iotas(shape=(TILE, WIDTH)):
    return lax.broadcasted_iota(jnp.int32, shape, 0), lax.broadcasted_iota(jnp.int32, shape, 1)


class Level:
    def __init__(self, level, zi, yi, xi, m):
        self.level = level
        self.split = level < 2
        self.pairs, self.rows, self.lanes = PAIRS[level], ROWS[level], LANES[level]
        self.zo, self.yo = ZO[level], YO[level]
        self.planes = self.pairs + ZHALO[level]
        self.height = WINDOW[level]
        self.own_height = TILE * (-(-self.rows // TILE))
        if self.split:
            self.zs = self.zo - ZHALO[level] * zi
            self.ys = pl.multiple_of(self.yo - YHALO[level] * yi, TILE)
            self.own_at = pl.multiple_of(YHALO[level] * yi, TILE)
        else:
            self.zs, self.ys, self.own_at = self.zo, self.yo, 0
        self.zi = zi
        self.m = m
        self.row = pl.ds(self.ys, self.height)
        lane = lax.broadcasted_iota(jnp.int32, (TILE, WIDTH), 1)
        if self.split:
            self.valid = jnp.logical_or(lane < self.lanes + 16 * (1 - xi), lane >= WIDTH - 16 * xi)
            edges = (lane == (self.lanes - 1) * xi,)
        else:
            self.valid = lane < self.lanes
            edges = (lane == 0, lane == self.lanes - 1)
        self.outer = edges[0] if self.split else jnp.logical_or(*edges)
        self.w = jnp.where(self.valid, 1.0 / 6.0, 0.0).astype(F32)[None]
        sub, lane = iotas((self.height, WIDTH))
        if self.split:
            count = jnp.where(lane == (self.lanes - 1) * xi, 1.0, 0.0) + jnp.where(sub == (self.height - 1) * yi, 1.0, 0.0)
        else:
            count = (jnp.where(lane == 0, 1.0, 0.0) + jnp.where(lane == self.lanes - 1, 1.0, 0.0)
                     + jnp.where(sub == 0, 1.0, 0.0) + jnp.where(sub == self.rows - 1, 1.0, 0.0))
        m[...] = count.astype(F32)

    def odd(self, height, flip):
        sub, lane = iotas()
        return jnp.broadcast_to((lax.rem(sub + lane, 2) == (0 if flip else 1))[None], (height // TILE, TILE, WIDTH))

    def scaled(self, s):
        if self.rows % TILE and not self.split:
            sub, lane = iotas((self.height, WIDTH))
            inside = jnp.logical_and(sub < self.rows, lane < self.lanes)
            return s * jnp.where(inside, 1.0 / 6.0, 0.0).astype(F32)
        return flat(tiled(s) * self.w)


def tiled(v):
    return v.reshape(v.shape[0] // TILE, TILE, WIDTH)


def flat(v):
    return v.reshape(v.shape[0] * TILE, WIDTH)


def choose(mask, a, b):
    return flat(jnp.where(mask, tiled(a), tiled(b)))


def loop(count, body):
    def step(i, carry):
        body(i)
        return carry
    lax.fori_loop(0, count, step, 0)


def unrolled(count, body):
    def step(i, carry):
        body(i)
        return carry
    if count == 1:
        body(0)
    elif count > 1:
        lax.fori_loop(0, count, step, 0, unroll=True)


def grouped(count, group, body):
    if count == group:
        unrolled(group, body)
    else:
        loop(count // group, lambda i: unrolled(group, lambda k: body(i * group + k)))


def ghost_planes(dst, src, lv):
    pairs = [(lv.zo - 1, lv.zo), (lv.zo + lv.pairs, lv.zo + lv.pairs - 1)]
    if lv.split:
        pairs = [tuple(a + (b - a) * lv.zi for a, b in zip(*pairs))]
    for to, frm in pairs:
        dst[to, lv.row, :] = -src[frm, lv.row, :]


def gather_sum(a, b, hb, z, y, height, mask, m):
    row = pl.ds(y, height)
    bc = b[z, row, :]
    s = bc + choose(mask, b[z + 1, row, :], b[z - 1, row, :])
    s = s + (b[z, pl.ds(y - 1, height), :] + b[z, pl.ds(y + 1, height), :])
    s = s + (pltpu.roll(bc, 1, 1) + pltpu.roll(bc, 127, 1))
    av = a[z, row, :]
    return s + (hb[z, row, :] - m * av), av


def half_sweep(a, b, hb, lv, colour):
    ghost_planes(b, a, lv)
    mask = lv.odd(lv.height, colour)

    def plane(k):
        z = lv.zs + k
        s, _ = gather_sum(a, b, hb, z, lv.ys, lv.height, mask, lv.m[...])
        a[z, lv.row, :] = lv.scaled(s)
    grouped(lv.planes, UNROLL[lv.level], plane)


def sweep(u, hb, lv):
    half_sweep(u[0], u[1], hb[0], lv, 0)
    half_sweep(u[1], u[0], hb[1], lv, 1)


def zero_start(u, hb, lv):
    def clear(i):
        u[1][i] = jnp.zeros(u[1].shape[1:], F32)
    loop(u[1].shape[0], clear)

    def plane(k):
        u[0][lv.zs + k, lv.row, :] = lv.scaled(hb[0][lv.zs + k, lv.row, :])
    grouped(lv.planes, UNROLL[lv.level], plane)


def restrict(u, hb, lv, sums, coarse, coarse_at):
    height = lv.own_height
    group = TILE if lv.pairs % TILE == 0 else 6
    for c in range(2):
        ghost_planes(u[1 - c], u[c], lv)
        mask = lv.odd(height, c)

        def plane(k, c=c, mask=mask):
            s, v = gather_sum(u[c], u[1 - c], hb[c], lv.zo + k, lv.yo, height, mask, lv.m[pl.ds(lv.own_at, height), :])
            q = s - 6.0 * v
            sums[k, 0:height, :] = q if c == 0 else sums[k, 0:height, :] + q
        grouped(lv.pairs, group, plane)

    half = lv.lanes // 2
    rows = TILE * (-(-(lv.rows // 2) // TILE))
    sub, lane = iotas((rows, WIDTH))
    even_idx = jnp.minimum(2 * lane, 126)
    odd_idx = even_idx + 1
    scale = jnp.where(iotas()[1] < half, 0.5, 0.0).astype(F32)[None]
    mask = lv.odd(rows, 0)
    zc, yc = coarse_at

    def fold(pair):
        c = []
        for s in range(2):
            z = 2 * pair + s
            v = sums[z, pl.ds(0, rows, stride=2), :] + sums[z, pl.ds(1, rows, stride=2), :]
            v = jnp.take_along_axis(v, even_idx, axis=1) + jnp.take_along_axis(v, odd_idx, axis=1)
            c.append(flat(tiled(v) * scale))
        coarse[0][zc + pair, pl.ds(yc, rows), :] = choose(mask, c[1], c[0])
        coarse[1][zc + pair, pl.ds(yc, rows), :] = choose(mask, c[0], c[1])
    grouped(lv.pairs // 2, min(6, lv.pairs // 2), fold)


def prolong(u, e, lv, lc, yi, xi, cx, d):
    planes = lv.planes
    crows = (lv.rows + YHALO[lv.level]) // 2
    height = TILE * (-(-crows // TILE))
    if lv.level == 0:
        zc, yc, off = lc.zo - (ZHALO[0] // 2) * lv.zi, lc.yo - (YHALO[0] // 2) * yi, 0
    elif lv.level == 1:
        zc = lc.zo + (PAIRS[2] - planes // 2) * lv.zi
        yc = lc.yo + (ROWS[2] - crows) * yi
        off = (LANES[1] // 2) * xi
    else:
        zc, yc, off = lc.zo, lc.yo, 0
    if lv.split:
        yc = pl.multiple_of(yc, TILE)
    sub, lane = iotas((height, WIDTH))
    fine_lane = jnp.where(lane < 112, lane, lane - WIDTH) if lv.split else lane
    near = lax.div(fine_lane + WIDTH, 2) - 64
    far = near + jnp.where(lax.rem(lane, 2) == 1, 1, -1)
    if lv.split:
        far = jnp.where(lane == (lv.lanes - 1) * xi, near, far)
    else:
        far = jnp.where(jnp.logical_or(lane == 0, lane == lv.lanes - 1), near, far)
    idx_near = lax.rem(near + off + WIDTH, WIDTH)
    idx_far = lax.rem(far + off + WIDTH, WIDTH)
    w_near = jnp.where(lv.valid, 0.75, 0.0).astype(F32)[None]
    w_far = jnp.where(lv.valid, jnp.where(lv.outer, -0.25, 0.25), 0.0).astype(F32)[None]
    mask = lv.odd(height, 0)

    def along_x(pair):
        r, b = e[0][zc + pair, pl.ds(yc, height), :], e[1][zc + pair, pl.ds(yc, height), :]
        for s in range(2):
            c = choose(mask, b, r) if s == 0 else choose(mask, r, b)
            c = (tiled(jnp.take_along_axis(c, idx_near, axis=1)) * w_near
                 + tiled(jnp.take_along_axis(c, idx_far, axis=1)) * w_far)
            cx[2 * pair + s, TILE:TILE + height, :] = flat(c)
    pairs = planes // 2
    grouped(pairs, 7 if pairs % 7 == 0 else (5 if pairs % 5 == 0 else min(6, pairs)), along_x)

    if lv.split:
        sides = ((7 + (crows + 1) * yi, TILE + (crows - 1) * yi),)
    else:
        sides = ((7, TILE), (TILE + crows, 7 + crows))

    def edge_rows(z):
        for to, frm in sides:
            cx[z, pl.ds(to, 1), :] = -cx[z, pl.ds(frm, 1), :]
    grouped(planes, 2, edge_rows)

    def along_y(z):
        mid = 0.75 * cx[z, TILE:TILE + height, :]
        d[lv.zs + z, pl.ds(lv.ys, height, stride=2), :] = mid + 0.25 * cx[z, 7:7 + height, :]
        d[lv.zs + z, pl.ds(lv.ys + 1, height, stride=2), :] = mid + 0.25 * cx[z, 9:9 + height, :]
    grouped(planes, 2, along_y)
    ghost_planes(d, d, lv)
    mask = lv.odd(lv.height, 0)

    def along_z(k):
        z = lv.zs + k
        mid = 0.75 * d[z, lv.row, :]
        up, down = 0.25 * d[z + 1, lv.row, :], 0.25 * d[z - 1, lv.row, :]
        r = u[0][z, lv.row, :] + (mid + choose(mask, up, down))
        b = u[1][z, lv.row, :] + (mid + choose(mask, down, up))
        if not lv.split and lv.rows % TILE:
            keep = iotas((lv.height, WIDTH))[0] < lv.rows
            r, b = jnp.where(keep, r, 0.0), jnp.where(keep, b, 0.0)
        u[0][z, lv.row, :] = r
        u[1][z, lv.row, :] = b
    grouped(planes, 2, along_z)


def kernel(f_hbm, u_hbm, out_hbm, *scratch):
    (u0r, u0b, f0r, f0b, u1r, u1b, h1r, h1b, u2r, u2b, h2r, h2b, u3r, u3b, h3r, h3b, u4r, u4b, h4r, h4b,
     u5r, u5b, h5r, h5b, d0, d1, d2, d3, d4, cx0, cx1, cx2, cx3, cx4, t0, t1, t2, t3, t4,
     m0, m1, m2, m3, m4, m5, raw, xs, xr0, xr1, xs1, xr2, c2r, c2b, box, gbox,
     in_sem, out_sem, x_send, x_recv, send, recv, g_send, g_recv) = scratch
    zi, yi, xi = lax.axis_index('z'), lax.axis_index('y'), lax.axis_index('x')
    peers = ({'x': 1 - xi}, {'y': 1 - yi}, {'z': 1 - zi}, {'z': 1 - zi, 'y': 1 - yi})

    chunks = [(src, c) for src in (u_hbm, f_hbm) for c in range(BRICK // CHUNK)]

    def load(n):
        src, c = chunks[n]
        return pltpu.make_async_copy(src.at[pl.ds(c * CHUNK, CHUNK)], raw.at[n % SLOTS], in_sem.at[n % SLOTS])
    for n in range(SLOTS):
        load(n).start()

    for ref in (u0r, u0b, f0r, f0b, d0):
        def clear(i, ref=ref):
            ref[i] = jnp.zeros((NY[0], WIDTH), F32)
        loop(NZ[0], clear)
    for ref in (h1r.at[0], h1b.at[0], h1r.at[1], h1b.at[1], u1r, u1b, d1):
        def clear(i, ref=ref):
            ref[i] = jnp.zeros((NY[1], WIDTH), F32)
        loop(NZ[1], clear)
    for ref in (u2r, u2b, h2r, h2b, u3r, u3b, h3r, h3b, u4r, u4b, h4r, h4b, u5r, u5b, h5r, h5b, d2, d3, d4,
                cx0, cx1, cx2, cx3, cx4, t0, t1, t2, t3, t4, box):
        def clear(i, ref=ref):
            ref[i] = jnp.zeros(ref.shape[1:], F32)
        loop(ref.shape[0], clear)

    barrier = pltpu.get_barrier_semaphore()
    for peer in peers:
        pl.semaphore_signal(barrier, inc=1, device_id=peer, device_id_type=MESH)

    sub, lane = iotas((BRICK, BRICK))
    odd96 = lax.rem(sub + lane, 2) == 1
    h_sq = (1.0 / N) ** 2
    for n in range(len(chunks)):
        load(n).wait()
        slot = n % SLOTS
        first = n < len(chunks) // 2
        red, black = (u0r, u0b) if first else (f0r, f0b)
        start = ZO[0] + (n % (BRICK // CHUNK)) * (CHUNK // 2)

        def pack(i):
            p0, p1 = raw[slot, 2 * i], raw[slot, 2 * i + 1]
            r, b = jnp.where(odd96, p1, p0), jnp.where(odd96, p0, p1)
            if not first:
                r, b = r * h_sq, b * h_sq
            red[start + i, YO[0]:YO[0] + BRICK, 0:BRICK] = r
            black[start + i, YO[0]:YO[0] + BRICK, 0:BRICK] = b
        loop(CHUNK // 2, pack)
        if n + SLOTS < len(chunks):
            load(n + SLOTS).start()
    pl.semaphore_wait(barrier, len(peers))

    lvs = [Level(level, zi, yi, xi, m) for level, m in enumerate((m0, m1, m2, m3, m4, m5))]
    us = ((u0r, u0b), (u1r, u1b), (u2r, u2b), (u3r, u3b), (u4r, u4b), (u5r, u5b))
    ds_ = (d0, d1, d2, d3, d4)
    cxs = (cx0, cx1, cx2, cx3, cx4)
    ts = (t0, t1, t2, t3, t4)

    box_lane = lax.broadcasted_iota(jnp.int32, (BOX, WIDTH), 1)
    quarter = lax.div(box_lane, 32)

    def exchange_x(arrays, lv, s_buf, r_buf, sem_at):
        row = pl.ds(lv.yo, lv.rows)
        wide = lax.broadcasted_iota(jnp.int32, (lv.rows, WIDTH), 1)
        group = lax.div(wide, 16)
        from_lane = (lv.lanes - 16) * (1 - xi)
        to_lane = lv.lanes + (112 - lv.lanes) * xi
        copies = []
        for n, a in enumerate(arrays):
            def pack_x(i, a=a, n=n):
                acc = None
                for k in range(TILE):
                    v = pltpu.roll(a[lv.zo + TILE * i + k, row, :], lax.rem(16 * k + WIDTH - from_lane, WIDTH), 1)
                    acc = v if k == 0 else jnp.where(group == k, v, acc)
                s_buf[n, i] = acc
            loop(lv.pairs // TILE, pack_x)
            copy = pltpu.make_async_remote_copy(
                src_ref=s_buf.at[n], dst_ref=r_buf.at[n], send_sem=x_send.at[sem_at + n], recv_sem=x_recv.at[sem_at + n],
                device_id=peers[0], device_id_type=MESH)
            copy.start()
            copies.append(copy)
        inside = jnp.logical_and(wide >= to_lane, wide < to_lane + 16)
        for n, a in enumerate(arrays):
            copies[n].wait()

            def unpack_x(i, a=a, n=n):
                acc = r_buf[n, i]
                for k in range(TILE):
                    z = lv.zo + TILE * i + k
                    v = pltpu.roll(acc, lax.rem(to_lane + WIDTH - 16 * k, WIDTH), 1)
                    a[z, row, :] = jnp.where(inside, v, a[z, row, :])
            loop(lv.pairs // TILE, unpack_x)

    def send_faces(specs, lv, sem_at):
        copies = []
        for a, zn, yn in specs:
            z_own, y_own = pl.ds(lv.zo, lv.pairs), pl.ds(lv.yo, lv.rows)
            y_in = pl.multiple_of(lv.yo + (lv.rows - yn) * (1 - yi), TILE)
            y_to = pl.multiple_of(lv.yo - yn + (lv.rows + yn) * yi, TILE)
            z_in = lv.zo + (lv.pairs - zn) * (1 - zi)
            z_to = lv.zo - zn + (lv.pairs + zn) * zi
            parts = (
                ((z_own, pl.ds(y_in, yn)), (z_own, pl.ds(y_to, yn)), peers[1]),
                ((pl.ds(z_in, zn), y_own), (pl.ds(z_to, zn), y_own), peers[2]),
                ((pl.ds(z_in, zn), pl.ds(y_in, yn)), (pl.ds(z_to, zn), pl.ds(y_to, yn)), peers[3]),
            )
            for src, dst, peer in parts:
                at = sem_at + len(copies)
                copy = pltpu.make_async_remote_copy(
                    src_ref=a.at[src[0], src[1]], dst_ref=a.at[dst[0], dst[1]], send_sem=send.at[at], recv_sem=recv.at[at],
                    device_id=peer, device_id_type=MESH)
                copy.start()
                copies.append(copy)
        return copies

    def gather_level2(cycle):
        def pack_box(i):
            for c, a in enumerate((c2r, c2b)):
                acc = a[4 * i]
                for k in range(1, 4):
                    acc = jnp.where(quarter == k, pltpu.roll(a[4 * i + k], 32 * k, 1), acc)
                box[cycle, c, i] = acc
        loop(3, pack_box)
        me = 4 * xi + 2 * zi + yi
        copies = []
        for n, peer in enumerate(peers):
            copy = pltpu.make_async_remote_copy(
                src_ref=box.at[cycle], dst_ref=gbox.at[cycle, me], send_sem=g_send.at[cycle, n], recv_sem=g_recv.at[cycle, n],
                device_id=peer, device_id_type=MESH)
            copy.start()
            copies.append(copy)
        for n, (dz, dy) in ((1, (0, 1)), (2, (1, 0)), (3, (1, 1))):
            copies[n].wait_recv()
            sz, sy = zi + dz - 2 * dz * zi, yi + dy - 2 * dy * yi
            at = 4 * xi + 2 * sz + sy
            copy = pltpu.make_async_remote_copy(
                src_ref=gbox.at[cycle, at], dst_ref=gbox.at[cycle, at], send_sem=g_send.at[cycle, 3 + n],
                recv_sem=g_recv.at[cycle, 3 + n], device_id=peers[0], device_id_type=MESH)
            copy.start()
            copies.append(copy)
        copies[0].wait_recv()
        for copy in copies[:4]:
            copy.wait_send()
        for copy in copies[4:]:
            copy.wait()
        for c, a in enumerate((c2r, c2b)):
            gbox[cycle, me, c] = box[cycle, c]

        def unpack_box(i):
            for c, a in enumerate((h2r, h2b)):
                for q in range(4):
                    sz, sy = divmod(q, 2)
                    lo, hi = gbox[cycle, q, c, i], gbox[cycle, 4 + q, c, i]
                    for k in range(4):
                        lower = pltpu.roll(lo, WIDTH - 32 * k, 1) if k else lo
                        upper = pltpu.roll(hi, (152 - 32 * k) % WIDTH, 1)
                        v = jnp.where(box_lane < BOX, lower, jnp.where(box_lane < 48, upper, 0.0))
                        a[ZO[2] + 12 * sz + 4 * i + k, YO[2] + BOX * sy:YO[2] + BOX * sy + BOX, :] = v
        loop(3, unpack_box)

    l0 = lvs[0]
    exchange_x((u0r, u0b, f0r, f0b), l0, xs, xr0, 0)
    for copy in send_faces(((u0r, 2, TILE), (u0b, 3, TILE), (f0r, 4, TILE), (f0b, 4, TILE)), l0, 0):
        copy.wait()

    def v_cycle(cycle):
        h1 = (h1r.at[cycle], h1b.at[cycle])
        hs = ((f0r, f0b), h1, (h2r, h2b), (h3r, h3b), (h4r, h4b), (h5r, h5b))
        l1 = lvs[1]
        loop(2, lambda i: sweep(us[0], hs[0], l0))
        restrict(us[0], hs[0], l0, ts[0], h1, (ZO[1], YO[1]))
        exchange_x(h1, l1, xs1, xr2.at[cycle], TILE)
        for copy in send_faces(((h1[0], 6, 16), (h1[1], 6, 16)), l1, 12):
            copy.wait()
        for level in range(1, 5):
            lv = lvs[level]
            zero_start(us[level], hs[level], lv)
            half_sweep(us[level][1], us[level][0], hs[level][1], lv, 1)
            sweep(us[level], hs[level], lv)
            if level == 1:
                restrict(us[1], h1, l1, ts[1], (c2r, c2b), (0, 0))
                gather_level2(cycle)
                exchange_x(us[0], l0, xs, xr1.at[cycle], 4)
                pending = send_faces(((u0r, 4, TILE), (u0b, 5, 16)), l0, 18)
            else:
                restrict(us[level], hs[level], lv, ts[level], hs[level + 1], (ZO[level + 1], YO[level + 1]))
        lv = lvs[5]
        zero_start(us[5], hs[5], lv)
        half_sweep(us[5][1], us[5][0], hs[5][1], lv, 1)
        loop(COARSE_SWEEPS - 1, lambda i: sweep(us[5], hs[5], lvs[5]))
        for level in range(4, -1, -1):
            lv = lvs[level]
            if level == 0:
                for copy in pending:
                    copy.wait()
            prolong(us[level], us[level + 1], lv, lvs[level + 1], yi, xi, cxs[level], ds_[level])
            loop(2, lambda i, lv=lv, level=level: sweep(us[level], hs[level], lv))
    loop(CYCLES, v_cycle)

    stores = []
    for n in range(BRICK // CHUNK):
        slot = n % SLOTS
        if n >= SLOTS:
            stores[n - SLOTS].wait()

        def unpack(i):
            z = ZO[0] + n * (CHUNK // 2) + i
            r, b = u0r[z, YO[0]:YO[0] + BRICK, 0:BRICK], u0b[z, YO[0]:YO[0] + BRICK, 0:BRICK]
            raw[slot, 2 * i] = jnp.where(odd96, b, r)
            raw[slot, 2 * i + 1] = jnp.where(odd96, r, b)
        loop(CHUNK // 2, unpack)
        copy = pltpu.make_async_copy(raw.at[slot], out_hbm.at[pl.ds(n * CHUNK, CHUNK)], out_sem.at[slot])
        copy.start()
        stores.append(copy)
    for copy in stores[-SLOTS:]:
        copy.wait()


def vmem(*shape):
    return pltpu.VMEM(shape, F32)


def scratch_shapes():
    arr = [vmem(NZ[level], NY[level], WIDTH) for level in range(6)]
    shapes = [arr[0]] * 4 + [arr[1]] * 2 + [vmem(2, NZ[1], NY[1], WIDTH)] * 2
    for level in range(2, 6):
        shapes += [arr[level]] * 4
    shapes += arr[:5]
    shapes += [vmem(56, 80, WIDTH), vmem(30, 48, WIDTH), vmem(BOX, 40, WIDTH), vmem(12, 32, WIDTH), vmem(6, BOX, WIDTH)]
    shapes += [vmem(48, BRICK, WIDTH), vmem(BOX, 48, WIDTH), vmem(BOX, 48, WIDTH), vmem(12, 32, WIDTH), vmem(6, 16, WIDTH)]
    shapes += [vmem(height, WIDTH) for height in WINDOW]
    shapes += [vmem(SLOTS, CHUNK, BRICK, BRICK)]
    shapes += [vmem(4, 6, BRICK, WIDTH), vmem(4, 6, BRICK, WIDTH), vmem(2, 2, 6, BRICK, WIDTH)]
    shapes += [vmem(2, 3, 48, WIDTH), vmem(2, 2, 3, 48, WIDTH)]
    shapes += [vmem(12, BOX, WIDTH), vmem(12, BOX, WIDTH), vmem(2, 2, 3, BOX, WIDTH), vmem(2, TILE, 2, 3, BOX, WIDTH)]
    dma = pltpu.SemaphoreType.DMA
    shapes += [dma((SLOTS,)), dma((SLOTS,)), dma((10,)), dma((10,)), dma((BOX,)), dma((BOX,)), dma((2, 7)), dma((2, 7))]
    return shapes


def solution(mesh):
    spec = P(('batch', 'z'), 'y', 'x')

    def local_solve(source, initial_guess):
        return pl.pallas_call(
            kernel,
            out_shape=jax.ShapeDtypeStruct(source.shape, F32),
            in_specs=[pl.BlockSpec(memory_space=pl.ANY)] * 2,
            out_specs=pl.BlockSpec(memory_space=pl.ANY),
            scratch_shapes=scratch_shapes(),
            compiler_params=pltpu.CompilerParams(collective_id=0, has_side_effects=True, vmem_limit_bytes=67043328),
            name='multigrid',
        )(source, initial_guess)

    return jax.shard_map(local_solve, mesh=mesh, in_specs=(spec, spec), out_specs=spec, check_vma=False)
```

```python
import jax
import jax.numpy as jnp
from jax import lax
from jax.experimental import pallas as pl
from jax.experimental.pallas import tpu as pltpu
from jax.sharding import PartitionSpec as P

N = 192
CYCLES = 2
COARSE_SWEEPS = 24
F32 = jnp.float32
MESH = pl.DeviceIdType.MESH

PAIRS = (48, 24, 24, 12, 6, 3)
ROWS = (96, 48, 48, 24, 12, 6)
LANES = (96, 48, 48, 24, 12, 6)
ZO = (9, 7, 1, 1, 1, 1)
NZ = (66, 38, 26, 14, 8, 5)
YO = (24, 24, 8, 8, 8, 8)
NY = (144, 96, 64, 40, 32, 24)
ZHALO = (8, 6, 0, 0, 0, 0)
YHALO = (16, 16, 0, 0, 0, 0)
WINDOW = (112, 64, 48, 24, 16, 8)
UNROLL = (8, 10, 12, 12, 6, 3)
CHUNK = 16
SLOTS = 4
WIDTH = 128
TILE = 8
BRICK = 96
BOX = 24
XHALO = 16


def iotas(shape=(TILE, WIDTH)):
    return lax.broadcasted_iota(jnp.int32, shape, 0), lax.broadcasted_iota(jnp.int32, shape, 1)


class Level:
    def __init__(self, level, zi, yi, xi, m):
        self.level = level
        self.split = level < 2
        self.pairs, self.rows, self.lanes = PAIRS[level], ROWS[level], LANES[level]
        self.zo, self.yo = ZO[level], YO[level]
        self.planes = self.pairs + ZHALO[level]
        self.height = WINDOW[level]
        self.own_height = TILE * (-(-self.rows // TILE))
        if self.split:
            self.zs = self.zo - ZHALO[level] * zi
            self.ys = pl.multiple_of(self.yo - YHALO[level] * yi, TILE)
            self.own_at = pl.multiple_of(YHALO[level] * yi, TILE)
        else:
            self.zs, self.ys, self.own_at = self.zo, self.yo, 0
        self.zi = zi
        self.m = m
        self.row = pl.ds(self.ys, self.height)
        lane = lax.broadcasted_iota(jnp.int32, (TILE, WIDTH), 1)
        if self.split:
            self.valid = jnp.logical_or(lane < self.lanes + XHALO * (1 - xi), lane >= WIDTH - XHALO * xi)
            edges = (lane == (self.lanes - 1) * xi,)
        else:
            self.valid = lane < self.lanes
            edges = (lane == 0, lane == self.lanes - 1)
        self.outer = edges[0] if self.split else jnp.logical_or(*edges)
        self.w = jnp.where(self.valid, 1.0 / 6.0, 0.0).astype(F32)[None]
        sub, lane = iotas((self.height, WIDTH))
        if self.split:
            count = ones(lane == (self.lanes - 1) * xi) + ones(sub == (self.height - 1) * yi)
        else:
            count = (ones(lane == 0) + ones(lane == self.lanes - 1)
                     + ones(sub == 0) + ones(sub == self.rows - 1))
        m[...] = count.astype(F32)

    def odd(self, height, flip):
        sub, lane = iotas()
        return jnp.broadcast_to((lax.rem(sub + lane, 2) == (0 if flip else 1))[None], (height // TILE, TILE, WIDTH))

    def scaled(self, s):
        if self.rows % TILE and not self.split:
            sub, lane = iotas((self.height, WIDTH))
            inside = jnp.logical_and(sub < self.rows, lane < self.lanes)
            return s * jnp.where(inside, 1.0 / 6.0, 0.0).astype(F32)
        return flat(tiled(s) * self.w)


def turn(v, by):
    return pltpu.roll(v, by, 1)


def pick(v, idx):
    return jnp.take_along_axis(v, idx, axis=1)


def ones(where):
    return jnp.where(where, 1.0, 0.0)


def tiled(v):
    return v.reshape(v.shape[0] // TILE, TILE, WIDTH)


def flat(v):
    return v.reshape(v.shape[0] * TILE, WIDTH)


def choose(mask, a, b):
    return flat(jnp.where(mask, tiled(a), tiled(b)))


def loop(count, body):
    def step(i, carry):
        body(i)
        return carry
    lax.fori_loop(0, count, step, 0)


def unrolled(count, body):
    def step(i, carry):
        body(i)
        return carry
    if count == 1:
        body(0)
    elif count > 1:
        lax.fori_loop(0, count, step, 0, unroll=True)


def grouped(count, group, body):
    if count == group:
        unrolled(group, body)
    else:
        loop(count // group, lambda i: unrolled(group, lambda k: body(i * group + k)))


def ghost_planes(dst, src, lv):
    pairs = [(lv.zo - 1, lv.zo), (lv.zo + lv.pairs, lv.zo + lv.pairs - 1)]
    if lv.split:
        pairs = [tuple(a + (b - a) * lv.zi for a, b in zip(*pairs))]
    for to, frm in pairs:
        dst[to, lv.row, :] = -src[frm, lv.row, :]


def gather_sum(a, b, hb, z, y, height, mask, m):
    row = pl.ds(y, height)
    bc = b[z, row, :]
    s = bc + choose(mask, b[z + 1, row, :], b[z - 1, row, :])
    s = s + (b[z, pl.ds(y - 1, height), :] + b[z, pl.ds(y + 1, height), :])
    s = s + (turn(bc, 1) + turn(bc, WIDTH - 1))
    av = a[z, row, :]
    return s + (hb[z, row, :] - m * av), av


def half_sweep(a, b, hb, lv, colour):
    ghost_planes(b, a, lv)
    mask = lv.odd(lv.height, colour)

    def plane(k):
        z = lv.zs + k
        s, _ = gather_sum(a, b, hb, z, lv.ys, lv.height, mask, lv.m[...])
        a[z, lv.row, :] = lv.scaled(s)
    grouped(lv.planes, UNROLL[lv.level], plane)


def sweep(u, hb, lv):
    half_sweep(u[0], u[1], hb[0], lv, 0)
    half_sweep(u[1], u[0], hb[1], lv, 1)


def zero_start(u, hb, lv):
    def clear(i):
        u[1][i] = jnp.zeros(u[1].shape[1:], F32)
    loop(u[1].shape[0], clear)

    def plane(k):
        u[0][lv.zs + k, lv.row, :] = lv.scaled(hb[0][lv.zs + k, lv.row, :])
    grouped(lv.planes, UNROLL[lv.level], plane)


def restrict(u, hb, lv, sums, coarse, coarse_at):
    height = lv.own_height
    group = TILE if lv.pairs % TILE == 0 else 6
    for c in range(2):
        ghost_planes(u[1 - c], u[c], lv)
        mask = lv.odd(height, c)

        def plane(k, c=c, mask=mask):
            s, v = gather_sum(u[c], u[1 - c], hb[c], lv.zo + k, lv.yo, height, mask, lv.m[pl.ds(lv.own_at, height), :])
            q = s - 6.0 * v
            sums[k, 0:height, :] = q if c == 0 else sums[k, 0:height, :] + q
        grouped(lv.pairs, group, plane)

    half = lv.lanes // 2
    rows = TILE * (-(-(lv.rows // 2) // TILE))
    sub, lane = iotas((rows, WIDTH))
    even_idx = jnp.minimum(2 * lane, 126)
    odd_idx = even_idx + 1
    scale = jnp.where(iotas()[1] < half, 0.5, 0.0).astype(F32)[None]
    mask = lv.odd(rows, 0)
    zc, yc = coarse_at

    def fold(pair):
        c = []
        for s in range(2):
            z = 2 * pair + s
            v = sums[z, pl.ds(0, rows, stride=2), :] + sums[z, pl.ds(1, rows, stride=2), :]
            v = pick(v, even_idx) + pick(v, odd_idx)
            c.append(flat(tiled(v) * scale))
        coarse[0][zc + pair, pl.ds(yc, rows), :] = choose(mask, c[1], c[0])
        coarse[1][zc + pair, pl.ds(yc, rows), :] = choose(mask, c[0], c[1])
    grouped(lv.pairs // 2, min(6, lv.pairs // 2), fold)


def prolong(u, e, lv, lc, yi, xi, cx, d):
    planes = lv.planes
    crows = (lv.rows + YHALO[lv.level]) // 2
    height = TILE * (-(-crows // TILE))
    if lv.level == 0:
        zc, yc, off = lc.zo - (ZHALO[0] // 2) * lv.zi, lc.yo - (YHALO[0] // 2) * yi, 0
    elif lv.level == 1:
        zc = lc.zo + (PAIRS[2] - planes // 2) * lv.zi
        yc = lc.yo + (ROWS[2] - crows) * yi
        off = (LANES[1] // 2) * xi
    else:
        zc, yc, off = lc.zo, lc.yo, 0
    if lv.split:
        yc = pl.multiple_of(yc, TILE)
    sub, lane = iotas((height, WIDTH))
    fine_lane = jnp.where(lane < 112, lane, lane - WIDTH) if lv.split else lane
    near = lax.div(fine_lane + WIDTH, 2) - 64
    far = near + jnp.where(lax.rem(lane, 2) == 1, 1, -1)
    if lv.split:
        far = jnp.where(lane == (lv.lanes - 1) * xi, near, far)
    else:
        far = jnp.where(jnp.logical_or(lane == 0, lane == lv.lanes - 1), near, far)
    idx_near = lax.rem(near + off + WIDTH, WIDTH)
    idx_far = lax.rem(far + off + WIDTH, WIDTH)
    w_near = jnp.where(lv.valid, 0.75, 0.0).astype(F32)[None]
    w_far = jnp.where(lv.valid, jnp.where(lv.outer, -0.25, 0.25), 0.0).astype(F32)[None]
    mask = lv.odd(height, 0)

    def along_x(pair):
        r, b = e[0][zc + pair, pl.ds(yc, height), :], e[1][zc + pair, pl.ds(yc, height), :]
        for s in range(2):
            c = choose(mask, b, r) if s == 0 else choose(mask, r, b)
            c = (tiled(pick(c, idx_near)) * w_near
                 + tiled(pick(c, idx_far)) * w_far)
            cx[2 * pair + s, TILE:TILE + height, :] = flat(c)
    pairs = planes // 2
    grouped(pairs, 7 if pairs % 7 == 0 else (5 if pairs % 5 == 0 else min(6, pairs)), along_x)

    if lv.split:
        sides = ((7 + (crows + 1) * yi, TILE + (crows - 1) * yi),)
    else:
        sides = ((7, TILE), (TILE + crows, 7 + crows))

    def edge_rows(z):
        for to, frm in sides:
            cx[z, pl.ds(to, 1), :] = -cx[z, pl.ds(frm, 1), :]
    grouped(planes, 2, edge_rows)

    def along_y(z):
        mid = 0.75 * cx[z, TILE:TILE + height, :]
        d[lv.zs + z, pl.ds(lv.ys, height, stride=2), :] = mid + 0.25 * cx[z, 7:7 + height, :]
        d[lv.zs + z, pl.ds(lv.ys + 1, height, stride=2), :] = mid + 0.25 * cx[z, 9:9 + height, :]
    grouped(planes, 2, along_y)
    ghost_planes(d, d, lv)
    mask = lv.odd(lv.height, 0)

    def along_z(k):
        z = lv.zs + k
        mid = 0.75 * d[z, lv.row, :]
        up, down = 0.25 * d[z + 1, lv.row, :], 0.25 * d[z - 1, lv.row, :]
        r = u[0][z, lv.row, :] + (mid + choose(mask, up, down))
        b = u[1][z, lv.row, :] + (mid + choose(mask, down, up))
        if not lv.split and lv.rows % TILE:
            keep = iotas((lv.height, WIDTH))[0] < lv.rows
            r, b = jnp.where(keep, r, 0.0), jnp.where(keep, b, 0.0)
        u[0][z, lv.row, :] = r
        u[1][z, lv.row, :] = b
    grouped(planes, 2, along_z)


def kernel(f_hbm, u_hbm, out_hbm, *scratch):
    (u0r, u0b, f0r, f0b, u1r, u1b, h1r, h1b, u2r, u2b, h2r, h2b, u3r, u3b, h3r, h3b, u4r, u4b, h4r, h4b,
     u5r, u5b, h5r, h5b, d0, d1, d2, d3, d4, cx0, cx1, cx2, cx3, cx4, t0, t1, t2, t3, t4,
     m0, m1, m2, m3, m4, m5, raw, xs, xr0, xr1, xs1, xr2, c2r, c2b, box, gbox,
     in_sem, out_sem, x_send, x_recv, send, recv, g_send, g_recv) = scratch
    zi, yi, xi = lax.axis_index('z'), lax.axis_index('y'), lax.axis_index('x')
    peers = ({'x': 1 - xi}, {'y': 1 - yi}, {'z': 1 - zi}, {'z': 1 - zi, 'y': 1 - yi})

    chunks = [(src, c) for src in (u_hbm, f_hbm) for c in range(BRICK // CHUNK)]

    def load(n):
        src, c = chunks[n]
        return pltpu.make_async_copy(src.at[pl.ds(c * CHUNK, CHUNK)], raw.at[n % SLOTS], in_sem.at[n % SLOTS])
    for n in range(SLOTS):
        load(n).start()

    for ref in (u0r, u0b, f0r, f0b, d0):
        def clear(i, ref=ref):
            ref[i] = jnp.zeros((NY[0], WIDTH), F32)
        loop(NZ[0], clear)
    for ref in (h1r.at[0], h1b.at[0], h1r.at[1], h1b.at[1], u1r, u1b, d1):
        def clear(i, ref=ref):
            ref[i] = jnp.zeros((NY[1], WIDTH), F32)
        loop(NZ[1], clear)
    for ref in (u2r, u2b, h2r, h2b, u3r, u3b, h3r, h3b, u4r, u4b, h4r, h4b, u5r, u5b, h5r, h5b, d2, d3, d4,
                cx0, cx1, cx2, cx3, cx4, t0, t1, t2, t3, t4, box):
        def clear(i, ref=ref):
            ref[i] = jnp.zeros(ref.shape[1:], F32)
        loop(ref.shape[0], clear)

    barrier = pltpu.get_barrier_semaphore()
    for peer in peers:
        pl.semaphore_signal(barrier, inc=1, device_id=peer, device_id_type=MESH)

    sub, lane = iotas((BRICK, BRICK))
    odd96 = lax.rem(sub + lane, 2) == 1
    h_sq = (1.0 / N) ** 2
    for n in range(len(chunks)):
        load(n).wait()
        slot = n % SLOTS
        first = n < len(chunks) // 2
        red, black = (u0r, u0b) if first else (f0r, f0b)
        start = ZO[0] + (n % (BRICK // CHUNK)) * (CHUNK // 2)

        def pack(i):
            p0, p1 = raw[slot, 2 * i], raw[slot, 2 * i + 1]
            r, b = jnp.where(odd96, p1, p0), jnp.where(odd96, p0, p1)
            if not first:
                r, b = r * h_sq, b * h_sq
            red[start + i, YO[0]:YO[0] + BRICK, 0:BRICK] = r
            black[start + i, YO[0]:YO[0] + BRICK, 0:BRICK] = b
        loop(CHUNK // 2, pack)
        if n + SLOTS < len(chunks):
            load(n + SLOTS).start()
    pl.semaphore_wait(barrier, len(peers))

    lvs = [Level(level, zi, yi, xi, m) for level, m in enumerate((m0, m1, m2, m3, m4, m5))]
    us = ((u0r, u0b), (u1r, u1b), (u2r, u2b), (u3r, u3b), (u4r, u4b), (u5r, u5b))
    ds_ = (d0, d1, d2, d3, d4)
    cxs = (cx0, cx1, cx2, cx3, cx4)
    ts = (t0, t1, t2, t3, t4)

    box_lane = lax.broadcasted_iota(jnp.int32, (BOX, WIDTH), 1)
    quarter = lax.div(box_lane, 32)

    class Columns:
        def __init__(self, arrays, lv, s_buf, r_buf, sem_at):
            self.arrays, self.lv, self.r_buf = arrays, lv, r_buf
            self.wide = lax.broadcasted_iota(jnp.int32, (lv.rows, WIDTH), 1)
            self.row = pl.ds(lv.yo, lv.rows)
            group = lax.div(self.wide, XHALO)
            from_lane = (lv.lanes - XHALO) * (1 - xi)
            self.copies = []
            for n, a in enumerate(arrays):
                def pack_x(i, a=a, n=n):
                    acc = None
                    for k in range(TILE):
                        v = turn(a[lv.zo + TILE * i + k, self.row, :], lax.rem(XHALO * k + WIDTH - from_lane, WIDTH))
                        acc = v if k == 0 else jnp.where(group == k, v, acc)
                    s_buf[n, i] = acc
                loop(lv.pairs // TILE, pack_x)
                at = sem_at + n
                copy = pltpu.make_async_remote_copy(
                    src_ref=s_buf.at[n], dst_ref=r_buf.at[n], send_sem=x_send.at[at], recv_sem=x_recv.at[at],
                    device_id=peers[0], device_id_type=MESH)
                copy.start()
                self.copies.append(copy)

        def finish(self):
            lv, row = self.lv, self.row
            to_lane = lv.lanes + (112 - lv.lanes) * xi
            inside = jnp.logical_and(self.wide >= to_lane, self.wide < to_lane + XHALO)
            for n, a in enumerate(self.arrays):
                self.copies[n].wait()

                def unpack_x(i, a=a, n=n):
                    acc = self.r_buf[n, i]
                    for k in range(TILE):
                        z = lv.zo + TILE * i + k
                        v = turn(acc, lax.rem(to_lane + WIDTH - XHALO * k, WIDTH))
                        a[z, row, :] = jnp.where(inside, v, a[z, row, :])
                loop(lv.pairs // TILE, unpack_x)

    def send_faces(specs, lv, sem_at, start=True):
        copies = []
        for a, zn, yn in specs:
            z_own, y_own = pl.ds(lv.zo, lv.pairs), pl.ds(lv.yo, lv.rows)
            y_in = lv.yo + (lv.rows - yn) * (1 - yi)
            y_to = lv.yo - yn + (lv.rows + yn) * yi
            z_in = lv.zo + (lv.pairs - zn) * (1 - zi)
            z_to = lv.zo - zn + (lv.pairs + zn) * zi
            parts = (
                ((z_own, pl.ds(y_in, yn)), (z_own, pl.ds(y_to, yn)), peers[1]),
                ((pl.ds(z_in, zn), y_own), (pl.ds(z_to, zn), y_own), peers[2]),
                ((pl.ds(z_in, zn), pl.ds(y_in, yn)), (pl.ds(z_to, zn), pl.ds(y_to, yn)), peers[3]),
            )
            for src, dst, peer in parts:
                at = sem_at + len(copies)
                copy = pltpu.make_async_remote_copy(
                    src_ref=a.at[src[0], src[1]], dst_ref=a.at[dst[0], dst[1]], send_sem=send.at[at], recv_sem=recv.at[at],
                    device_id=peer, device_id_type=MESH)
                if start:
                    copy.start()
                copies.append(copy)
        return copies

    def gather_level2(cycle):
        def pack_box(i):
            for c, a in enumerate((c2r, c2b)):
                acc = a[4 * i]
                for k in range(1, 4):
                    acc = jnp.where(quarter == k, turn(a[4 * i + k], 32 * k), acc)
                box[cycle, c, i] = acc
        loop(3, pack_box)
        me = 4 * xi + 2 * zi + yi
        copies = []
        for n, peer in enumerate(peers):
            copy = pltpu.make_async_remote_copy(
                src_ref=box.at[cycle], dst_ref=gbox.at[cycle, me], send_sem=g_send.at[cycle, n], recv_sem=g_recv.at[cycle, n],
                device_id=peer, device_id_type=MESH)
            copy.start()
            copies.append(copy)
        for n, (dz, dy) in ((1, (0, 1)), (2, (1, 0)), (3, (1, 1))):
            copies[n].wait_recv()
            sz, sy = zi + dz - 2 * dz * zi, yi + dy - 2 * dy * yi
            at = 4 * xi + 2 * sz + sy
            copy = pltpu.make_async_remote_copy(
                src_ref=gbox.at[cycle, at], dst_ref=gbox.at[cycle, at], send_sem=g_send.at[cycle, 3 + n],
                recv_sem=g_recv.at[cycle, 3 + n], device_id=peers[0], device_id_type=MESH)
            copy.start()
            copies.append(copy)
        copies[0].wait_recv()
        for copy in copies[:4]:
            copy.wait_send()
        for copy in copies[4:]:
            copy.wait()
        for c, a in enumerate((c2r, c2b)):
            gbox[cycle, me, c] = box[cycle, c]

        def unpack_box(i):
            for c, a in enumerate((h2r, h2b)):
                for q in range(4):
                    sz, sy = divmod(q, 2)
                    lo, hi = gbox[cycle, q, c, i], gbox[cycle, 4 + q, c, i]
                    for k in range(4):
                        lower = turn(lo, WIDTH - 32 * k) if k else lo
                        upper = turn(hi, (152 - 32 * k) % WIDTH)
                        v = jnp.where(box_lane < BOX, lower, jnp.where(box_lane < 48, upper, 0.0))
                        a[ZO[2] + 12 * sz + 4 * i + k, YO[2] + BOX * sy:YO[2] + BOX * sy + BOX, :] = v
        loop(3, unpack_box)

    l0 = lvs[0]
    x_u = Columns((u0r, u0b), l0, xs, xr0, 0)
    x_f = Columns((f0r, f0b), l0, xs.at[2:4], xr0.at[2:4], 2)
    x_u.finish()
    faces = send_faces(((u0r, 2, 4), (u0b, 3, 5)), l0, 0)
    x_f.finish()
    faces += send_faces(((f0r, 2, 4), (f0b, 2, 4)), l0, 6)
    for copy in faces:
        copy.wait()

    def v_cycle(cycle):
        h1 = (h1r.at[cycle], h1b.at[cycle])
        hs = ((f0r, f0b), h1, (h2r, h2b), (h3r, h3b), (h4r, h4b), (h5r, h5b))
        l1 = lvs[1]
        loop(2, lambda i: sweep(us[0], hs[0], l0))
        restrict(us[0], hs[0], l0, ts[0], h1, (ZO[1], YO[1]))
        Columns(h1, l1, xs1, xr2.at[cycle], TILE).finish()
        faces = send_faces(((h1[0], 6, 12), (h1[1], 6, 12)), l1, 12)
        Columns(us[0], l0, xs, xr1.at[cycle], 4).finish()
        for copy in faces:
            copy.wait()
        for level in range(1, 5):
            lv = lvs[level]
            zero_start(us[level], hs[level], lv)
            half_sweep(us[level][1], us[level][0], hs[level][1], lv, 1)
            sweep(us[level], hs[level], lv)
            if level == 1:
                restrict(us[1], h1, l1, ts[1], (c2r, c2b), (0, 0))
                gather_level2(cycle)
                pending = send_faces(((u0r, 4, TILE), (u0b, 5, 9)), l0, 18)

                @pl.when(cycle == 0)
                def deeper_source():
                    send_faces(((f0r, 4, TILE), (f0b, 4, TILE)), l0, 0)
            else:
                restrict(us[level], hs[level], lv, ts[level], hs[level + 1], (ZO[level + 1], YO[level + 1]))
        lv = lvs[5]
        zero_start(us[5], hs[5], lv)
        half_sweep(us[5][1], us[5][0], hs[5][1], lv, 1)
        loop(COARSE_SWEEPS - 1, lambda i: sweep(us[5], hs[5], lvs[5]))
        for level in range(4, -1, -1):
            lv = lvs[level]
            if level == 0:
                for copy in pending:
                    copy.wait()

                @pl.when(cycle == 0)
                def deeper_source_arrived():
                    for copy in send_faces(((f0r, 4, TILE), (f0b, 4, TILE)), l0, 0, False):
                        copy.wait()
            prolong(us[level], us[level + 1], lv, lvs[level + 1], yi, xi, cxs[level], ds_[level])
            loop(2, lambda i, lv=lv, level=level: sweep(us[level], hs[level], lv))
    loop(CYCLES, v_cycle)

    stores = []
    for n in range(BRICK // CHUNK):
        slot = n % SLOTS
        if n >= SLOTS:
            stores[n - SLOTS].wait()

        def unpack(i):
            z = ZO[0] + n * (CHUNK // 2) + i
            r, b = u0r[z, YO[0]:YO[0] + BRICK, 0:BRICK], u0b[z, YO[0]:YO[0] + BRICK, 0:BRICK]
            raw[slot, 2 * i] = jnp.where(odd96, b, r)
            raw[slot, 2 * i + 1] = jnp.where(odd96, r, b)
        loop(CHUNK // 2, unpack)
        copy = pltpu.make_async_copy(raw.at[slot], out_hbm.at[pl.ds(n * CHUNK, CHUNK)], out_sem.at[slot])
        copy.start()
        stores.append(copy)
    for copy in stores[-SLOTS:]:
        copy.wait()


def vmem(*shape):
    return pltpu.VMEM(shape, F32)


def scratch_shapes():
    arr = [vmem(NZ[level], NY[level], WIDTH) for level in range(6)]
    shapes = [arr[0]] * 4 + [arr[1]] * 2 + [vmem(2, NZ[1], NY[1], WIDTH)] * 2
    for level in range(2, 6):
        shapes += [arr[level]] * 4
    shapes += arr[:5]
    shapes += [vmem(56, 80, WIDTH), vmem(30, 48, WIDTH), vmem(BOX, 40, WIDTH), vmem(12, 32, WIDTH), vmem(6, BOX, WIDTH)]
    shapes += [vmem(48, BRICK, WIDTH), vmem(BOX, 48, WIDTH), vmem(BOX, 48, WIDTH), vmem(12, 32, WIDTH), vmem(6, XHALO, WIDTH)]
    shapes += [vmem(height, WIDTH) for height in WINDOW]
    shapes += [vmem(SLOTS, CHUNK, BRICK, BRICK)]
    shapes += [vmem(4, 6, BRICK, WIDTH), vmem(4, 6, BRICK, WIDTH), vmem(2, 2, 6, BRICK, WIDTH)]
    shapes += [vmem(2, 3, 48, WIDTH), vmem(2, 2, 3, 48, WIDTH)]
    shapes += [vmem(12, BOX, WIDTH), vmem(12, BOX, WIDTH), vmem(2, 2, 3, BOX, WIDTH), vmem(2, TILE, 2, 3, BOX, WIDTH)]
    dma = pltpu.SemaphoreType.DMA
    shapes += [dma((SLOTS,)), dma((SLOTS,)), dma((10,)), dma((10,)), dma((BOX,)), dma((BOX,)), dma((2, 7)), dma((2, 7))]
    return shapes


def solution(mesh):
    spec = P(('batch', 'z'), 'y', 'x')

    def local_solve(source, initial_guess):
        return pl.pallas_call(
            kernel,
            out_shape=jax.ShapeDtypeStruct(source.shape, F32),
            in_specs=[pl.BlockSpec(memory_space=pl.ANY)] * 2,
            out_specs=pl.BlockSpec(memory_space=pl.ANY),
            scratch_shapes=scratch_shapes(),
            compiler_params=pltpu.CompilerParams(collective_id=0, has_side_effects=True, vmem_limit_bytes=67043328),
            name='multigrid',
        )(source, initial_guess)

    return jax.shard_map(local_solve, mesh=mesh, in_specs=(spec, spec), out_specs=spec, check_vma=False)
```

```python
import jax
import jax.numpy as jnp
from jax import lax
from jax.experimental import pallas as pl
from jax.experimental.pallas import tpu as pltpu
from jax.sharding import PartitionSpec as P

N = 192
CYCLES = 2
COARSE_SWEEPS = 24
F32 = jnp.float32
MESH = pl.DeviceIdType.MESH

PAIRS = (48, 24, 24, 12, 6, 3)
ROWS = (96, 48, 48, 24, 12, 6)
LANES = (96, 48, 48, 24, 12, 6)
ZO = (9, 7, 1, 1, 1, 1)
NZ = (66, 38, 26, 14, 8, 5)
YO = (24, 24, 8, 8, 8, 8)
NY = (144, 96, 64, 40, 32, 24)
ZHALO = (8, 6, 0, 0, 0, 0)
YHALO = (16, 16, 0, 0, 0, 0)
WINDOW = (112, 64, 48, 24, 16, 8)
UNROLL = (8, 10, 12, 12, 6, 3)
CHUNK = 16
SLOTS = 4
WIDTH = 128
TILE = 8
BRICK = 96
BOX = 24
XHALO = 16
DEEP = 12


def iotas(shape=(TILE, WIDTH)):
    return lax.broadcasted_iota(jnp.int32, shape, 0), lax.broadcasted_iota(jnp.int32, shape, 1)


class Level:
    def __init__(self, level, zi, yi, xi, m):
        self.level = level
        self.split = level < 2
        self.pairs, self.rows, self.lanes = PAIRS[level], ROWS[level], LANES[level]
        self.zo, self.yo = ZO[level], YO[level]
        self.planes = self.pairs + ZHALO[level]
        self.height = WINDOW[level]
        self.own_height = TILE * (-(-self.rows // TILE))
        if self.split:
            self.zs = self.zo - ZHALO[level] * zi
            self.ys = pl.multiple_of(self.yo - YHALO[level] * yi, TILE)
            self.own_at = pl.multiple_of(YHALO[level] * yi, TILE)
        else:
            self.zs, self.ys, self.own_at = self.zo, self.yo, 0
        self.zi = zi
        self.side = zi.astype(F32)
        self.z_at = self.zo - self.zs
        self.m = m
        self.row = pl.ds(self.ys, self.height)
        lane = lax.broadcasted_iota(jnp.int32, (TILE, WIDTH), 1)
        if self.split:
            self.valid = jnp.logical_or(lane < self.lanes + XHALO * (1 - xi), lane >= WIDTH - XHALO * xi)
            edges = (lane == (self.lanes - 1) * xi,)
        else:
            self.valid = lane < self.lanes
            edges = (lane == 0, lane == self.lanes - 1)
        self.outer = edges[0] if self.split else jnp.logical_or(*edges)
        self.w = jnp.where(self.valid, 1.0 / 6.0, 0.0).astype(F32)[None]
        sub, lane = iotas((self.height, WIDTH))
        if self.split:
            count = ones(lane == (self.lanes - 1) * xi) + ones(sub == (self.height - 1) * yi)
        else:
            count = (ones(lane == 0) + ones(lane == self.lanes - 1)
                     + ones(sub == 0) + ones(sub == self.rows - 1))
        m[...] = count.astype(F32)

    def ghosts(self):
        low, high = (self.zo - 1, self.zo), (self.zo + self.pairs, self.zo + self.pairs - 1)
        if self.split:
            return [tuple(a + (b - a) * self.zi for a, b in zip(low, high))]
        return [low, high]

    def odd(self, height, flip):
        sub, lane = iotas()
        return jnp.broadcast_to((lax.rem(sub + lane, 2) == (0 if flip else 1))[None], (height // TILE, TILE, WIDTH))

    def scaled(self, s):
        if self.rows % TILE and not self.split:
            sub, lane = iotas((self.height, WIDTH))
            inside = jnp.logical_and(sub < self.rows, lane < self.lanes)
            return s * jnp.where(inside, 1.0 / 6.0, 0.0).astype(F32)
        return flat(tiled(s) * self.w)


def turn(v, by):
    return pltpu.roll(v, by, 1)


def pick(v, idx):
    return jnp.take_along_axis(v, idx, axis=1)


def ones(where):
    return jnp.where(where, 1.0, 0.0)


def tiled(v):
    return v.reshape(v.shape[0] // TILE, TILE, WIDTH)


def flat(v):
    return v.reshape(v.shape[0] * TILE, WIDTH)


def choose(mask, a, b):
    return flat(jnp.where(mask, tiled(a), tiled(b)))


def loop(count, body):
    def step(i, carry):
        body(i)
        return carry
    lax.fori_loop(0, count, step, 0)


def unrolled(count, body):
    def step(i, carry):
        body(i)
        return carry
    if count == 1:
        body(0)
    elif count > 1:
        lax.fori_loop(0, count, step, 0, unroll=True)


def grouped(count, group, body):
    if count == group:
        unrolled(group, body)
    else:
        loop(count // group, lambda i: unrolled(group, lambda k: body(i * group + k)))


def ghost_planes(dst, src, lv):
    for to, frm in lv.ghosts():
        dst[to, lv.row, :] = -src[frm, lv.row, :]


def gather_sum(a, b, hb, z, y, height, mask, m):
    row = pl.ds(y, height)
    bc = b[z, row, :]
    s = bc + choose(mask, b[z + 1, row, :], b[z - 1, row, :])
    s = s + (b[z, pl.ds(y - 1, height), :] + b[z, pl.ds(y + 1, height), :])
    s = s + (turn(bc, 1) + turn(bc, WIDTH - 1))
    av = a[z, row, :]
    return s + (hb[z, row, :] - m * av), av


def half_sweep(a, b, hb, lv, colour, sums=None):
    ghost_planes(b, a, lv)
    mask = lv.odd(lv.height, colour)

    def plane(k):
        z = lv.zs + k
        m = lv.m[...]
        s, old = gather_sum(a, b, hb, z, lv.ys, lv.height, mask, m)
        new = lv.scaled(s)
        a[z, lv.row, :] = new
        if sums is not None:
            sums[k, 0:lv.height, :] = m * (old - new)
    grouped(lv.planes, UNROLL[lv.level], plane)
    if sums is not None:
        for n, (to, frm) in enumerate(lv.ghosts()):
            delta = -(a[frm, lv.row, :] + b[to, lv.row, :])
            up = lv.side if lv.split else float(n)
            k = frm - lv.zs
            sums[k, 0:lv.height, :] = sums[k, 0:lv.height, :] + choose(mask, delta * up, delta * (1.0 - up))


def relax(u, hb, lv, colour, sums=None):
    half_sweep(u[colour], u[1 - colour], hb[colour], lv, colour, sums)


def sweep(u, hb, lv):
    relax(u, hb, lv, 0)
    relax(u, hb, lv, 1)


def zero_start(u, hb, lv):
    def clear(i):
        u[1][i] = jnp.zeros(u[1].shape[1:], F32)
    loop(u[1].shape[0], clear)

    def plane(k):
        u[0][lv.zs + k, lv.row, :] = lv.scaled(hb[0][lv.zs + k, lv.row, :])
    grouped(lv.planes, UNROLL[lv.level], plane)


def restrict(u, hb, lv, sums, coarse, coarse_at):
    height = lv.own_height
    own = pl.ds(lv.own_at, height)
    ghost_planes(u[1], u[0], lv)
    mask = lv.odd(height, 0)

    def plane(k):
        s, v = gather_sum(u[0], u[1], hb[0], lv.zo + k, lv.yo, height, mask, lv.m[own, :])
        sums[lv.z_at + k, own, :] = sums[lv.z_at + k, own, :] + (s - 6.0 * v)
    grouped(lv.pairs, TILE if lv.pairs % TILE == 0 else 6, plane)

    half = lv.lanes // 2
    rows = TILE * (-(-(lv.rows // 2) // TILE))
    sub, lane = iotas((rows, WIDTH))
    even_idx = jnp.minimum(2 * lane, 126)
    odd_idx = even_idx + 1
    scale = jnp.where(iotas()[1] < half, 0.5, 0.0).astype(F32)[None]
    mask = lv.odd(rows, 0)
    zc, yc = coarse_at

    def fold(pair):
        c = []
        for s in range(2):
            z = lv.z_at + 2 * pair + s
            v = sums[z, pl.ds(lv.own_at, rows, stride=2), :] + sums[z, pl.ds(lv.own_at + 1, rows, stride=2), :]
            v = pick(v, even_idx) + pick(v, odd_idx)
            c.append(flat(tiled(v) * scale))
        coarse[0][zc + pair, pl.ds(yc, rows), :] = choose(mask, c[1], c[0])
        coarse[1][zc + pair, pl.ds(yc, rows), :] = choose(mask, c[0], c[1])
    grouped(lv.pairs // 2, min(6, lv.pairs // 2), fold)


def prolong(u, e, lv, lc, yi, xi, cx, d):
    planes = lv.planes
    crows = (lv.rows + YHALO[lv.level]) // 2
    height = TILE * (-(-crows // TILE))
    if lv.level == 0:
        zc, yc, off = lc.zo - (ZHALO[0] // 2) * lv.zi, lc.yo - (YHALO[0] // 2) * yi, 0
    elif lv.level == 1:
        zc = lc.zo + (PAIRS[2] - planes // 2) * lv.zi
        yc = lc.yo + (ROWS[2] - crows) * yi
        off = (LANES[1] // 2) * xi
    else:
        zc, yc, off = lc.zo, lc.yo, 0
    if lv.split:
        yc = pl.multiple_of(yc, TILE)
    sub, lane = iotas((height, WIDTH))
    fine_lane = jnp.where(lane < 112, lane, lane - WIDTH) if lv.split else lane
    near = lax.div(fine_lane + WIDTH, 2) - 64
    far = near + jnp.where(lax.rem(lane, 2) == 1, 1, -1)
    if lv.split:
        far = jnp.where(lane == (lv.lanes - 1) * xi, near, far)
    else:
        far = jnp.where(jnp.logical_or(lane == 0, lane == lv.lanes - 1), near, far)
    idx_near = lax.rem(near + off + WIDTH, WIDTH)
    idx_far = lax.rem(far + off + WIDTH, WIDTH)
    w_near = jnp.where(lv.valid, 0.75, 0.0).astype(F32)[None]
    w_far = jnp.where(lv.valid, jnp.where(lv.outer, -0.25, 0.25), 0.0).astype(F32)[None]
    mask = lv.odd(height, 0)

    def along_x(pair):
        r, b = e[0][zc + pair, pl.ds(yc, height), :], e[1][zc + pair, pl.ds(yc, height), :]
        for s in range(2):
            c = choose(mask, b, r) if s == 0 else choose(mask, r, b)
            c = (tiled(pick(c, idx_near)) * w_near
                 + tiled(pick(c, idx_far)) * w_far)
            cx[2 * pair + s, TILE:TILE + height, :] = flat(c)
    pairs = planes // 2
    grouped(pairs, 7 if pairs % 7 == 0 else (5 if pairs % 5 == 0 else min(6, pairs)), along_x)

    if lv.split:
        sides = ((7 + (crows + 1) * yi, TILE + (crows - 1) * yi),)
    else:
        sides = ((7, TILE), (TILE + crows, 7 + crows))

    def edge_rows(z):
        for to, frm in sides:
            cx[z, pl.ds(to, 1), :] = -cx[z, pl.ds(frm, 1), :]
    grouped(planes, 2, edge_rows)

    def along_y(z):
        mid = 0.75 * cx[z, TILE:TILE + height, :]
        d[lv.zs + z, pl.ds(lv.ys, height, stride=2), :] = mid + 0.25 * cx[z, 7:7 + height, :]
        d[lv.zs + z, pl.ds(lv.ys + 1, height, stride=2), :] = mid + 0.25 * cx[z, 9:9 + height, :]
    grouped(planes, 2, along_y)
    ghost_planes(d, d, lv)
    mask = lv.odd(lv.height, 0)

    def along_z(k):
        z = lv.zs + k
        mid = 0.75 * d[z, lv.row, :]
        up, down = 0.25 * d[z + 1, lv.row, :], 0.25 * d[z - 1, lv.row, :]
        r = u[0][z, lv.row, :] + (mid + choose(mask, up, down))
        b = u[1][z, lv.row, :] + (mid + choose(mask, down, up))
        if not lv.split and lv.rows % TILE:
            keep = iotas((lv.height, WIDTH))[0] < lv.rows
            r, b = jnp.where(keep, r, 0.0), jnp.where(keep, b, 0.0)
        u[0][z, lv.row, :] = r
        u[1][z, lv.row, :] = b
    grouped(planes, 2, along_z)


def kernel(f_hbm, u_hbm, out_hbm, *scratch):
    (u0r, u0b, f0r, f0b, u1r, u1b, h1r, h1b, u2r, u2b, h2r, h2b, u3r, u3b, h3r, h3b, u4r, u4b, h4r, h4b,
     u5r, u5b, h5r, h5b, d0, d1, d2, d3, d4, cx0, cx1, cx2, cx3, cx4, t0, t1, t2, t3, t4,
     m0, m1, m2, m3, m4, m5, raw, xs, xr0, xr1, xs1, xr2, ys, yr, zs, zr, es, er, c2r, c2b, box, gbox,
     in_sem, out_sem, x_send, x_recv, send, recv, g_send, g_recv) = scratch
    zi, yi, xi = lax.axis_index('z'), lax.axis_index('y'), lax.axis_index('x')
    peers = ({'x': 1 - xi}, {'y': 1 - yi}, {'z': 1 - zi}, {'z': 1 - zi, 'y': 1 - yi})

    chunks = [(src, c) for src in (u_hbm, f_hbm) for c in range(BRICK // CHUNK)]

    def load(n):
        src, c = chunks[n]
        return pltpu.make_async_copy(src.at[pl.ds(c * CHUNK, CHUNK)], raw.at[n % SLOTS], in_sem.at[n % SLOTS])
    for n in range(SLOTS):
        load(n).start()

    for ref in (u0r, u0b, f0r, f0b):
        def clear(i, ref=ref):
            ref[i] = jnp.zeros((NY[0], WIDTH), F32)
        loop(NZ[0], clear)
    for ref in (h1r.at[0], h1b.at[0], h1r.at[1], h1b.at[1]):
        def clear(i, ref=ref):
            ref[i] = jnp.zeros((NY[1], WIDTH), F32)
        loop(NZ[1], clear)

    barrier = pltpu.get_barrier_semaphore()
    for peer in peers:
        pl.semaphore_signal(barrier, inc=1, device_id=peer, device_id_type=MESH)

    sub, lane = iotas((BRICK, BRICK))
    odd96 = lax.rem(sub + lane, 2) == 1
    h_sq = (1.0 / N) ** 2
    for n in range(len(chunks)):
        load(n).wait()
        slot = n % SLOTS
        first = n < len(chunks) // 2
        red, black = (u0r, u0b) if first else (f0r, f0b)
        start = ZO[0] + (n % (BRICK // CHUNK)) * (CHUNK // 2)

        def pack(i):
            p0, p1 = raw[slot, 2 * i], raw[slot, 2 * i + 1]
            r, b = jnp.where(odd96, p1, p0), jnp.where(odd96, p0, p1)
            if not first:
                r, b = r * h_sq, b * h_sq
            red[start + i, YO[0]:YO[0] + BRICK, 0:BRICK] = r
            black[start + i, YO[0]:YO[0] + BRICK, 0:BRICK] = b
        loop(CHUNK // 2, pack)
        if n + SLOTS < len(chunks):
            load(n + SLOTS).start()
    pl.semaphore_wait(barrier, len(peers))

    lvs = [Level(level, zi, yi, xi, m) for level, m in enumerate((m0, m1, m2, m3, m4, m5))]
    us = ((u0r, u0b), (u1r, u1b), (u2r, u2b), (u3r, u3b), (u4r, u4b), (u5r, u5b))
    ds_ = (d0, d1, d2, d3, d4)
    cxs = (cx0, cx1, cx2, cx3, cx4)
    ts = (t0, t1, t2, t3, t4)

    box_lane = lax.broadcasted_iota(jnp.int32, (BOX, WIDTH), 1)
    quarter = lax.div(box_lane, 32)

    class Columns:
        def __init__(self, arrays, lv, s_buf, r_buf, sem_at):
            self.arrays, self.lv, self.r_buf = arrays, lv, r_buf
            self.wide = lax.broadcasted_iota(jnp.int32, (lv.rows, WIDTH), 1)
            self.row = pl.ds(lv.yo, lv.rows)
            group = lax.div(self.wide, XHALO)
            from_lane = (lv.lanes - XHALO) * (1 - xi)
            self.copies = []
            for n, a in enumerate(arrays):
                def pack_x(i, a=a, n=n):
                    acc = None
                    for k in range(TILE):
                        v = turn(a[lv.zo + TILE * i + k, self.row, :], lax.rem(XHALO * k + WIDTH - from_lane, WIDTH))
                        acc = v if k == 0 else jnp.where(group == k, v, acc)
                    s_buf[n, i] = acc
                loop(lv.pairs // TILE, pack_x)
                at = sem_at + n
                copy = pltpu.make_async_remote_copy(
                    src_ref=s_buf.at[n], dst_ref=r_buf.at[n], send_sem=x_send.at[at], recv_sem=x_recv.at[at],
                    device_id=peers[0], device_id_type=MESH)
                copy.start()
                self.copies.append(copy)

        def finish(self):
            lv, row = self.lv, self.row
            to_lane = lv.lanes + (112 - lv.lanes) * xi
            inside = jnp.logical_and(self.wide >= to_lane, self.wide < to_lane + XHALO)
            for n, a in enumerate(self.arrays):
                self.copies[n].wait()

                def unpack_x(i, a=a, n=n):
                    acc = self.r_buf[n, i]
                    for k in range(TILE):
                        z = lv.zo + TILE * i + k
                        v = turn(acc, lax.rem(to_lane + WIDTH - XHALO * k, WIDTH))
                        a[z, row, :] = jnp.where(inside, v, a[z, row, :])
                loop(lv.pairs // TILE, unpack_x)

    def send_faces(specs, lv, sem_at, start=True):
        copies = []
        for a, zn, yn in specs:
            z_own, y_own = pl.ds(lv.zo, lv.pairs), pl.ds(lv.yo, lv.rows)
            y_in = lv.yo + (lv.rows - yn) * (1 - yi)
            y_to = lv.yo - yn + (lv.rows + yn) * yi
            z_in = lv.zo + (lv.pairs - zn) * (1 - zi)
            z_to = lv.zo - zn + (lv.pairs + zn) * zi
            parts = (
                ((z_own, pl.ds(y_in, yn)), (z_own, pl.ds(y_to, yn)), peers[1]),
                ((pl.ds(z_in, zn), y_own), (pl.ds(z_to, zn), y_own), peers[2]),
                ((pl.ds(z_in, zn), pl.ds(y_in, yn)), (pl.ds(z_to, zn), pl.ds(y_to, yn)), peers[3]),
            )
            for src, dst, peer in parts:
                at = sem_at + len(copies)
                copy = pltpu.make_async_remote_copy(
                    src_ref=a.at[src[0], src[1]], dst_ref=a.at[dst[0], dst[1]], send_sem=send.at[at], recv_sem=recv.at[at],
                    device_id=peer, device_id_type=MESH)
                if start:
                    copy.start()
                copies.append(copy)
        return copies

    class Faces:
        def __init__(self, h, lv, cycle):
            self.h, self.cycle = h, cycle
            thick = DEEP // 2
            y_in, z_in = lv.yo + (lv.rows - DEEP) * (1 - yi), lv.zo + (lv.pairs - thick) * (1 - zi)
            y_to, z_to = lv.yo + lv.rows - (lv.rows + DEEP) * yi, lv.zo + lv.pairs - (lv.pairs + thick) * zi
            self.parts = ((ys, yr, lv.zo, lv.pairs, y_in, DEEP, lv.zo, y_to),
                          (zs, zr, z_in, thick, lv.yo, lv.rows, z_to, lv.yo),
                          (es, er, z_in, thick, y_in, DEEP, z_to, y_to))
            self.copies = []
            for n, (out, into, z, planes, y, rows, _, _) in enumerate(self.parts):
                lane = lax.broadcasted_iota(jnp.int32, (rows, WIDTH), 1)

                def pack(i):
                    r, b = h[0][z + i, pl.ds(y, rows), :], h[1][z + i, pl.ds(y, rows), :]
                    out[i] = jnp.where(lane < 64, turn(r, XHALO * xi), turn(b, XHALO * xi + 64))
                grouped(planes, 6, pack)
                at = 12 + n
                copy = pltpu.make_async_remote_copy(
                    src_ref=out, dst_ref=into.at[cycle], send_sem=send.at[at], recv_sem=recv.at[at],
                    device_id=peers[n + 1], device_id_type=MESH)
                copy.start()
                self.copies.append(copy)

        def finish(self):
            for copy, (_, into, _, planes, _, rows, z, y) in zip(self.copies, self.parts):
                copy.wait()
                lane = lax.broadcasted_iota(jnp.int32, (rows, WIDTH), 1)
                valid = jnp.logical_or(lane < 64 - XHALO * xi, lane >= WIDTH - XHALO * xi)

                def unpack(i):
                    v = into[self.cycle, i]
                    for c in range(2):
                        w = turn(v, lax.rem(WIDTH - 64 * c - XHALO * xi, WIDTH))
                        self.h[c][z + i, pl.ds(y, rows), :] = jnp.where(valid, w, 0.0)
                grouped(planes, 6, unpack)

    def gather_level2(cycle):
        def pack_box(i):
            for c, a in enumerate((c2r, c2b)):
                acc = a[4 * i]
                for k in range(1, 4):
                    acc = jnp.where(quarter == k, turn(a[4 * i + k], 32 * k), acc)
                box[cycle, c, i] = acc
        loop(3, pack_box)
        me = 4 * xi + 2 * zi + yi
        copies = []
        for n, peer in enumerate(peers):
            copy = pltpu.make_async_remote_copy(
                src_ref=box.at[cycle], dst_ref=gbox.at[cycle, me], send_sem=g_send.at[cycle, n], recv_sem=g_recv.at[cycle, n],
                device_id=peer, device_id_type=MESH)
            copy.start()
            copies.append(copy)
        for n, (dz, dy) in ((1, (0, 1)), (2, (1, 0)), (3, (1, 1))):
            copies[n].wait_recv()
            sz, sy = zi + dz - 2 * dz * zi, yi + dy - 2 * dy * yi
            at = 4 * xi + 2 * sz + sy
            copy = pltpu.make_async_remote_copy(
                src_ref=gbox.at[cycle, at], dst_ref=gbox.at[cycle, at], send_sem=g_send.at[cycle, 3 + n],
                recv_sem=g_recv.at[cycle, 3 + n], device_id=peers[0], device_id_type=MESH)
            copy.start()
            copies.append(copy)
        copies[0].wait_recv()
        for copy in copies[:4]:
            copy.wait_send()
        for copy in copies[4:]:
            copy.wait()
        for c, a in enumerate((c2r, c2b)):
            gbox[cycle, me, c] = box[cycle, c]

        def unpack_box(i):
            for c, a in enumerate((h2r, h2b)):
                for q in range(4):
                    sz, sy = divmod(q, 2)
                    lo, hi = gbox[cycle, q, c, i], gbox[cycle, 4 + q, c, i]
                    for k in range(4):
                        lower = turn(lo, WIDTH - 32 * k) if k else lo
                        upper = turn(hi, (152 - 32 * k) % WIDTH)
                        v = jnp.where(box_lane < BOX, lower, jnp.where(box_lane < 48, upper, 0.0))
                        a[ZO[2] + 12 * sz + 4 * i + k, YO[2] + BOX * sy:YO[2] + BOX * sy + BOX, :] = v
        loop(3, unpack_box)

    l0 = lvs[0]
    x_u = Columns((u0r, u0b), l0, xs, xr0, 0)
    x_f = Columns((f0r, f0b), l0, xs.at[2:4], xr0.at[2:4], 2)
    x_u.finish()
    faces = send_faces(((u0r, 2, 4), (u0b, 3, 5)), l0, 0)
    x_f.finish()
    faces += send_faces(((f0r, 2, 4), (f0b, 2, 4)), l0, 6)
    for ref in (u1r, u1b, u2r, u2b, h2r, h2b, u3r, u3b, h3r, h3b, u4r, u4b, h4r, h4b, u5r, u5b, h5r, h5b,
                d0, d1, d2, d3, d4, cx0, cx1, cx2, cx3, cx4, t0, t1, t2, t3, t4):
        def clear(i, ref=ref):
            ref[i] = jnp.zeros(ref.shape[1:], F32)
        loop(ref.shape[0], clear)
    for copy in faces:
        copy.wait()

    def v_cycle(cycle):
        h1 = (h1r.at[cycle], h1b.at[cycle])
        hs = ((f0r, f0b), h1, (h2r, h2b), (h3r, h3b), (h4r, h4b), (h5r, h5b))
        l1 = lvs[1]
        sweep(us[0], hs[0], l0)
        relax(us[0], hs[0], l0, 0)
        relax(us[0], hs[0], l0, 1, ts[0])
        restrict(us[0], hs[0], l0, ts[0], h1, (ZO[1], YO[1]))
        Columns(h1, l1, xs1, xr2.at[cycle], TILE).finish()
        faces = Faces(h1, l1, cycle)
        Columns(us[0], l0, xs, xr1.at[cycle], 4).finish()
        faces.finish()
        for level in range(1, 5):
            lv = lvs[level]
            zero_start(us[level], hs[level], lv)
            u, h = us[level], hs[level]
            relax(u, h, lv, 1)
            relax(u, h, lv, 0)
            relax(u, h, lv, 1, ts[level])
            if level == 1:
                restrict(us[1], h1, l1, ts[1], (c2r, c2b), (0, 0))
                gather_level2(cycle)
                pending = send_faces(((u0r, 4, TILE), (u0b, 5, 9)), l0, 18)

                @pl.when(cycle == 0)
                def deeper_source():
                    send_faces(((f0r, 4, TILE), (f0b, 4, TILE)), l0, 0)
            else:
                restrict(us[level], hs[level], lv, ts[level], hs[level + 1], (ZO[level + 1], YO[level + 1]))
        lv = lvs[5]
        zero_start(us[5], hs[5], lv)
        relax(us[5], hs[5], lv, 1)
        loop(COARSE_SWEEPS - 1, lambda i: sweep(us[5], hs[5], lvs[5]))
        for level in range(4, -1, -1):
            lv = lvs[level]
            if level == 0:
                for copy in pending:
                    copy.wait()

                @pl.when(cycle == 0)
                def deeper_source_arrived():
                    for copy in send_faces(((f0r, 4, TILE), (f0b, 4, TILE)), l0, 0, False):
                        copy.wait()
            prolong(us[level], us[level + 1], lv, lvs[level + 1], yi, xi, cxs[level], ds_[level])
            loop(2, lambda i, lv=lv, level=level: sweep(us[level], hs[level], lv))
    loop(CYCLES, v_cycle)

    stores = []
    for n in range(BRICK // CHUNK):
        slot = n % SLOTS
        if n >= SLOTS:
            stores[n - SLOTS].wait()

        def unpack(i):
            z = ZO[0] + n * (CHUNK // 2) + i
            r, b = u0r[z, YO[0]:YO[0] + BRICK, 0:BRICK], u0b[z, YO[0]:YO[0] + BRICK, 0:BRICK]
            raw[slot, 2 * i] = jnp.where(odd96, b, r)
            raw[slot, 2 * i + 1] = jnp.where(odd96, r, b)
        loop(CHUNK // 2, unpack)
        copy = pltpu.make_async_copy(raw.at[slot], out_hbm.at[pl.ds(n * CHUNK, CHUNK)], out_sem.at[slot])
        copy.start()
        stores.append(copy)
    for copy in stores[-SLOTS:]:
        copy.wait()


def vmem(*shape):
    return pltpu.VMEM(shape, F32)


def scratch_shapes():
    arr = [vmem(NZ[level], NY[level], WIDTH) for level in range(6)]
    shapes = [arr[0]] * 4 + [arr[1]] * 2 + [vmem(2, NZ[1], NY[1], WIDTH)] * 2
    for level in range(2, 6):
        shapes += [arr[level]] * 4
    shapes += arr[:5]
    for extra in (BOX, 0):
        for level in range(5):
            rows = WINDOW[level] // 2 + extra if extra else -(-WINDOW[level] // XHALO) * XHALO
            shapes.append(vmem(PAIRS[level] + ZHALO[level], rows, WIDTH))
    shapes += [vmem(height, WIDTH) for height in WINDOW]
    shapes += [vmem(SLOTS, CHUNK, BRICK, BRICK)]
    shapes += [vmem(4, 6, BRICK, WIDTH), vmem(4, 6, BRICK, WIDTH), vmem(2, 2, 6, BRICK, WIDTH)]
    shapes += [vmem(2, 3, 48, WIDTH), vmem(2, 2, 3, 48, WIDTH)]
    for planes, rows in ((BOX, DEEP), (DEEP // 2, ROWS[1]), (DEEP // 2, DEEP)):
        shapes += [vmem(planes, rows, WIDTH), vmem(2, planes, rows, WIDTH)]
    shapes += [vmem(12, BOX, WIDTH), vmem(12, BOX, WIDTH), vmem(2, 2, 3, BOX, WIDTH), vmem(2, TILE, 2, 3, BOX, WIDTH)]
    dma = pltpu.SemaphoreType.DMA
    shapes += [dma((SLOTS,)), dma((SLOTS,)), dma((10,)), dma((10,)), dma((BOX,)), dma((BOX,)), dma((2, 7)), dma((2, 7))]
    return shapes


def solution(mesh):
    spec = P(('batch', 'z'), 'y', 'x')

    def local_solve(source, initial_guess):
        return pl.pallas_call(
            kernel,
            out_shape=jax.ShapeDtypeStruct(source.shape, F32),
            in_specs=[pl.BlockSpec(memory_space=pl.ANY)] * 2,
            out_specs=pl.BlockSpec(memory_space=pl.ANY),
            scratch_shapes=scratch_shapes(),
            compiler_params=pltpu.CompilerParams(collective_id=0, has_side_effects=True, vmem_limit_bytes=67043328),
            name='multigrid',
        )(source, initial_guess)

    return jax.shard_map(local_solve, mesh=mesh, in_specs=(spec, spec), out_specs=spec, check_vma=False)
```

```python
import jax
import jax.numpy as jnp
from jax import lax
from jax.experimental import pallas as pl
from jax.experimental.pallas import tpu as pltpu
from jax.sharding import PartitionSpec as P

N = 192
CYCLES = 2
COARSE_SWEEPS = 24
F32 = jnp.float32
MESH = pl.DeviceIdType.MESH

ROWS = LANES = (96, 48, 48, 24, 12, 6)
PAIRS = tuple(rows // 2 for rows in ROWS)
ZO = (9, 7, 1, 1, 1, 1)
NZ = tuple(pairs + 2 * first for pairs, first in zip(PAIRS, ZO))
YO = (24, 24, 8, 8, 8, 8)
NY = tuple(-(-rows // 8) * 8 + 2 * first for rows, first in zip(ROWS, YO))
ZHALO = (8, 6, 0, 0, 0, 0)
YHALO = (16, 16, 0, 0, 0, 0)
WINDOW = tuple(-(-(rows + halo) // 8) * 8 for rows, halo in zip(ROWS, YHALO))
UNROLL = (14, 15, 24, 12, 6, 3)
CHUNK = 16
SLOTS = 4
WIDTH = 128
TILE = 8
BRICK = 96
BOX = 24
XHALO = 16
DEEP = 12
HALF = 64


def iotas(shape=(TILE, WIDTH)):
    return lax.broadcasted_iota(jnp.int32, shape, 0), lax.broadcasted_iota(jnp.int32, shape, 1)


class Level:
    def __init__(self, level, zi, yi, xi, m, zhalo, yhalo, unroll):
        self.level = level
        self.unroll = unroll
        self.split = level < 2
        self.pairs, self.rows, self.lanes = PAIRS[level], ROWS[level], LANES[level]
        self.zo, self.yo = ZO[level], YO[level]
        self.planes = self.pairs + zhalo
        self.height = TILE * (-(-(self.rows + yhalo) // TILE))
        self.own_height = TILE * (-(-self.rows // TILE))
        if self.split:
            self.zs = self.zo - zhalo * zi
            self.ys = pl.multiple_of(self.yo - yhalo * yi, TILE)
            self.own_at = pl.multiple_of(yhalo * yi, TILE)
        else:
            self.zs, self.ys, self.own_at = self.zo, self.yo, 0
        self.zi = zi
        self.side = zi.astype(F32)
        self.z_at = self.zo - self.zs
        self.m = m
        self.row = pl.ds(self.ys, self.height)
        lane = lax.broadcasted_iota(jnp.int32, (TILE, WIDTH), 1)
        if self.split:
            self.valid = jnp.logical_or(lane < self.lanes + XHALO * (1 - xi), lane >= WIDTH - XHALO * xi)
            edges = (lane == (self.lanes - 1) * xi,)
        else:
            self.valid = lane < self.lanes
            edges = (lane == 0, lane == self.lanes - 1)
        self.outer = edges[0] if self.split else jnp.logical_or(*edges)
        self.w = jnp.where(self.valid, 1.0 / 6.0, 0.0).astype(F32)[None]
        sub, lane = iotas((self.height, WIDTH))
        if self.split:
            count = ones(lane == (self.lanes - 1) * xi) + ones(sub == (self.height - 1) * yi)
        else:
            count = (ones(lane == 0) + ones(lane == self.lanes - 1)
                     + ones(sub == 0) + ones(sub == self.rows - 1))
        m[...] = count.astype(F32)

    def ghosts(self):
        low, high = (self.zo - 1, self.zo), (self.zo + self.pairs, self.zo + self.pairs - 1)
        if self.split:
            return [tuple(a + (b - a) * self.zi for a, b in zip(low, high))]
        return [low, high]

    def odd(self, height, flip):
        sub, lane = iotas()
        return jnp.broadcast_to((lax.rem(sub + lane, 2) == (0 if flip else 1))[None], (height // TILE, TILE, WIDTH))

    def scaled(self, s):
        if self.rows % TILE and not self.split:
            sub, lane = iotas((self.height, WIDTH))
            inside = jnp.logical_and(sub < self.rows, lane < self.lanes)
            return s * jnp.where(inside, 1.0 / 6.0, 0.0).astype(F32)
        return flat(tiled(s) * self.w)


def turn(v, by):
    return pltpu.roll(v, by, 1)


def pick(v, idx):
    return jnp.take_along_axis(v, idx, axis=1)


def ones(where):
    return jnp.where(where, 1.0, 0.0)


def tiled(v):
    return v.reshape(v.shape[0] // TILE, TILE, WIDTH)


def flat(v):
    return v.reshape(v.shape[0] * TILE, WIDTH)


def choose(mask, a, b):
    return flat(jnp.where(mask, tiled(a), tiled(b)))


def loop(count, body):
    def step(i, carry):
        body(i)
        return carry
    lax.fori_loop(0, count, step, 0)


def unrolled(count, body):
    def step(i, carry):
        body(i)
        return carry
    if count == 1:
        body(0)
    elif count > 1:
        lax.fori_loop(0, count, step, 0, unroll=True)


def grouped(count, group, body):
    if count == group:
        unrolled(group, body)
    else:
        loop(count // group, lambda i: unrolled(group, lambda k: body(i * group + k)))


def ghost_planes(dst, src, lv):
    for to, frm in lv.ghosts():
        dst[to, lv.row, :] = -src[frm, lv.row, :]


def gather_sum(a, b, hb, z, y, height, mask, m):
    row = pl.ds(y, height)
    bc = b[z, row, :]
    s = bc + choose(mask, b[z + 1, row, :], b[z - 1, row, :])
    s = s + (b[z, pl.ds(y - 1, height), :] + b[z, pl.ds(y + 1, height), :])
    s = s + (turn(bc, 1) + turn(bc, WIDTH - 1))
    av = a[z, row, :]
    return s + (hb[z, row, :] - m * av), av


def half_sweep(a, b, hb, lv, colour, sums=None):
    ghost_planes(b, a, lv)
    mask = lv.odd(lv.height, colour)

    def plane(k):
        z = lv.zs + k
        m = lv.m[...]
        s, old = gather_sum(a, b, hb, z, lv.ys, lv.height, mask, m)
        new = lv.scaled(s)
        if sums is not None:
            new = new + lv.scaled(s - 6.0 * new)
        a[z, lv.row, :] = new
        if sums is not None:
            sums[k, 0:lv.height, :] = m * (old - new)
    grouped(lv.planes, lv.unroll, plane)
    if sums is not None:
        for n, (to, frm) in enumerate(lv.ghosts()):
            delta = -(a[frm, lv.row, :] + b[to, lv.row, :])
            up = lv.side if lv.split else float(n)
            k = frm - lv.zs
            sums[k, 0:lv.height, :] = sums[k, 0:lv.height, :] + choose(mask, delta * up, delta * (1.0 - up))


def relax(u, hb, lv, colour, sums=None):
    half_sweep(u[colour], u[1 - colour], hb[colour], lv, colour, sums)


def sweep(u, hb, lv):
    relax(u, hb, lv, 0)
    relax(u, hb, lv, 1)


def zero_start(u, hb, lv):
    def clear(i):
        u[1][i] = jnp.zeros(u[1].shape[1:], F32)
    loop(u[1].shape[0], clear)

    def plane(k):
        u[0][lv.zs + k, lv.row, :] = lv.scaled(hb[0][lv.zs + k, lv.row, :])
    grouped(lv.planes, lv.unroll, plane)


def restrict(u, hb, lv, sums, coarse, coarse_at):
    height = lv.own_height
    own = pl.ds(lv.own_at, height)
    ghost_planes(u[1], u[0], lv)
    mask = lv.odd(height, 0)

    def plane(k):
        s, v = gather_sum(u[0], u[1], hb[0], lv.zo + k, lv.yo, height, mask, lv.m[own, :])
        sums[lv.z_at + k, own, :] = sums[lv.z_at + k, own, :] + (s - 6.0 * v)
    grouped(lv.pairs, min(12, lv.pairs), plane)

    half = lv.lanes // 2
    rows = TILE * (-(-(lv.rows // 2) // TILE))
    sub, lane = iotas((rows, WIDTH))
    even_idx = jnp.minimum(2 * lane, 126)
    odd_idx = even_idx + 1
    scale = jnp.where(iotas()[1] < half, 0.5, 0.0).astype(F32)[None]
    mask = lv.odd(rows, 0)
    zc, yc = coarse_at

    def fold(pair):
        c = []
        for s in range(2):
            z = lv.z_at + 2 * pair + s
            v = sums[z, pl.ds(lv.own_at, rows, stride=2), :] + sums[z, pl.ds(lv.own_at + 1, rows, stride=2), :]
            v = pick(v, even_idx) + pick(v, odd_idx)
            c.append(flat(tiled(v) * scale))
        coarse[0][zc + pair, pl.ds(yc, rows), :] = choose(mask, c[1], c[0])
        coarse[1][zc + pair, pl.ds(yc, rows), :] = choose(mask, c[0], c[1])
    grouped(lv.pairs // 2, min(6, lv.pairs // 2), fold)


def prolong(u, e, lv, lc, yi, xi, cx, d):
    planes = lv.planes
    crows = (lv.rows + YHALO[lv.level]) // 2
    height = TILE * (-(-crows // TILE))
    if lv.level == 0:
        zc, yc, off = lc.zo - (ZHALO[0] // 2) * lv.zi, lc.yo - (YHALO[0] // 2) * yi, 0
    elif lv.level == 1:
        zc = lc.zo + (PAIRS[2] - planes // 2) * lv.zi
        yc = lc.yo + (ROWS[2] - crows) * yi
        off = (LANES[1] // 2) * xi
    else:
        zc, yc, off = lc.zo, lc.yo, 0
    if lv.split:
        yc = pl.multiple_of(yc, TILE)
    sub, lane = iotas((height, WIDTH))
    fine_lane = jnp.where(lane < 112, lane, lane - WIDTH) if lv.split else lane
    near = lax.div(fine_lane + WIDTH, 2) - 64
    far = near + jnp.where(lax.rem(lane, 2) == 1, 1, -1)
    if lv.split:
        far = jnp.where(lane == (lv.lanes - 1) * xi, near, far)
    else:
        far = jnp.where(jnp.logical_or(lane == 0, lane == lv.lanes - 1), near, far)
    idx_near = lax.rem(near + off + WIDTH, WIDTH)
    idx_far = lax.rem(far + off + WIDTH, WIDTH)
    w_near = jnp.where(lv.valid, 0.75, 0.0).astype(F32)[None]
    w_far = jnp.where(lv.valid, jnp.where(lv.outer, -0.25, 0.25), 0.0).astype(F32)[None]
    mask = lv.odd(height, 0)

    def along_x(pair):
        r, b = e[0][zc + pair, pl.ds(yc, height), :], e[1][zc + pair, pl.ds(yc, height), :]
        for s in range(2):
            c = choose(mask, b, r) if s == 0 else choose(mask, r, b)
            c = (tiled(pick(c, idx_near)) * w_near
                 + tiled(pick(c, idx_far)) * w_far)
            cx[2 * pair + s, TILE:TILE + height, :] = flat(c)
    pairs = planes // 2
    grouped(pairs, 7 if pairs % 7 == 0 else (5 if pairs % 5 == 0 else min(6, pairs)), along_x)

    if lv.split:
        sides = ((7 + (crows + 1) * yi, TILE + (crows - 1) * yi),)
    else:
        sides = ((7, TILE), (TILE + crows, 7 + crows))

    def edge_rows(z):
        for to, frm in sides:
            cx[z, pl.ds(to, 1), :] = -cx[z, pl.ds(frm, 1), :]
    grouped(planes, 2, edge_rows)

    def along_y(z):
        mid = 0.75 * cx[z, TILE:TILE + height, :]
        d[lv.zs + z, pl.ds(lv.ys, height, stride=2), :] = mid + 0.25 * cx[z, 7:7 + height, :]
        d[lv.zs + z, pl.ds(lv.ys + 1, height, stride=2), :] = mid + 0.25 * cx[z, 9:9 + height, :]
    grouped(planes, 2, along_y)
    ghost_planes(d, d, lv)
    mask = lv.odd(lv.height, 0)

    def along_z(k):
        z = lv.zs + k
        mid = 0.75 * d[z, lv.row, :]
        up, down = 0.25 * d[z + 1, lv.row, :], 0.25 * d[z - 1, lv.row, :]
        r = u[0][z, lv.row, :] + (mid + choose(mask, up, down))
        b = u[1][z, lv.row, :] + (mid + choose(mask, down, up))
        if not lv.split and lv.rows % TILE:
            keep = iotas((lv.height, WIDTH))[0] < lv.rows
            r, b = jnp.where(keep, r, 0.0), jnp.where(keep, b, 0.0)
        u[0][z, lv.row, :] = r
        u[1][z, lv.row, :] = b
    grouped(planes, 2, along_z)


def coarsest(h, u, lv, qu, qh):
    edge = lv.lanes
    box = (edge, TILE, WIDTH)
    x, y, lane = (lax.broadcasted_iota(jnp.int32, box, d) for d in range(3))
    rows = pl.ds(TILE, TILE)
    for c in range(2):
        for k in range(lv.pairs):
            v = h[c][lv.zo + k, rows, :]
            for i in range(edge):
                qh[c, k, i] = pick(v, jnp.full((TILE, WIDTH), i, jnp.int32))
    clear_all((qu,))
    inner = ones(y < edge).astype(F32) / 6.0
    faces = (ones(x == 0) + ones(x == edge - 1) + ones(y == 0) + ones(y == edge - 1)).astype(F32)
    own = pl.ds(1, edge)

    def sweeps(_):
        for c in range(2):
            up = lax.rem(x + y + c, 2) == 1
            up_f = ones(up).astype(F32)
            for k in range(lv.pairs):
                m = faces
                if k == 0:
                    m = m + (1.0 - up_f)
                if k == lv.pairs - 1:
                    m = m + up_f
                z = k + 1
                b, a = qu.at[1 - c], qu.at[c]
                s = b[z, own, rows, :] + jnp.where(up, b[z + 1, own, rows, :], b[z - 1, own, rows, :])
                s = s + (b[z, own, pl.ds(TILE - 1, TILE), :] + b[z, own, pl.ds(TILE + 1, TILE), :])
                s = s + (b[z, pl.ds(0, edge), rows, :] + b[z, pl.ds(2, edge), rows, :])
                a[z, own, rows, :] = (s + (qh[c, k] - m * a[z, own, rows, :])) * inner
    loop(COARSE_SWEEPS, sweeps)
    for c in range(2):
        for k in range(lv.pairs):
            v = qu[c, k + 1, own, rows, :]
            total = jnp.where(lane[0] == 0, v[0], 0.0)
            for i in range(1, edge):
                total = jnp.where(lane[0] == i, v[i], total)
            u[c][lv.zo + k, rows, :] = total


def clear_all(refs):
    for ref in refs:
        def clear(i, ref=ref):
            ref[i] = jnp.zeros(ref.shape[1:], F32)
        loop(ref.shape[0], clear)


def kernel(f_hbm, u_hbm, out_hbm, *scratch):
    (u0r, u0b, f0r, f0b, u1r, u1b, h1r, h1b, u2r, u2b, h2r, h2b, u3r, u3b, h3r, h3b, u4r, u4b, h4r, h4b,
     u5r, u5b, h5r, h5b, d0, d1, d2, d3, d4, cx0, cx1, cx2, cx3, cx4, t0, t1, t2, t3, t4,
     m0, m1, m2, m3, m4, m5, m6, raw, xs, xr0, xr1, xs1, xr2, ys, yr, zs, zr, es, er, qu, qh, c2r, c2b, box, gbox,
     in_sem, out_sem, x_send, x_recv, send, recv, g_send, g_recv) = scratch
    zi, yi, xi = lax.axis_index('z'), lax.axis_index('y'), lax.axis_index('x')
    nx, ny, nz = 1 - xi, 1 - yi, 1 - zi
    peers = ({'x': nx}, {'y': ny}, {'z': nz}, {'z': nz, 'y': ny})

    chunks = [(src, c) for src in (u_hbm, f_hbm) for c in range(BRICK // CHUNK)]

    def load(n):
        src, c = chunks[n]
        return pltpu.make_async_copy(src.at[pl.ds(c * CHUNK, CHUNK)], raw.at[n % SLOTS], in_sem.at[n % SLOTS])
    for n in range(SLOTS):
        load(n).start()

    for ref in (u0r, u0b, f0r, f0b):
        clear_all((ref,))
    for ref in (h1r.at[0], h1b.at[0], h1r.at[1], h1b.at[1]):
        clear_all((ref,))

    barrier = pltpu.get_barrier_semaphore()
    for peer in peers:
        pl.semaphore_signal(barrier, inc=1, device_id=peer, device_id_type=MESH)

    sub, lane = iotas((BRICK, BRICK))
    odd96 = lax.rem(sub + lane, 2) == 1
    h_sq = (1.0 / N) ** 2
    for n in range(len(chunks)):
        load(n).wait()
        slot = n % SLOTS
        first = n < len(chunks) // 2
        red, black = (u0r, u0b) if first else (f0r, f0b)
        start = ZO[0] + (n % (BRICK // CHUNK)) * (CHUNK // 2)

        def pack(i):
            p0, p1 = raw[slot, 2 * i], raw[slot, 2 * i + 1]
            r, b = jnp.where(odd96, p1, p0), jnp.where(odd96, p0, p1)
            if not first:
                r, b = r * h_sq, b * h_sq
            red[start + i, YO[0]:YO[0] + BRICK, 0:BRICK] = r
            black[start + i, YO[0]:YO[0] + BRICK, 0:BRICK] = b
        loop(CHUNK // 2, pack)
        if n + SLOTS < len(chunks):
            load(n + SLOTS).start()
    pl.semaphore_wait(barrier, len(peers))

    lvs = [Level(level, zi, yi, xi, m, ZHALO[level], YHALO[level], UNROLL[level])
           for level, m in enumerate((m0, m1, m2, m3, m4, m5))]
    near = Level(0, zi, yi, xi, m6, 4, TILE, 13)
    us = ((u0r, u0b), (u1r, u1b), (u2r, u2b), (u3r, u3b), (u4r, u4b), (u5r, u5b))
    ds_ = (d0, d1, d2, d3, d4)
    cxs = (cx0, cx1, cx2, cx3, cx4)
    ts = (t0, t1, t2, t3, t4)

    box_lane = lax.broadcasted_iota(jnp.int32, (BOX, WIDTH), 1)
    quarter = lax.div(box_lane, 32)

    class Columns:
        def __init__(self, arrays, lv, s_buf, r_buf, sem_at):
            self.arrays, self.lv, self.r_buf = arrays, lv, r_buf
            self.wide = lax.broadcasted_iota(jnp.int32, (lv.rows, WIDTH), 1)
            self.row = pl.ds(lv.yo, lv.rows)
            group = lax.div(self.wide, XHALO)
            from_lane = (lv.lanes - XHALO) * nx
            self.copies = []
            for n, a in enumerate(arrays):
                def pack_x(i, a=a, n=n):
                    acc = None
                    for k in range(TILE):
                        v = turn(a[lv.zo + TILE * i + k, self.row, :], lax.rem(XHALO * k + WIDTH - from_lane, WIDTH))
                        acc = v if k == 0 else jnp.where(group == k, v, acc)
                    s_buf[n, i] = acc
                loop(lv.pairs // TILE, pack_x)
                at = sem_at + n
                copy = pltpu.make_async_remote_copy(
                    src_ref=s_buf.at[n], dst_ref=r_buf.at[n], send_sem=x_send.at[at], recv_sem=x_recv.at[at],
                    device_id=peers[0], device_id_type=MESH)
                copy.start()
                self.copies.append(copy)

        def finish(self):
            lv, row = self.lv, self.row
            to_lane = lv.lanes + (112 - lv.lanes) * xi
            inside = jnp.logical_and(self.wide >= to_lane, self.wide < to_lane + XHALO)
            for n, a in enumerate(self.arrays):
                self.copies[n].wait()

                def unpack_x(i, a=a, n=n):
                    acc = self.r_buf[n, i]
                    for k in range(TILE):
                        z = lv.zo + TILE * i + k
                        v = turn(acc, lax.rem(to_lane + WIDTH - XHALO * k, WIDTH))
                        a[z, row, :] = jnp.where(inside, v, a[z, row, :])
                loop(lv.pairs // TILE, unpack_x)

    def send_faces(specs, lv, sem_at, start=True):
        copies = []
        for a, zn, yn in specs:
            z_own, y_own = pl.ds(lv.zo, lv.pairs), pl.ds(lv.yo, lv.rows)
            y_in = lv.yo + (lv.rows - yn) * ny
            y_to = lv.yo - yn + (lv.rows + yn) * yi
            z_in = lv.zo + (lv.pairs - zn) * nz
            z_to = lv.zo - zn + (lv.pairs + zn) * zi
            parts = (
                ((z_own, pl.ds(y_in, yn)), (z_own, pl.ds(y_to, yn)), peers[1]),
                ((pl.ds(z_in, zn), y_own), (pl.ds(z_to, zn), y_own), peers[2]),
                ((pl.ds(z_in, zn), pl.ds(y_in, yn)), (pl.ds(z_to, zn), pl.ds(y_to, yn)), peers[3]),
            )
            for src, dst, peer in parts:
                at = sem_at + len(copies)
                copy = pltpu.make_async_remote_copy(
                    src_ref=a.at[src[0], src[1]], dst_ref=a.at[dst[0], dst[1]], send_sem=send.at[at], recv_sem=recv.at[at],
                    device_id=peer, device_id_type=MESH)
                if start:
                    copy.start()
                copies.append(copy)
        return copies

    class Faces:
        def __init__(self, h, lv, cycle):
            self.h, self.cycle = h, cycle
            thick = DEEP // 2
            y_in, z_in = lv.yo + (lv.rows - DEEP) * ny, lv.zo + (lv.pairs - thick) * nz
            y_to, z_to = lv.yo + lv.rows - (lv.rows + DEEP) * yi, lv.zo + lv.pairs - (lv.pairs + thick) * zi
            self.parts = ((ys, yr, lv.zo, lv.pairs, y_in, DEEP, lv.zo, y_to),
                          (zs, zr, z_in, thick, lv.yo, lv.rows, z_to, lv.yo),
                          (es, er, z_in, thick, y_in, DEEP, z_to, y_to))
            self.copies = []
            for n, (out, into, z, planes, y, rows, _, _) in enumerate(self.parts):
                lane = lax.broadcasted_iota(jnp.int32, (rows, WIDTH), 1)

                def pack(i):
                    r, b = h[0][z + i, pl.ds(y, rows), :], h[1][z + i, pl.ds(y, rows), :]
                    out[i] = jnp.where(lane < HALF, turn(r, XHALO * xi), turn(b, XHALO * xi + HALF))
                grouped(planes, 6, pack)
                at = 12 + n
                copy = pltpu.make_async_remote_copy(
                    src_ref=out, dst_ref=into.at[cycle], send_sem=send.at[at], recv_sem=recv.at[at],
                    device_id=peers[n + 1], device_id_type=MESH)
                copy.start()
                self.copies.append(copy)

        def finish(self):
            for copy, (_, into, _, planes, _, rows, z, y) in zip(self.copies, self.parts):
                copy.wait()
                lane = lax.broadcasted_iota(jnp.int32, (rows, WIDTH), 1)
                valid = jnp.logical_or(lane < HALF - XHALO * xi, lane >= WIDTH - XHALO * xi)

                def unpack(i):
                    v = into[self.cycle, i]
                    for c in range(2):
                        w = turn(v, lax.rem(WIDTH - HALF * c - XHALO * xi, WIDTH))
                        self.h[c][z + i, pl.ds(y, rows), :] = jnp.where(valid, w, 0.0)
                grouped(planes, 6, unpack)

    def gather_level2(cycle):
        def pack_box(i):
            for c, a in enumerate((c2r, c2b)):
                acc = a[4 * i]
                for k in range(1, 4):
                    acc = jnp.where(quarter == k, turn(a[4 * i + k], 32 * k), acc)
                box[cycle, c, i] = acc
        loop(3, pack_box)
        me = 4 * xi + 2 * zi + yi
        copies = []
        for n, peer in enumerate(peers):
            copy = pltpu.make_async_remote_copy(
                src_ref=box.at[cycle], dst_ref=gbox.at[cycle, me], send_sem=g_send.at[cycle, n], recv_sem=g_recv.at[cycle, n],
                device_id=peer, device_id_type=MESH)
            copy.start()
            copies.append(copy)
        for n in range(1, len(peers)):
            dz, dy = divmod(n, 2)
            copies[n].wait_recv()
            sz, sy = zi + dz - 2 * dz * zi, yi + dy - 2 * dy * yi
            at = 4 * xi + 2 * sz + sy
            copy = pltpu.make_async_remote_copy(
                src_ref=gbox.at[cycle, at], dst_ref=gbox.at[cycle, at], send_sem=g_send.at[cycle, 3 + n],
                recv_sem=g_recv.at[cycle, 3 + n], device_id=peers[0], device_id_type=MESH)
            copy.start()
            copies.append(copy)
        copies[0].wait_recv()
        for copy in copies[:4]:
            copy.wait_send()
        for copy in copies[4:]:
            copy.wait()
        for c, a in enumerate((c2r, c2b)):
            gbox[cycle, me, c] = box[cycle, c]

        def unpack_box(i):
            for c, a in enumerate((h2r, h2b)):
                for q in range(4):
                    sz, sy = divmod(q, 2)
                    lo, hi = gbox[cycle, q, c, i], gbox[cycle, 4 + q, c, i]
                    for k in range(4):
                        lower = turn(lo, WIDTH - 32 * k) if k else lo
                        upper = turn(hi, (152 - 32 * k) % WIDTH)
                        v = jnp.where(box_lane < BOX, lower, jnp.where(box_lane < 48, upper, 0.0))
                        a[ZO[2] + 12 * sz + 4 * i + k, YO[2] + BOX * sy:YO[2] + BOX * sy + BOX, :] = v
        loop(3, unpack_box)

    l0 = lvs[0]
    x_u = Columns((u0r, u0b), l0, xs, xr0, 0)
    x_f = Columns((f0r, f0b), l0, xs.at[2:4], xr0.at[2:4], 2)
    x_u.finish()
    faces = send_faces(((u0r, 2, 4), (u0b, 3, 5)), l0, 0)
    x_f.finish()
    faces += send_faces(((f0r, 2, 4),), l0, 6)
    send_faces(((f0b, 2, 3),), l0, 9)
    for ref in (u1r, u1b, u2r, u2b, h2r, h2b, u3r, u3b, h3r, h3b, u4r, u4b, h4r, h4b, u5r, u5b, h5r, h5b,
                d0, d1, d2, d3, d4, cx0, cx1, cx2, cx3, cx4, t0, t1, t2, t3, t4):
        clear_all((ref,))
    for copy in faces:
        copy.wait()

    def v_cycle(cycle):
        h1 = (h1r.at[cycle], h1b.at[cycle])
        hs = ((f0r, f0b), h1, (h2r, h2b), (h3r, h3b), (h4r, h4b), (h5r, h5b))
        l1 = lvs[1]
        relax(us[0], (f0r, f0b), near, 0)

        @pl.when(cycle == 0)
        def black_source_arrived():
            for copy in send_faces(((f0b, 2, 3),), l0, 9, False):
                copy.wait()
        relax(us[0], (f0r, f0b), near, 1)
        relax(us[0], (f0r, f0b), near, 0)
        relax(us[0], (f0r, f0b), near, 1, ts[0])
        restrict(us[0], (f0r, f0b), near, ts[0], h1, (ZO[1], YO[1]))
        Columns(h1, l1, xs1, xr2.at[cycle], TILE).finish()
        faces = Faces(h1, l1, cycle)
        Columns(us[0], l0, xs, xr1.at[cycle], 4).finish()
        faces.finish()
        for level in range(1, 5):
            lv = lvs[level]
            zero_start(us[level], hs[level], lv)
            u, h = us[level], hs[level]
            relax(u, h, lv, 1)
            relax(u, h, lv, 0)
            relax(u, h, lv, 1, ts[level])
            if level == 1:
                restrict(us[1], h1, l1, ts[1], (c2r, c2b), (0, 0))
                gather_level2(cycle)
                pending = send_faces(((u0r, 4, TILE), (u0b, 5, 9)), l0, 18)

                @pl.when(cycle == 0)
                def deeper_source():
                    send_faces(((f0r, 4, TILE), (f0b, 4, TILE)), l0, 0)
            else:
                restrict(us[level], hs[level], lv, ts[level], hs[level + 1], (ZO[level + 1], YO[level + 1]))
        coarsest(hs[5], us[5], lvs[5], qu, qh)
        for level in range(4, -1, -1):
            lv = lvs[level]
            if level == 0:
                for copy in pending:
                    copy.wait()

                @pl.when(cycle == 0)
                def deeper_source_arrived():
                    for copy in send_faces(((f0r, 4, TILE), (f0b, 4, TILE)), l0, 0, False):
                        copy.wait()
            prolong(us[level], us[level + 1], lv, lvs[level + 1], yi, xi, cxs[level], ds_[level])
            if level:
                loop(2, lambda i, lv=lv, level=level: sweep(us[level], hs[level], lv))

        @pl.when(cycle < CYCLES - 1)
        def wide_sweeps():
            loop(2, lambda i: sweep(us[0], (f0r, f0b), l0))

        @pl.when(cycle == CYCLES - 1)
        def last_sweeps():
            loop(2, lambda i: sweep(us[0], (f0r, f0b), near))
    loop(CYCLES, v_cycle)

    stores = []
    for n in range(BRICK // CHUNK):
        slot = n % SLOTS
        if n >= SLOTS:
            stores[n - SLOTS].wait()

        def unpack(i):
            z = ZO[0] + n * (CHUNK // 2) + i
            r, b = u0r[z, YO[0]:YO[0] + BRICK, 0:BRICK], u0b[z, YO[0]:YO[0] + BRICK, 0:BRICK]
            raw[slot, 2 * i] = jnp.where(odd96, b, r)
            raw[slot, 2 * i + 1] = jnp.where(odd96, r, b)
        loop(CHUNK // 2, unpack)
        copy = pltpu.make_async_copy(raw.at[slot], out_hbm.at[pl.ds(n * CHUNK, CHUNK)], out_sem.at[slot])
        copy.start()
        stores.append(copy)
    for copy in stores[-SLOTS:]:
        copy.wait()


def vmem(*shape):
    return pltpu.VMEM(shape, F32)


def scratch_shapes():
    arr = [vmem(NZ[level], NY[level], WIDTH) for level in range(6)]
    shapes = [arr[0]] * 4 + [arr[1]] * 2 + [vmem(2, NZ[1], NY[1], WIDTH)] * 2
    for level in range(2, 6):
        shapes += [arr[level]] * 4
    shapes += arr[:5]
    for extra in (BOX, 0):
        for level in range(5):
            rows = WINDOW[level] // 2 + extra if extra else -(-WINDOW[level] // XHALO) * XHALO
            shapes.append(vmem(PAIRS[level] + ZHALO[level], rows, WIDTH))
    shapes += [vmem(height, WIDTH) for height in (*WINDOW, WINDOW[0] - TILE)]
    shapes += [vmem(SLOTS, CHUNK, BRICK, BRICK)]
    shapes += [vmem(4, 6, BRICK, WIDTH), vmem(4, 6, BRICK, WIDTH), vmem(2, 2, 6, BRICK, WIDTH)]
    shapes += [vmem(2, 3, 48, WIDTH), vmem(2, 2, 3, 48, WIDTH)]
    for planes, rows in ((BOX, DEEP), (DEEP // 2, ROWS[1]), (DEEP // 2, DEEP)):
        shapes += [vmem(planes, rows, WIDTH), vmem(2, planes, rows, WIDTH)]
    last = LANES[5]
    shapes += [vmem(2, PAIRS[5] + 2, last + 2, 3 * TILE, WIDTH), vmem(2, PAIRS[5], last, TILE, WIDTH)]
    shapes += [vmem(12, BOX, WIDTH), vmem(12, BOX, WIDTH), vmem(2, 2, 3, BOX, WIDTH), vmem(2, TILE, 2, 3, BOX, WIDTH)]
    dma = pltpu.SemaphoreType.DMA
    shapes += [dma((SLOTS,)), dma((SLOTS,)), dma((10,)), dma((10,)), dma((BOX,)), dma((BOX,)), dma((2, 7)), dma((2, 7))]
    return shapes


def solution(mesh):
    spec = P(('batch', 'z'), 'y', 'x')

    def local_solve(source, initial_guess):
        return pl.pallas_call(
            kernel,
            out_shape=jax.ShapeDtypeStruct(source.shape, F32),
            in_specs=[pl.BlockSpec(memory_space=pl.ANY)] * 2,
            out_specs=pl.BlockSpec(memory_space=pl.ANY),
            scratch_shapes=scratch_shapes(),
            compiler_params=pltpu.CompilerParams(collective_id=0, has_side_effects=True, vmem_limit_bytes=67043328),
            name='multigrid',
        )(source, initial_guess)

    return jax.shard_map(local_solve, mesh=mesh, in_specs=(spec, spec), out_specs=spec, check_vma=False)
```

```python
import jax
import jax.numpy as jnp
from jax import lax
from jax.experimental import pallas as pl
from jax.experimental.pallas import tpu as pltpu
from jax.sharding import PartitionSpec as P

N = 192
CYCLES = 2
COARSE_SWEEPS = 24
F32 = jnp.float32
MESH = pl.DeviceIdType.MESH

ROWS = LANES = (96, 48, 48, 24, 12, 6)
PAIRS = tuple(rows // 2 for rows in ROWS)
ZO = (9, 7, 1, 1, 1, 1)
NZ = tuple(pairs + 2 * first for pairs, first in zip(PAIRS, ZO))
YO = (24, 24, 8, 8, 8, 8)
NY = tuple(-(-rows // 8) * 8 + 2 * first for rows, first in zip(ROWS, YO))
ZHALO = (8, 6, 0, 0, 0, 0)
YHALO = (16, 16, 0, 0, 0, 0)
WINDOW = tuple(-(-(rows + halo) // 8) * 8 for rows, halo in zip(ROWS, YHALO))
UNROLL = (14, 15, 24, 12, 6, 3)
CHUNK = 16
SLOTS = 4
WIDTH = 128
TILE = 8
BRICK = 96
BOX = 24
XHALO = 16
DEEP = 12
LAST = 5
HALF = 64


def iotas(shape=(TILE, WIDTH)):
    return lax.broadcasted_iota(jnp.int32, shape, 0), lax.broadcasted_iota(jnp.int32, shape, 1)


class Level:
    def __init__(self, level, zi, yi, xi, m, zhalo, yhalo, unroll):
        self.level = level
        self.unroll = unroll
        self.split = level < 2
        self.pairs, self.rows, self.lanes = PAIRS[level], ROWS[level], LANES[level]
        self.zo, self.yo = ZO[level], YO[level]
        self.planes = self.pairs + zhalo
        self.height = TILE * (-(-(self.rows + yhalo) // TILE))
        self.own_height = TILE * (-(-self.rows // TILE))
        if self.split:
            self.zs = self.zo - zhalo * zi
            self.ys = pl.multiple_of(self.yo - yhalo * yi, TILE)
            self.own_at = pl.multiple_of(yhalo * yi, TILE)
        else:
            self.zs, self.ys, self.own_at = self.zo, self.yo, 0
        self.zi = zi
        self.side = zi.astype(F32)
        self.z_at = self.zo - self.zs
        self.m = m
        self.row = pl.ds(self.ys, self.height)
        lane = lax.broadcasted_iota(jnp.int32, (TILE, WIDTH), 1)
        if self.split:
            self.valid = jnp.logical_or(lane < self.lanes + XHALO * (1 - xi), lane >= WIDTH - XHALO * xi)
            edges = (lane == (self.lanes - 1) * xi,)
        else:
            self.valid = lane < self.lanes
            edges = (lane == 0, lane == self.lanes - 1)
        self.outer = edges[0] if self.split else jnp.logical_or(*edges)
        self.w = jnp.where(self.valid, 1.0 / 6.0, 0.0).astype(F32)[None]
        sub, lane = iotas((self.height, WIDTH))
        if self.split:
            count = ones(lane == (self.lanes - 1) * xi) + ones(sub == (self.height - 1) * yi)
        else:
            count = (ones(lane == 0) + ones(lane == self.lanes - 1)
                     + ones(sub == 0) + ones(sub == self.rows - 1))
        m[...] = count.astype(F32)

    def ghosts(self):
        low, high = (self.zo - 1, self.zo), (self.zo + self.pairs, self.zo + self.pairs - 1)
        if self.split:
            return [tuple(a + (b - a) * self.zi for a, b in zip(low, high))]
        return [low, high]

    def odd(self, height, flip):
        sub, lane = iotas()
        return jnp.broadcast_to((lax.rem(sub + lane, 2) == (0 if flip else 1))[None], (height // TILE, TILE, WIDTH))

    def scaled(self, s):
        if self.rows % TILE and not self.split:
            sub, lane = iotas((self.height, WIDTH))
            inside = jnp.logical_and(sub < self.rows, lane < self.lanes)
            return s * jnp.where(inside, 1.0 / 6.0, 0.0).astype(F32)
        return flat(tiled(s) * self.w)


def turn(v, by):
    return pltpu.roll(v, by, 1)


def pick(v, idx):
    return jnp.take_along_axis(v, idx, axis=1)


def ones(where):
    return jnp.where(where, 1.0, 0.0)


def tiled(v):
    return v.reshape(v.shape[0] // TILE, TILE, WIDTH)


def flat(v):
    return v.reshape(v.shape[0] * TILE, WIDTH)


def choose(mask, a, b):
    return flat(jnp.where(mask, tiled(a), tiled(b)))


def loop(count, body):
    def step(i, carry):
        body(i)
        return carry
    lax.fori_loop(0, count, step, 0)


def unrolled(count, body):
    def step(i, carry):
        body(i)
        return carry
    if count == 1:
        body(0)
    elif count > 1:
        lax.fori_loop(0, count, step, 0, unroll=True)


def grouped(count, group, body):
    if count == group:
        unrolled(group, body)
    else:
        loop(count // group, lambda i: unrolled(group, lambda k: body(i * group + k)))


def ghost_planes(dst, src, lv):
    for to, frm in lv.ghosts():
        dst[to, lv.row, :] = -src[frm, lv.row, :]


def gather_sum(a, b, hb, z, y, height, mask, m):
    row = pl.ds(y, height)
    bc = b[z, row, :]
    s = bc + choose(mask, b[z + 1, row, :], b[z - 1, row, :])
    s = s + (b[z, pl.ds(y - 1, height), :] + b[z, pl.ds(y + 1, height), :])
    s = s + (turn(bc, 1) + turn(bc, WIDTH - 1))
    av = a[z, row, :]
    return s + (hb[z, row, :] - m * av), av


def half_sweep(a, b, hb, lv, colour, sums=None):
    ghost_planes(b, a, lv)
    mask = lv.odd(lv.height, colour)

    def plane(k):
        z = lv.zs + k
        m = lv.m[...]
        s, old = gather_sum(a, b, hb, z, lv.ys, lv.height, mask, m)
        new = lv.scaled(s)
        if sums is not None:
            new = new + lv.scaled(s - 6.0 * new)
        a[z, lv.row, :] = new
        if sums is not None:
            sums[k, 0:lv.height, :] = m * (old - new)
    grouped(lv.planes, lv.unroll, plane)
    if sums is not None:
        for n, (to, frm) in enumerate(lv.ghosts()):
            delta = -(a[frm, lv.row, :] + b[to, lv.row, :])
            up = lv.side if lv.split else float(n)
            k = frm - lv.zs
            sums[k, 0:lv.height, :] = sums[k, 0:lv.height, :] + choose(mask, delta * up, delta * (1.0 - up))


def relax(u, hb, lv, colour, sums=None):
    half_sweep(u[colour], u[1 - colour], hb[colour], lv, colour, sums)


def sweep(u, hb, lv):
    relax(u, hb, lv, 0)
    relax(u, hb, lv, 1)


def zero_start(u, hb, lv):
    def clear(i):
        u[1][i] = jnp.zeros(u[1].shape[1:], F32)
    loop(u[1].shape[0], clear)

    def plane(k):
        u[0][lv.zs + k, lv.row, :] = lv.scaled(hb[0][lv.zs + k, lv.row, :])
    grouped(lv.planes, lv.unroll, plane)


def restrict(u, hb, lv, sums, coarse, coarse_at):
    height = lv.own_height
    own = pl.ds(lv.own_at, height)
    ghost_planes(u[1], u[0], lv)
    mask = lv.odd(height, 0)

    def plane(k):
        s, v = gather_sum(u[0], u[1], hb[0], lv.zo + k, lv.yo, height, mask, lv.m[own, :])
        sums[lv.z_at + k, own, :] = sums[lv.z_at + k, own, :] + (s - 6.0 * v)
    grouped(lv.pairs, min(12, lv.pairs), plane)

    half = lv.lanes // 2
    rows = TILE * (-(-(lv.rows // 2) // TILE))
    sub, lane = iotas((rows, WIDTH))
    even_idx = jnp.minimum(2 * lane, 126)
    odd_idx = even_idx + 1
    scale = jnp.where(iotas()[1] < half, 0.5, 0.0).astype(F32)[None]
    mask = lv.odd(rows, 0)
    zc, yc = coarse_at

    def fold(pair):
        c = []
        for s in range(2):
            z = lv.z_at + 2 * pair + s
            v = sums[z, pl.ds(lv.own_at, rows, stride=2), :] + sums[z, pl.ds(lv.own_at + 1, rows, stride=2), :]
            v = pick(v, even_idx) + pick(v, odd_idx)
            c.append(flat(tiled(v) * scale))
        coarse[0][zc + pair, pl.ds(yc, rows), :] = choose(mask, c[1], c[0])
        coarse[1][zc + pair, pl.ds(yc, rows), :] = choose(mask, c[0], c[1])
    grouped(lv.pairs // 2, min(6, lv.pairs // 2), fold)


def prolong(u, e, lv, lc, yi, xi, cx, d):
    planes = lv.planes
    crows = (lv.rows + YHALO[lv.level]) // 2
    height = TILE * (-(-crows // TILE))
    if lv.level == 0:
        zc, yc, off = lc.zo - (ZHALO[0] // 2) * lv.zi, lc.yo - (YHALO[0] // 2) * yi, 0
    elif lv.level == 1:
        zc = lc.zo + (PAIRS[2] - planes // 2) * lv.zi
        yc = lc.yo + (ROWS[2] - crows) * yi
        off = (LANES[1] // 2) * xi
    else:
        zc, yc, off = lc.zo, lc.yo, 0
    if lv.split:
        yc = pl.multiple_of(yc, TILE)
    sub, lane = iotas((height, WIDTH))
    fine_lane = jnp.where(lane < 112, lane, lane - WIDTH) if lv.split else lane
    near = lax.div(fine_lane + WIDTH, 2) - 64
    far = near + jnp.where(lax.rem(lane, 2) == 1, 1, -1)
    if lv.split:
        far = jnp.where(lane == (lv.lanes - 1) * xi, near, far)
    else:
        far = jnp.where(jnp.logical_or(lane == 0, lane == lv.lanes - 1), near, far)
    idx_near = lax.rem(near + off + WIDTH, WIDTH)
    idx_far = lax.rem(far + off + WIDTH, WIDTH)
    w_near = jnp.where(lv.valid, 0.75, 0.0).astype(F32)[None]
    w_far = jnp.where(lv.valid, jnp.where(lv.outer, -0.25, 0.25), 0.0).astype(F32)[None]
    mask = lv.odd(height, 0)

    def along_x(pair):
        r, b = e[0][zc + pair, pl.ds(yc, height), :], e[1][zc + pair, pl.ds(yc, height), :]
        for s in range(2):
            c = choose(mask, b, r) if s == 0 else choose(mask, r, b)
            c = (tiled(pick(c, idx_near)) * w_near
                 + tiled(pick(c, idx_far)) * w_far)
            cx[2 * pair + s, TILE:TILE + height, :] = flat(c)
    pairs = planes // 2
    grouped(pairs, 7 if pairs % 7 == 0 else (5 if pairs % 5 == 0 else min(6, pairs)), along_x)

    if lv.split:
        sides = ((7 + (crows + 1) * yi, TILE + (crows - 1) * yi),)
    else:
        sides = ((7, TILE), (TILE + crows, 7 + crows))

    def edge_rows(z):
        for to, frm in sides:
            cx[z, pl.ds(to, 1), :] = -cx[z, pl.ds(frm, 1), :]
    grouped(planes, 2, edge_rows)

    def along_y(z):
        mid = 0.75 * cx[z, TILE:TILE + height, :]
        d[lv.zs + z, pl.ds(lv.ys, height, stride=2), :] = mid + 0.25 * cx[z, 7:7 + height, :]
        d[lv.zs + z, pl.ds(lv.ys + 1, height, stride=2), :] = mid + 0.25 * cx[z, 9:9 + height, :]
    grouped(planes, 2, along_y)
    ghost_planes(d, d, lv)
    mask = lv.odd(lv.height, 0)

    def along_z(k):
        z = lv.zs + k
        mid = 0.75 * d[z, lv.row, :]
        up, down = 0.25 * d[z + 1, lv.row, :], 0.25 * d[z - 1, lv.row, :]
        r = u[0][z, lv.row, :] + (mid + choose(mask, up, down))
        b = u[1][z, lv.row, :] + (mid + choose(mask, down, up))
        if not lv.split and lv.rows % TILE:
            keep = iotas((lv.height, WIDTH))[0] < lv.rows
            r, b = jnp.where(keep, r, 0.0), jnp.where(keep, b, 0.0)
        u[0][z, lv.row, :] = r
        u[1][z, lv.row, :] = b
    grouped(planes, 2, along_z)


def coarsest(h, u, lv, qu, qh):
    edge = lv.lanes
    box = (edge, TILE, WIDTH)
    x, y, lane = (lax.broadcasted_iota(jnp.int32, box, d) for d in range(3))
    rows = pl.ds(TILE, TILE)
    for c in range(2):
        for k in range(lv.pairs):
            v = h[c][lv.zo + k, rows, :]
            for i in range(edge):
                qh[c, k, i] = pick(v, jnp.full((TILE, WIDTH), i, jnp.int32))
    clear_all((qu,))
    inner = ones(y < edge).astype(F32) / 6.0
    faces = (ones(x == 0) + ones(x == edge - 1) + ones(y == 0) + ones(y == edge - 1)).astype(F32)
    own = pl.ds(1, edge)

    def sweeps(_):
        for c in range(2):
            up = lax.rem(x + y + c, 2) == 1
            up_f = ones(up).astype(F32)
            for k in range(lv.pairs):
                m = faces
                if k == 0:
                    m = m + (1.0 - up_f)
                if k == lv.pairs - 1:
                    m = m + up_f
                z = k + 1
                b, a = qu.at[1 - c], qu.at[c]
                s = b[z, own, rows, :] + jnp.where(up, b[z + 1, own, rows, :], b[z - 1, own, rows, :])
                s = s + (b[z, own, pl.ds(TILE - 1, TILE), :] + b[z, own, pl.ds(TILE + 1, TILE), :])
                s = s + (b[z, pl.ds(0, edge), rows, :] + b[z, pl.ds(2, edge), rows, :])
                a[z, own, rows, :] = (s + (qh[c, k] - m * a[z, own, rows, :])) * inner
    loop(COARSE_SWEEPS, sweeps)
    for c in range(2):
        for k in range(lv.pairs):
            v = qu[c, k + 1, own, rows, :]
            total = jnp.where(lane[0] == 0, v[0], 0.0)
            for i in range(1, edge):
                total = jnp.where(lane[0] == i, v[i], total)
            u[c][lv.zo + k, rows, :] = total


def clear_all(refs):
    for ref in refs:
        def clear(i, ref=ref):
            ref[i] = jnp.zeros(ref.shape[1:], F32)
        loop(ref.shape[0], clear)


def kernel(f_hbm, u_hbm, out_hbm, *scratch):
    (u0r, u0b, f0r, f0b, u1r, u1b, h1r, h1b, u2r, u2b, h2r, h2b, u3r, u3b, h3r, h3b, u4r, u4b, h4r, h4b,
     u5r, u5b, h5r, h5b, d0, d1, d2, d3, d4, cx0, cx1, cx2, cx3, cx4, t0, t1, t2, t3, t4,
     m0, m1, m2, m3, m4, m5, m6, raw, xs, xr0, xr1, xs1, xr2, ys, yr, zs, zr, es, er, qu, qh, c2r, c2b, box, gbox,
     in_sem, out_sem, x_send, x_recv, send, recv, g_send, g_recv) = scratch
    zi, yi, xi = lax.axis_index('z'), lax.axis_index('y'), lax.axis_index('x')
    nx, ny, nz = 1 - xi, 1 - yi, 1 - zi
    peers = ({'x': nx}, {'y': ny}, {'z': nz}, {'z': nz, 'y': ny})

    chunks = [(src, c) for src in (u_hbm, f_hbm) for c in range(BRICK // CHUNK)]

    def load(n):
        src, c = chunks[n]
        return pltpu.make_async_copy(src.at[pl.ds(c * CHUNK, CHUNK)], raw.at[n % SLOTS], in_sem.at[n % SLOTS])
    for n in range(SLOTS):
        load(n).start()

    for ref in (u0r, u0b, f0r, f0b):
        clear_all((ref,))
    for ref in (h1r.at[0], h1b.at[0], h1r.at[1], h1b.at[1]):
        clear_all((ref,))

    barrier = pltpu.get_barrier_semaphore()
    for peer in peers:
        pl.semaphore_signal(barrier, inc=1, device_id=peer, device_id_type=MESH)

    sub, lane = iotas((BRICK, BRICK))
    odd96 = lax.rem(sub + lane, 2) == 1
    h_sq = (1.0 / N) ** 2
    for n in range(len(chunks)):
        load(n).wait()
        slot = n % SLOTS
        first = n < len(chunks) // 2
        red, black = (u0r, u0b) if first else (f0r, f0b)
        half = CHUNK // 2
        start = ZO[0] + (n % (BRICK // CHUNK)) * half

        def pack(i):
            p0, p1 = raw[slot, 2 * i], raw[slot, 2 * i + 1]
            r, b = jnp.where(odd96, p1, p0), jnp.where(odd96, p0, p1)
            if not first:
                r, b = r * h_sq, b * h_sq
            red[start + i, YO[0]:YO[0] + BRICK, :BRICK] = r
            black[start + i, YO[0]:YO[0] + BRICK, :BRICK] = b
        loop(half, pack)
        if n + SLOTS < len(chunks):
            load(n + SLOTS).start()
    pl.semaphore_wait(barrier, len(peers))

    lvs = [Level(level, zi, yi, xi, m, ZHALO[level], YHALO[level], UNROLL[level])
           for level, m in enumerate((m0, m1, m2, m3, m4, m5))]
    near = Level(0, zi, yi, xi, m6, 4, TILE, 13)
    us = ((u0r, u0b), (u1r, u1b), (u2r, u2b), (u3r, u3b), (u4r, u4b), (u5r, u5b))
    ds_ = (d0, d1, d2, d3, d4)
    cxs = (cx0, cx1, cx2, cx3, cx4)
    ts = (t0, t1, t2, t3, t4)

    box_lane = lax.broadcasted_iota(jnp.int32, (BOX, WIDTH), 1)
    quarter = lax.div(box_lane, 32)

    class Columns:
        def __init__(self, arrays, lv, s_buf, r_buf, sem_at):
            self.arrays, self.lv, self.r_buf = arrays, lv, r_buf
            self.wide = lax.broadcasted_iota(jnp.int32, (lv.rows, WIDTH), 1)
            self.row = pl.ds(lv.yo, lv.rows)
            group = lax.div(self.wide, XHALO)
            from_lane = (lv.lanes - XHALO) * nx
            self.copies = []
            for n, a in enumerate(arrays):
                def pack_x(i, a=a, n=n):
                    acc = None
                    for k in range(TILE):
                        v = turn(a[lv.zo + TILE * i + k, self.row, :], lax.rem(XHALO * k + WIDTH - from_lane, WIDTH))
                        acc = v if k == 0 else jnp.where(group == k, v, acc)
                    s_buf[n, i] = acc
                loop(lv.pairs // TILE, pack_x)
                at = sem_at + n
                copy = pltpu.make_async_remote_copy(
                    src_ref=s_buf.at[n], dst_ref=r_buf.at[n], send_sem=x_send.at[at], recv_sem=x_recv.at[at],
                    device_id=peers[0], device_id_type=MESH)
                copy.start()
                self.copies.append(copy)

        def finish(self):
            lv, row = self.lv, self.row
            to_lane = lv.lanes + (112 - lv.lanes) * xi
            inside = jnp.logical_and(self.wide >= to_lane, self.wide < to_lane + XHALO)
            for n, a in enumerate(self.arrays):
                self.copies[n].wait()

                def unpack_x(i, a=a, n=n):
                    acc = self.r_buf[n, i]
                    for k in range(TILE):
                        z = lv.zo + TILE * i + k
                        v = turn(acc, lax.rem(to_lane + WIDTH - XHALO * k, WIDTH))
                        a[z, row, :] = jnp.where(inside, v, a[z, row, :])
                loop(lv.pairs // TILE, unpack_x)

    def send_faces(specs, lv, sem_at, start=True):
        copies = []
        def layers(first, count, size, skip, high):
            inside = first + skip + (count - size - 2 * skip) * (1 - high)
            outside = first - skip - size + (count + size + 2 * skip) * high
            return pl.ds(inside, size), pl.ds(outside, size)

        for a, zn, yn, *there in specs:
            z_skip, y_skip = there or (0, 0)
            z_own, y_own = pl.ds(lv.zo, lv.pairs), pl.ds(lv.yo, lv.rows)
            y_in, y_to = layers(lv.yo, lv.rows, yn - y_skip, y_skip, yi)
            z_in, z_to = layers(lv.zo, lv.pairs, zn - z_skip, z_skip, zi)
            y_all, z_all = layers(lv.yo, lv.rows, yn, 0, yi), layers(lv.zo, lv.pairs, zn, 0, zi)
            parts = (
                ((z_own, y_in), (z_own, y_to), peers[1]),
                ((z_in, y_own), (z_to, y_own), peers[2]),
                ((z_all[0], y_all[0]), (z_all[1], y_all[1]), peers[3]),
            )
            for src, dst, peer in parts:
                at = sem_at + len(copies)
                copy = pltpu.make_async_remote_copy(
                    src_ref=a.at[src[0], src[1]], dst_ref=a.at[dst[0], dst[1]], send_sem=send.at[at], recv_sem=recv.at[at],
                    device_id=peer, device_id_type=MESH)
                if start:
                    copy.start()
                copies.append(copy)
        return copies

    class Faces:
        def __init__(self, h, lv, cycle):
            self.h, self.cycle = h, cycle
            thick = DEEP // 2
            y_in, z_in = lv.yo + (lv.rows - DEEP) * ny, lv.zo + (lv.pairs - thick) * nz
            y_to, z_to = lv.yo + lv.rows - (lv.rows + DEEP) * yi, lv.zo + lv.pairs - (lv.pairs + thick) * zi
            self.parts = ((ys, yr, lv.zo, lv.pairs, y_in, DEEP, lv.zo, y_to),
                          (zs, zr, z_in, thick, lv.yo, lv.rows, z_to, lv.yo),
                          (es, er, z_in, thick, y_in, DEEP, z_to, y_to))
            self.copies = []
            for n, (out, into, z, planes, y, rows, _, _) in enumerate(self.parts):
                lane = lax.broadcasted_iota(jnp.int32, (rows, WIDTH), 1)

                def pack(i):
                    r, b = (colour[z + i, pl.ds(y, rows), :] for colour in h)
                    out[i] = jnp.where(lane < HALF, turn(r, XHALO * xi), turn(b, XHALO * xi + HALF))
                grouped(planes, 6, pack)
                at = 12 + n
                copy = pltpu.make_async_remote_copy(
                    src_ref=out, dst_ref=into.at[cycle], send_sem=send.at[at], recv_sem=recv.at[at],
                    device_id=peers[n + 1], device_id_type=MESH)
                copy.start()
                self.copies.append(copy)

        def finish(self):
            for copy, (_, into, _, planes, _, rows, z, y) in zip(self.copies, self.parts):
                copy.wait()
                lane = lax.broadcasted_iota(jnp.int32, (rows, WIDTH), 1)
                valid = jnp.logical_or(lane < HALF - XHALO * xi, lane >= WIDTH - XHALO * xi)

                def unpack(i):
                    v = into[self.cycle, i]
                    for c in range(2):
                        w = turn(v, lax.rem(WIDTH - HALF * c - XHALO * xi, WIDTH))
                        self.h[c][z + i, pl.ds(y, rows), :] = jnp.where(valid, w, 0.0)
                grouped(planes, 6, unpack)

    def gather_level2(cycle):
        def pack_box(i):
            for c, a in enumerate((c2r, c2b)):
                acc = a[4 * i]
                for k in range(1, 4):
                    acc = jnp.where(quarter == k, turn(a[4 * i + k], 32 * k), acc)
                box[cycle, c, i] = acc
        loop(3, pack_box)
        me = 4 * xi + 2 * zi + yi
        copies = []
        for n, peer in enumerate(peers):
            copy = pltpu.make_async_remote_copy(
                src_ref=box.at[cycle], dst_ref=gbox.at[cycle, me], send_sem=g_send.at[cycle, n], recv_sem=g_recv.at[cycle, n],
                device_id=peer, device_id_type=MESH)
            copy.start()
            copies.append(copy)
        for n in range(1, len(peers)):
            dz, dy = divmod(n, 2)
            copies[n].wait_recv()
            sz, sy = zi + dz - 2 * dz * zi, yi + dy - 2 * dy * yi
            at = 4 * xi + 2 * sz + sy
            copy = pltpu.make_async_remote_copy(
                src_ref=gbox.at[cycle, at], dst_ref=gbox.at[cycle, at], send_sem=g_send.at[cycle, 3 + n],
                recv_sem=g_recv.at[cycle, 3 + n], device_id=peers[0], device_id_type=MESH)
            copy.start()
            copies.append(copy)
        copies[0].wait_recv()
        for copy in copies[:4]:
            copy.wait_send()
        for copy in copies[4:]:
            copy.wait()
        for c, a in enumerate((c2r, c2b)):
            gbox[cycle, me, c] = box[cycle, c]

        def unpack_box(i):
            for c, a in enumerate((h2r, h2b)):
                for q in range(4):
                    sz, sy = divmod(q, 2)
                    lo, hi = gbox[cycle, q, c, i], gbox[cycle, 4 + q, c, i]
                    for k in range(4):
                        lower = turn(lo, WIDTH - 32 * k) if k else lo
                        upper = turn(hi, (152 - 32 * k) % WIDTH)
                        v = jnp.where(box_lane < BOX, lower, jnp.where(box_lane < 48, upper, 0.0))
                        a[ZO[2] + 12 * sz + 4 * i + k, YO[2] + BOX * sy:YO[2] + BOX * sy + BOX, :] = v
        loop(3, unpack_box)

    l0 = lvs[0]
    x_u = Columns((u0r, u0b), l0, xs, xr0, 0)
    x_f = Columns((f0r, f0b), l0, xs.at[2:4], xr0.at[2:4], 2)
    x_u.finish()
    faces = send_faces(((u0r, 2, 4), (u0b, 3, 5)), l0, 0)
    x_f.finish()
    faces += send_faces(((f0r, 2, 4),), l0, 6)
    send_faces(((f0b, 2, 3),), l0, 9)
    for ref in (u1r, u1b, u2r, u2b, h2r, h2b, u3r, u3b, h3r, h3b, u4r, u4b, h4r, h4b, u5r, u5b, h5r, h5b,
                d0, d1, d2, d3, d4, cx0, cx1, cx2, cx3, cx4, t0, t1, t2, t3, t4):
        clear_all((ref,))
    for copy in faces:
        copy.wait()

    deeper = ((f0r, 4, TILE, 2, 4), (f0b, 4, TILE, 2, 3))

    def v_cycle(cycle):
        h1 = (h1r.at[cycle], h1b.at[cycle])
        hs = ((f0r, f0b), h1, (h2r, h2b), (h3r, h3b), (h4r, h4b), (h5r, h5b))
        l1 = lvs[1]
        relax(us[0], (f0r, f0b), near, 0)

        @pl.when(cycle == 0)
        def black_source_arrived():
            for copy in send_faces(((f0b, 2, 3),), l0, 9, False):
                copy.wait()
        relax(us[0], (f0r, f0b), near, 1)
        relax(us[0], (f0r, f0b), near, 0)
        relax(us[0], (f0r, f0b), near, 1, ts[0])
        restrict(us[0], (f0r, f0b), near, ts[0], h1, (ZO[1], YO[1]))
        Columns(h1, l1, xs1, xr2.at[cycle], TILE).finish()
        faces = Faces(h1, l1, cycle)
        Columns(us[0], l0, xs, xr1.at[cycle], 4).finish()
        faces.finish()

        @pl.when(cycle == 0)
        def deeper_source():
            send_faces(deeper, l0, 0)
        for level in range(1, LAST):
            lv = lvs[level]
            zero_start(us[level], hs[level], lv)
            u, h = us[level], hs[level]
            relax(u, h, lv, 1)
            relax(u, h, lv, 0)
            relax(u, h, lv, 1, ts[level])
            if level == 1:
                restrict(u, h, lv, ts[level], (c2r, c2b), (0, 0))
                gather_level2(cycle)
                pending = send_faces(((u0r, 4, TILE), (u0b, 5, 9)), l0, 18)

            else:
                lower = level + 1
                restrict(u, h, lv, ts[level], hs[lower], (ZO[lower], YO[lower]))
        coarsest(hs[LAST], us[LAST], lvs[LAST], qu, qh)
        for level in range(4, -1, -1):
            lv = lvs[level]
            if level == 0:
                for copy in pending:
                    copy.wait()

                @pl.when(cycle == 0)
                def deeper_source_arrived():
                    for copy in send_faces(deeper, l0, 0, False):
                        copy.wait()
            prolong(us[level], us[level + 1], lv, lvs[level + 1], yi, xi, cxs[level], ds_[level])
            if level:
                loop(2, lambda i, lv=lv, level=level: sweep(us[level], hs[level], lv))

        @pl.when(cycle < CYCLES - 1)
        def wide_sweeps():
            loop(2, lambda i: sweep(us[0], (f0r, f0b), l0))

        @pl.when(cycle == CYCLES - 1)
        def last_sweeps():
            loop(2, lambda i: sweep(us[0], (f0r, f0b), near))
    loop(CYCLES, v_cycle)

    stores = []
    for n in range(BRICK // CHUNK):
        slot = n % SLOTS
        if n >= SLOTS:
            stores[n - SLOTS].wait()

        def unpack(i):
            z = l0.zo + n * half + i
            r, b = (colour[z, YO[0]:YO[0] + BRICK, :BRICK] for colour in us[0])
            raw[slot, 2 * i] = jnp.where(odd96, b, r)
            raw[slot, 2 * i + 1] = jnp.where(odd96, r, b)
        loop(half, unpack)
        copy = pltpu.make_async_copy(raw.at[slot], out_hbm.at[pl.ds(n * CHUNK, CHUNK)], out_sem.at[slot])
        copy.start()
        stores.append(copy)
    for copy in stores[-SLOTS:]:
        copy.wait()


def vmem(*shape):
    return pltpu.VMEM(shape, F32)


def scratch_shapes():
    arr = [vmem(NZ[level], NY[level], WIDTH) for level in range(6)]
    shapes = [arr[0]] * 4 + [arr[1]] * 2 + [vmem(2, NZ[1], NY[1], WIDTH)] * 2
    for level in range(2, 6):
        shapes += [arr[level]] * 4
    shapes += arr[:5]
    for extra in (BOX, 0):
        for level in range(LAST):
            rows = WINDOW[level] // 2 + extra if extra else -(-WINDOW[level] // XHALO) * XHALO
            shapes.append(vmem(PAIRS[level] + ZHALO[level], rows, WIDTH))
    shapes += [vmem(height, WIDTH) for height in (*WINDOW, WINDOW[0] - TILE)]
    shapes += [vmem(SLOTS, CHUNK, BRICK, BRICK)]
    shapes += [vmem(4, 6, BRICK, WIDTH), vmem(4, 6, BRICK, WIDTH), vmem(2, 2, 6, BRICK, WIDTH)]
    shapes += [vmem(2, 3, 48, WIDTH), vmem(2, 2, 3, 48, WIDTH)]
    for planes, rows in ((BOX, DEEP), (DEEP // 2, ROWS[1]), (DEEP // 2, DEEP)):
        shapes += [vmem(planes, rows, WIDTH), vmem(2, planes, rows, WIDTH)]
    last = LANES[LAST]
    shapes += [vmem(2, PAIRS[LAST] + 2, last + 2, 3 * TILE, WIDTH), vmem(2, PAIRS[LAST], last, TILE, WIDTH)]
    shapes += [vmem(12, BOX, WIDTH), vmem(12, BOX, WIDTH), vmem(2, 2, 3, BOX, WIDTH), vmem(2, TILE, 2, 3, BOX, WIDTH)]
    dma = pltpu.SemaphoreType.DMA
    for shape in ((SLOTS,), (10,), (BOX,), (2, 7)):
        shapes += [dma(shape), dma(shape)]
    return shapes


def solution(mesh):
    spec = P(('batch', 'z'), 'y', 'x')

    def local_solve(source, initial_guess):
        return pl.pallas_call(
            kernel,
            out_shape=jax.ShapeDtypeStruct(source.shape, F32),
            in_specs=[pl.BlockSpec(memory_space=pl.ANY)] * 2,
            out_specs=pl.BlockSpec(memory_space=pl.ANY),
            scratch_shapes=scratch_shapes(),
            compiler_params=pltpu.CompilerParams(collective_id=0, has_side_effects=True, vmem_limit_bytes=67043328),
            name='multigrid',
        )(source, initial_guess)

    return jax.shard_map(local_solve, mesh=mesh, in_specs=(spec, spec), out_specs=spec, check_vma=False)
```

```python
import jax
import jax.numpy as jnp
from jax import lax
from jax.experimental import pallas as pl
from jax.experimental.pallas import tpu as pltpu
from jax.sharding import PartitionSpec as P

N = 192
CYCLES = 2
COARSE_SWEEPS = 24
F32 = jnp.float32
MESH = pl.DeviceIdType.MESH

ROWS = LANES = (96, 48, 48, 24, 12, 6)
PAIRS = tuple(rows // 2 for rows in ROWS)
ZO = (9, 7, 1, 1, 1, 1)
NZ = tuple(pairs + 2 * first for pairs, first in zip(PAIRS, ZO))
YO = (24, 24, 8, 8, 8, 8)
NY = tuple(-(-rows // 8) * 8 + 2 * first for rows, first in zip(ROWS, YO))
ZHALO = (8, 6, 0, 0, 0, 0)
YHALO = (16, 16, 0, 0, 0, 0)
WINDOW = tuple(-(-(rows + halo) // 8) * 8 for rows, halo in zip(ROWS, YHALO))
UNROLL = (14, 15, 24, 12, 6, 3)
CHUNK = 16
SLOTS = 4
WIDTH = 128
TILE = 8
BRICK = 96
BOX = 24
XHALO = 16
DEEP = 12
LAST = 5
HALF = 64


def iotas(shape=(TILE, WIDTH)):
    return lax.broadcasted_iota(jnp.int32, shape, 0), lax.broadcasted_iota(jnp.int32, shape, 1)


class Level:
    def __init__(self, level, zi, yi, xi, m, zhalo, yhalo, unroll):
        self.level = level
        self.unroll = unroll
        self.split = level < 2
        self.pairs, self.rows, self.lanes = PAIRS[level], ROWS[level], LANES[level]
        self.zo, self.yo = ZO[level], YO[level]
        self.planes = self.pairs + zhalo
        self.height = TILE * (-(-(self.rows + yhalo) // TILE))
        self.own_height = TILE * (-(-self.rows // TILE))
        if self.split:
            self.zs = self.zo - zhalo * zi
            self.ys = pl.multiple_of(self.yo - yhalo * yi, TILE)
            self.own_at = pl.multiple_of(yhalo * yi, TILE)
        else:
            self.zs, self.ys, self.own_at = self.zo, self.yo, 0
        self.zi = zi
        self.side = zi.astype(F32)
        self.z_at = self.zo - self.zs
        self.m = m
        self.row = pl.ds(self.ys, self.height)
        lane = lax.broadcasted_iota(jnp.int32, (TILE, WIDTH), 1)
        if self.split:
            self.valid = jnp.logical_or(lane < self.lanes + XHALO * (1 - xi), lane >= WIDTH - XHALO * xi)
            edges = (lane == (self.lanes - 1) * xi,)
        else:
            self.valid = lane < self.lanes
            edges = (lane == 0, lane == self.lanes - 1)
        self.outer = edges[0] if self.split else jnp.logical_or(*edges)
        self.w = jnp.where(self.valid, 1.0 / 6.0, 0.0).astype(F32)[None]
        sub, lane = iotas((self.height, WIDTH))
        if self.split:
            count = ones(lane == (self.lanes - 1) * xi) + ones(sub == (self.height - 1) * yi)
        else:
            count = (ones(lane == 0) + ones(lane == self.lanes - 1)
                     + ones(sub == 0) + ones(sub == self.rows - 1))
        m[...] = count.astype(F32)

    def ghosts(self):
        low, high = (self.zo - 1, self.zo), (self.zo + self.pairs, self.zo + self.pairs - 1)
        if self.split:
            return [tuple(a + (b - a) * self.zi for a, b in zip(low, high))]
        return [low, high]

    def odd(self, height, flip):
        sub, lane = iotas()
        return jnp.broadcast_to((lax.rem(sub + lane, 2) == (0 if flip else 1))[None], (height // TILE, TILE, WIDTH))

    def scaled(self, s):
        if self.rows % TILE and not self.split:
            sub, lane = iotas((self.height, WIDTH))
            inside = jnp.logical_and(sub < self.rows, lane < self.lanes)
            return s * jnp.where(inside, 1.0 / 6.0, 0.0).astype(F32)
        return flat(tiled(s) * self.w)


def turn(v, by):
    return pltpu.roll(v, by, 1)


def pick(v, idx):
    return jnp.take_along_axis(v, idx, axis=1)


def ones(where):
    return jnp.where(where, 1.0, 0.0)


def tiled(v):
    return v.reshape(v.shape[0] // TILE, TILE, WIDTH)


def flat(v):
    return v.reshape(v.shape[0] * TILE, WIDTH)


def choose(mask, a, b):
    return flat(jnp.where(mask, tiled(a), tiled(b)))


def loop(count, body):
    def step(i, carry):
        body(i)
        return carry
    lax.fori_loop(0, count, step, 0)


def unrolled(count, body):
    def step(i, carry):
        body(i)
        return carry
    if count == 1:
        body(0)
    elif count > 1:
        lax.fori_loop(0, count, step, 0, unroll=True)


def grouped(count, group, body):
    if count == group:
        unrolled(group, body)
    else:
        loop(count // group, lambda i: unrolled(group, lambda k: body(i * group + k)))


def ghost_planes(dst, src, lv):
    for to, frm in lv.ghosts():
        dst[to, lv.row, :] = -src[frm, lv.row, :]


def gather_sum(a, b, hb, z, y, height, mask, m):
    row = pl.ds(y, height)
    bc = b[z, row, :]
    s = bc + choose(mask, b[z + 1, row, :], b[z - 1, row, :])
    s = s + (b[z, pl.ds(y - 1, height), :] + b[z, pl.ds(y + 1, height), :])
    s = s + (turn(bc, 1) + turn(bc, WIDTH - 1))
    av = a[z, row, :]
    return s + (hb[z, row, :] - m * av), av


def half_sweep(a, b, hb, lv, colour, sums=None):
    ghost_planes(b, a, lv)
    mask = lv.odd(lv.height, colour)

    def plane(k):
        z = lv.zs + k
        m = lv.m[...]
        s, old = gather_sum(a, b, hb, z, lv.ys, lv.height, mask, m)
        new = lv.scaled(s)
        if sums is not None:
            new = new + lv.scaled(s - 6.0 * new)
        a[z, lv.row, :] = new
        if sums is not None:
            sums[k, 0:lv.height, :] = m * (old - new)
    grouped(lv.planes, lv.unroll, plane)
    if sums is not None:
        for n, (to, frm) in enumerate(lv.ghosts()):
            delta = -(a[frm, lv.row, :] + b[to, lv.row, :])
            up = lv.side if lv.split else float(n)
            k = frm - lv.zs
            sums[k, 0:lv.height, :] = sums[k, 0:lv.height, :] + choose(mask, delta * up, delta * (1.0 - up))


def relax(u, hb, lv, colour, sums=None):
    half_sweep(u[colour], u[1 - colour], hb[colour], lv, colour, sums)


def sweep(u, hb, lv):
    relax(u, hb, lv, 0)
    relax(u, hb, lv, 1)


def zero_start(u, hb, lv):
    def clear(i):
        u[1][i] = jnp.zeros(u[1].shape[1:], F32)
    loop(u[1].shape[0], clear)

    def plane(k):
        u[0][lv.zs + k, lv.row, :] = lv.scaled(hb[0][lv.zs + k, lv.row, :])
    grouped(lv.planes, lv.unroll, plane)


def restrict(u, hb, lv, sums, coarse, coarse_at):
    height = lv.own_height
    own = pl.ds(lv.own_at, height)
    ghost_planes(u[1], u[0], lv)
    mask = lv.odd(height, 0)

    def plane(k):
        s, v = gather_sum(u[0], u[1], hb[0], lv.zo + k, lv.yo, height, mask, lv.m[own, :])
        sums[lv.z_at + k, own, :] = sums[lv.z_at + k, own, :] + (s - 6.0 * v)
    grouped(lv.pairs, min(12, lv.pairs), plane)

    half = lv.lanes // 2
    rows = TILE * (-(-(lv.rows // 2) // TILE))
    sub, lane = iotas((rows, WIDTH))
    even_idx = jnp.minimum(2 * lane, 126)
    odd_idx = even_idx + 1
    scale = jnp.where(iotas()[1] < half, 0.5, 0.0).astype(F32)[None]
    mask = lv.odd(rows, 0)
    zc, yc = coarse_at

    def fold(pair):
        c = []
        for s in range(2):
            z = lv.z_at + 2 * pair + s
            v = sums[z, pl.ds(lv.own_at, rows, stride=2), :] + sums[z, pl.ds(lv.own_at + 1, rows, stride=2), :]
            v = pick(v, even_idx) + pick(v, odd_idx)
            c.append(flat(tiled(v) * scale))
        coarse[0][zc + pair, pl.ds(yc, rows), :] = choose(mask, c[1], c[0])
        coarse[1][zc + pair, pl.ds(yc, rows), :] = choose(mask, c[0], c[1])
    grouped(lv.pairs // 2, min(6, lv.pairs // 2), fold)


def prolong(u, e, lv, lc, yi, xi, cx, d):
    planes = lv.planes
    crows = (lv.rows + YHALO[lv.level]) // 2
    height = TILE * (-(-crows // TILE))
    if lv.level == 0:
        zc, yc, off = lc.zo - (ZHALO[0] // 2) * lv.zi, lc.yo - (YHALO[0] // 2) * yi, 0
    elif lv.level == 1:
        zc = lc.zo + (PAIRS[2] - planes // 2) * lv.zi
        yc = lc.yo + (ROWS[2] - crows) * yi
        off = (LANES[1] // 2) * xi
    else:
        zc, yc, off = lc.zo, lc.yo, 0
    if lv.split:
        yc = pl.multiple_of(yc, TILE)
    sub, lane = iotas((height, WIDTH))
    fine_lane = jnp.where(lane < 112, lane, lane - WIDTH) if lv.split else lane
    near = lax.div(fine_lane + WIDTH, 2) - 64
    far = near + jnp.where(lax.rem(lane, 2) == 1, 1, -1)
    if lv.split:
        far = jnp.where(lane == (lv.lanes - 1) * xi, near, far)
    else:
        far = jnp.where(jnp.logical_or(lane == 0, lane == lv.lanes - 1), near, far)
    idx_near = lax.rem(near + off + WIDTH, WIDTH)
    idx_far = lax.rem(far + off + WIDTH, WIDTH)
    w_near = jnp.where(lv.valid, 0.75, 0.0).astype(F32)[None]
    w_far = jnp.where(lv.valid, jnp.where(lv.outer, -0.25, 0.25), 0.0).astype(F32)[None]
    mask = lv.odd(height, 0)

    def along_x(pair):
        r, b = e[0][zc + pair, pl.ds(yc, height), :], e[1][zc + pair, pl.ds(yc, height), :]
        for s in range(2):
            c = choose(mask, b, r) if s == 0 else choose(mask, r, b)
            c = (tiled(pick(c, idx_near)) * w_near
                 + tiled(pick(c, idx_far)) * w_far)
            cx[2 * pair + s, TILE:TILE + height, :] = flat(c)
    pairs = planes // 2
    grouped(pairs, 7 if pairs % 7 == 0 else (5 if pairs % 5 == 0 else min(6, pairs)), along_x)

    if lv.split:
        sides = ((7 + (crows + 1) * yi, TILE + (crows - 1) * yi),)
    else:
        sides = ((7, TILE), (TILE + crows, 7 + crows))

    def edge_rows(z):
        for to, frm in sides:
            cx[z, pl.ds(to, 1), :] = -cx[z, pl.ds(frm, 1), :]
    grouped(planes, 2, edge_rows)

    def along_y(z):
        mid = 0.75 * cx[z, TILE:TILE + height, :]
        d[lv.zs + z, pl.ds(lv.ys, height, stride=2), :] = mid + 0.25 * cx[z, 7:7 + height, :]
        d[lv.zs + z, pl.ds(lv.ys + 1, height, stride=2), :] = mid + 0.25 * cx[z, 9:9 + height, :]
    grouped(planes, 2, along_y)
    ghost_planes(d, d, lv)
    mask = lv.odd(lv.height, 0)

    def along_z(k):
        z = lv.zs + k
        mid = 0.75 * d[z, lv.row, :]
        up, down = 0.25 * d[z + 1, lv.row, :], 0.25 * d[z - 1, lv.row, :]
        r = u[0][z, lv.row, :] + (mid + choose(mask, up, down))
        b = u[1][z, lv.row, :] + (mid + choose(mask, down, up))
        if not lv.split and lv.rows % TILE:
            keep = iotas((lv.height, WIDTH))[0] < lv.rows
            r, b = jnp.where(keep, r, 0.0), jnp.where(keep, b, 0.0)
        u[0][z, lv.row, :] = r
        u[1][z, lv.row, :] = b
    grouped(planes, 2, along_z)


def coarsest(h, u, lv, qu, qh):
    edge = lv.lanes
    box = (edge, TILE, WIDTH)
    x, y, lane = (lax.broadcasted_iota(jnp.int32, box, d) for d in range(3))
    rows = pl.ds(TILE, TILE)
    for c in range(2):
        for k in range(lv.pairs):
            v = h[c][lv.zo + k, rows, :]
            for i in range(edge):
                qh[c, k, i] = pick(v, jnp.full((TILE, WIDTH), i, jnp.int32))
    clear_all((qu,))
    inner = ones(y < edge).astype(F32) / 6.0
    faces = (ones(x == 0) + ones(x == edge - 1) + ones(y == 0) + ones(y == edge - 1)).astype(F32)
    own = pl.ds(1, edge)

    def sweeps(_):
        for c in range(2):
            up = lax.rem(x + y + c, 2) == 1
            up_f = ones(up).astype(F32)
            for k in range(lv.pairs):
                m = faces
                if k == 0:
                    m = m + (1.0 - up_f)
                if k == lv.pairs - 1:
                    m = m + up_f
                z = k + 1
                b, a = qu.at[1 - c], qu.at[c]
                s = b[z, own, rows, :] + jnp.where(up, b[z + 1, own, rows, :], b[z - 1, own, rows, :])
                s = s + (b[z, own, pl.ds(TILE - 1, TILE), :] + b[z, own, pl.ds(TILE + 1, TILE), :])
                s = s + (b[z, pl.ds(0, edge), rows, :] + b[z, pl.ds(2, edge), rows, :])
                a[z, own, rows, :] = (s + (qh[c, k] - m * a[z, own, rows, :])) * inner
    loop(COARSE_SWEEPS, sweeps)
    for c in range(2):
        for k in range(lv.pairs):
            v = qu[c, k + 1, own, rows, :]
            total = jnp.where(lane[0] == 0, v[0], 0.0)
            for i in range(1, edge):
                total = jnp.where(lane[0] == i, v[i], total)
            u[c][lv.zo + k, rows, :] = total


def clear_all(refs):
    for ref in refs:
        def clear(i, ref=ref):
            ref[i] = jnp.zeros(ref.shape[1:], F32)
        loop(ref.shape[0], clear)


def kernel(f_hbm, u_hbm, out_hbm, *scratch):
    (u0r, u0b, f0r, f0b, u1r, u1b, h1r, h1b, u2r, u2b, h2r, h2b, u3r, u3b, h3r, h3b, u4r, u4b, h4r, h4b,
     u5r, u5b, h5r, h5b, d0, d1, d2, d3, d4, cx0, cx1, cx2, cx3, cx4, t0, t1, t2, t3, t4,
     m0, m1, m2, m3, m4, m5, m6, raw, xs, xr0, xr1, xs1, xr2, ys, yr, zs, zr, es, er, qu, qh, c2r, c2b, box, gbox,
     in_sem, out_sem, x_send, x_recv, send, recv, g_send, g_recv) = scratch
    zi, yi, xi = lax.axis_index('z'), lax.axis_index('y'), lax.axis_index('x')
    nx, ny, nz = 1 - xi, 1 - yi, 1 - zi
    peers = ({'x': nx}, {'y': ny}, {'z': nz}, {'z': nz, 'y': ny})

    chunks = [(src, c) for src in (u_hbm, f_hbm) for c in range(BRICK // CHUNK)]

    def load(n):
        src, c = chunks[n]
        return pltpu.make_async_copy(src.at[pl.ds(c * CHUNK, CHUNK)], raw.at[n % SLOTS], in_sem.at[n % SLOTS])
    for n in range(SLOTS):
        load(n).start()

    for ref in (u0r, u0b, f0r, f0b):
        clear_all((ref,))
    for ref in (h1r.at[0], h1b.at[0], h1r.at[1], h1b.at[1]):
        clear_all((ref,))

    barrier = pltpu.get_barrier_semaphore()
    for peer in peers:
        pl.semaphore_signal(barrier, inc=1, device_id=peer, device_id_type=MESH)

    sub, lane = iotas((BRICK, BRICK))
    odd96 = lax.rem(sub + lane, 2) == 1
    h_sq = (1.0 / N) ** 2
    half = CHUNK // 2

    def ingest(n):
        load(n).wait()
        slot = n % SLOTS
        first = n < len(chunks) // 2
        red, black = (u0r, u0b) if first else (f0r, f0b)
        start = ZO[0] + (n % (BRICK // CHUNK)) * half

        def pack(i):
            p0, p1 = raw[slot, 2 * i], raw[slot, 2 * i + 1]
            r, b = jnp.where(odd96, p1, p0), jnp.where(odd96, p0, p1)
            if not first:
                r, b = r * h_sq, b * h_sq
            red[start + i, YO[0]:YO[0] + BRICK, :BRICK] = r
            black[start + i, YO[0]:YO[0] + BRICK, :BRICK] = b
        loop(half, pack)
        if n + SLOTS < len(chunks):
            load(n + SLOTS).start()

    lvs = [Level(level, zi, yi, xi, m, ZHALO[level], YHALO[level], UNROLL[level])
           for level, m in enumerate((m0, m1, m2, m3, m4, m5))]
    near = Level(0, zi, yi, xi, m6, 4, TILE, 13)
    us = ((u0r, u0b), (u1r, u1b), (u2r, u2b), (u3r, u3b), (u4r, u4b), (u5r, u5b))
    ds_ = (d0, d1, d2, d3, d4)
    cxs = (cx0, cx1, cx2, cx3, cx4)
    ts = (t0, t1, t2, t3, t4)

    box_lane = lax.broadcasted_iota(jnp.int32, (BOX, WIDTH), 1)
    quarter = lax.div(box_lane, 32)

    class Columns:
        def __init__(self, arrays, lv, s_buf, r_buf, sem_at):
            self.arrays, self.lv, self.r_buf = arrays, lv, r_buf
            self.wide = lax.broadcasted_iota(jnp.int32, (lv.rows, WIDTH), 1)
            self.row = pl.ds(lv.yo, lv.rows)
            group = lax.div(self.wide, XHALO)
            from_lane = (lv.lanes - XHALO) * nx
            self.copies = []
            for n, a in enumerate(arrays):
                def pack_x(i, a=a, n=n):
                    acc = None
                    for k in range(TILE):
                        v = turn(a[lv.zo + TILE * i + k, self.row, :], lax.rem(XHALO * k + WIDTH - from_lane, WIDTH))
                        acc = v if k == 0 else jnp.where(group == k, v, acc)
                    s_buf[n, i] = acc
                loop(lv.pairs // TILE, pack_x)
                at = sem_at + n
                copy = pltpu.make_async_remote_copy(
                    src_ref=s_buf.at[n], dst_ref=r_buf.at[n], send_sem=x_send.at[at], recv_sem=x_recv.at[at],
                    device_id=peers[0], device_id_type=MESH)
                copy.start()
                self.copies.append(copy)

        def finish(self):
            lv, row = self.lv, self.row
            to_lane = lv.lanes + (112 - lv.lanes) * xi
            inside = jnp.logical_and(self.wide >= to_lane, self.wide < to_lane + XHALO)
            for n, a in enumerate(self.arrays):
                self.copies[n].wait()

                def unpack_x(i, a=a, n=n):
                    acc = self.r_buf[n, i]
                    for k in range(TILE):
                        z = lv.zo + TILE * i + k
                        v = turn(acc, lax.rem(to_lane + WIDTH - XHALO * k, WIDTH))
                        a[z, row, :] = jnp.where(inside, v, a[z, row, :])
                loop(lv.pairs // TILE, unpack_x)

    def send_faces(specs, lv, sem_at, start=True):
        copies = []
        def layers(first, count, size, skip, high):
            inside = first + skip + (count - size - 2 * skip) * (1 - high)
            outside = first - skip - size + (count + size + 2 * skip) * high
            return pl.ds(inside, size), pl.ds(outside, size)

        for a, zn, yn, *there in specs:
            z_skip, y_skip = there or (0, 0)
            z_own, y_own = pl.ds(lv.zo, lv.pairs), pl.ds(lv.yo, lv.rows)
            y_in, y_to = layers(lv.yo, lv.rows, yn - y_skip, y_skip, yi)
            z_in, z_to = layers(lv.zo, lv.pairs, zn - z_skip, z_skip, zi)
            y_all, z_all = layers(lv.yo, lv.rows, yn, 0, yi), layers(lv.zo, lv.pairs, zn, 0, zi)
            parts = (
                ((z_own, y_in), (z_own, y_to), peers[1]),
                ((z_in, y_own), (z_to, y_own), peers[2]),
                ((z_all[0], y_all[0]), (z_all[1], y_all[1]), peers[3]),
            )
            for src, dst, peer in parts:
                at = sem_at + len(copies)
                copy = pltpu.make_async_remote_copy(
                    src_ref=a.at[src[0], src[1]], dst_ref=a.at[dst[0], dst[1]], send_sem=send.at[at], recv_sem=recv.at[at],
                    device_id=peer, device_id_type=MESH)
                if start:
                    copy.start()
                copies.append(copy)
        return copies

    class Faces:
        def __init__(self, h, lv, cycle):
            self.h, self.cycle = h, cycle
            thick = DEEP // 2
            y_in, z_in = lv.yo + (lv.rows - DEEP) * ny, lv.zo + (lv.pairs - thick) * nz
            y_to, z_to = lv.yo + lv.rows - (lv.rows + DEEP) * yi, lv.zo + lv.pairs - (lv.pairs + thick) * zi
            self.parts = ((ys, yr, lv.zo, lv.pairs, y_in, DEEP, lv.zo, y_to),
                          (zs, zr, z_in, thick, lv.yo, lv.rows, z_to, lv.yo),
                          (es, er, z_in, thick, y_in, DEEP, z_to, y_to))
            self.copies = []
            for n, (out, into, z, planes, y, rows, _, _) in enumerate(self.parts):
                lane = lax.broadcasted_iota(jnp.int32, (rows, WIDTH), 1)

                def pack(i):
                    r, b = (colour[z + i, pl.ds(y, rows), :] for colour in h)
                    out[i] = jnp.where(lane < HALF, turn(r, XHALO * xi), turn(b, XHALO * xi + HALF))
                grouped(planes, 6, pack)
                at = 12 + n
                copy = pltpu.make_async_remote_copy(
                    src_ref=out, dst_ref=into.at[cycle], send_sem=send.at[at], recv_sem=recv.at[at],
                    device_id=peers[n + 1], device_id_type=MESH)
                copy.start()
                self.copies.append(copy)

        def finish(self):
            for copy, (_, into, _, planes, _, rows, z, y) in zip(self.copies, self.parts):
                copy.wait()
                lane = lax.broadcasted_iota(jnp.int32, (rows, WIDTH), 1)
                valid = jnp.logical_or(lane < HALF - XHALO * xi, lane >= WIDTH - XHALO * xi)

                def unpack(i):
                    v = into[self.cycle, i]
                    for c in range(2):
                        w = turn(v, lax.rem(WIDTH - HALF * c - XHALO * xi, WIDTH))
                        self.h[c][z + i, pl.ds(y, rows), :] = jnp.where(valid, w, 0.0)
                grouped(planes, 6, unpack)

    def gather_level2(cycle):
        def pack_box(i):
            for c, a in enumerate((c2r, c2b)):
                acc = a[4 * i]
                for k in range(1, 4):
                    acc = jnp.where(quarter == k, turn(a[4 * i + k], 32 * k), acc)
                box[cycle, c, i] = acc
        loop(3, pack_box)
        me = 4 * xi + 2 * zi + yi
        copies = []
        for n, peer in enumerate(peers):
            copy = pltpu.make_async_remote_copy(
                src_ref=box.at[cycle], dst_ref=gbox.at[cycle, me], send_sem=g_send.at[cycle, n], recv_sem=g_recv.at[cycle, n],
                device_id=peer, device_id_type=MESH)
            copy.start()
            copies.append(copy)
        for n in range(1, len(peers)):
            dz, dy = divmod(n, 2)
            copies[n].wait_recv()
            sz, sy = zi + dz - 2 * dz * zi, yi + dy - 2 * dy * yi
            at = 4 * xi + 2 * sz + sy
            copy = pltpu.make_async_remote_copy(
                src_ref=gbox.at[cycle, at], dst_ref=gbox.at[cycle, at], send_sem=g_send.at[cycle, 3 + n],
                recv_sem=g_recv.at[cycle, 3 + n], device_id=peers[0], device_id_type=MESH)
            copy.start()
            copies.append(copy)
        copies[0].wait_recv()
        for copy in copies[:4]:
            copy.wait_send()
        for copy in copies[4:]:
            copy.wait()
        for c, a in enumerate((c2r, c2b)):
            gbox[cycle, me, c] = box[cycle, c]

        def unpack_box(i):
            for c, a in enumerate((h2r, h2b)):
                for q in range(4):
                    sz, sy = divmod(q, 2)
                    lo, hi = gbox[cycle, q, c, i], gbox[cycle, 4 + q, c, i]
                    for k in range(4):
                        lower = turn(lo, WIDTH - 32 * k) if k else lo
                        upper = turn(hi, (152 - 32 * k) % WIDTH)
                        v = jnp.where(box_lane < BOX, lower, jnp.where(box_lane < 48, upper, 0.0))
                        a[ZO[2] + 12 * sz + 4 * i + k, YO[2] + BOX * sy:YO[2] + BOX * sy + BOX, :] = v
        loop(3, unpack_box)

    l0 = lvs[0]
    count = len(chunks) // 2
    for n in range(count):
        ingest(n)
    pl.semaphore_wait(barrier, len(peers))
    x_u = Columns(us[0], l0, xs, xr0, 0)
    for n in range(count):
        ingest(count + n)
    x_u.finish()
    faces = send_faces(((u0r, 2, 4), (u0b, 3, 5)), l0, 0)
    x_f = Columns((f0r, f0b), l0, xs.at[2:4], xr0.at[2:4], 2)
    x_f.finish()
    faces += send_faces(((f0r, 2, 4),), l0, 6)
    send_faces(((f0b, 2, 3),), l0, 9)
    for ref in (u1r, u1b, u2r, u2b, h2r, h2b, u3r, u3b, h3r, h3b, u4r, u4b, h4r, h4b, u5r, u5b, h5r, h5b,
                d0, d1, d2, d3, d4, cx0, cx1, cx2, cx3, cx4, t0, t1, t2, t3, t4):
        clear_all((ref,))
    for copy in faces:
        copy.wait()

    deeper = ((f0r, 4, TILE, 2, 4), (f0b, 4, TILE, 2, 3))

    def v_cycle(cycle):
        h1 = (h1r.at[cycle], h1b.at[cycle])
        hs = ((f0r, f0b), h1, (h2r, h2b), (h3r, h3b), (h4r, h4b), (h5r, h5b))
        l1 = lvs[1]
        relax(us[0], (f0r, f0b), near, 0)

        @pl.when(cycle == 0)
        def black_source_arrived():
            for copy in send_faces(((f0b, 2, 3),), l0, 9, False):
                copy.wait()
        relax(us[0], (f0r, f0b), near, 1)
        relax(us[0], (f0r, f0b), near, 0)
        relax(us[0], (f0r, f0b), near, 1, ts[0])
        restrict(us[0], (f0r, f0b), near, ts[0], h1, (ZO[1], YO[1]))
        Columns(h1, l1, xs1, xr2.at[cycle], TILE).finish()
        faces = Faces(h1, l1, cycle)
        Columns(us[0], l0, xs, xr1.at[cycle], 4).finish()
        faces.finish()

        @pl.when(cycle == 0)
        def deeper_source():
            send_faces(deeper, l0, 0)
        for level in range(1, LAST):
            lv = lvs[level]
            zero_start(us[level], hs[level], lv)
            u, h = us[level], hs[level]
            relax(u, h, lv, 1)
            relax(u, h, lv, 0)
            relax(u, h, lv, 1, ts[level])
            if level == 1:
                restrict(u, h, lv, ts[level], (c2r, c2b), (0, 0))
                gather_level2(cycle)
                pending = send_faces(((u0r, 4, TILE), (u0b, 5, 9)), l0, 18)

            else:
                lower = level + 1
                restrict(u, h, lv, ts[level], hs[lower], (ZO[lower], YO[lower]))
        coarsest(hs[LAST], us[LAST], lvs[LAST], qu, qh)
        for level in range(4, -1, -1):
            lv = lvs[level]
            if level == 0:
                for copy in pending:
                    copy.wait()

                @pl.when(cycle == 0)
                def deeper_source_arrived():
                    for copy in send_faces(deeper, l0, 0, False):
                        copy.wait()
            prolong(us[level], us[level + 1], lv, lvs[level + 1], yi, xi, cxs[level], ds_[level])
            if level:
                loop(2, lambda i, lv=lv, level=level: sweep(us[level], hs[level], lv))

        @pl.when(cycle < CYCLES - 1)
        def wide_sweeps():
            loop(2, lambda i: sweep(us[0], (f0r, f0b), l0))

        @pl.when(cycle == CYCLES - 1)
        def last_sweeps():
            loop(2, lambda i: sweep(us[0], (f0r, f0b), near))
    loop(CYCLES, v_cycle)

    stores = []
    for n in range(BRICK // CHUNK):
        slot = n % SLOTS
        if n >= SLOTS:
            stores[n - SLOTS].wait()

        def unpack(i):
            z = l0.zo + n * half + i
            r, b = (colour[z, YO[0]:YO[0] + BRICK, :BRICK] for colour in us[0])
            raw[slot, 2 * i] = jnp.where(odd96, b, r)
            raw[slot, 2 * i + 1] = jnp.where(odd96, r, b)
        loop(half, unpack)
        copy = pltpu.make_async_copy(raw.at[slot], out_hbm.at[pl.ds(n * CHUNK, CHUNK)], out_sem.at[slot])
        copy.start()
        stores.append(copy)
    for copy in stores[-SLOTS:]:
        copy.wait()


def vmem(*shape):
    return pltpu.VMEM(shape, F32)


def scratch_shapes():
    arr = [vmem(NZ[level], NY[level], WIDTH) for level in range(6)]
    shapes = [arr[0]] * 4 + [arr[1]] * 2 + [vmem(2, NZ[1], NY[1], WIDTH)] * 2
    for level in range(2, 6):
        shapes += [arr[level]] * 4
    shapes += arr[:5]
    for extra in (BOX, 0):
        for level in range(LAST):
            rows = WINDOW[level] // 2 + extra if extra else -(-WINDOW[level] // XHALO) * XHALO
            shapes.append(vmem(PAIRS[level] + ZHALO[level], rows, WIDTH))
    shapes += [vmem(height, WIDTH) for height in (*WINDOW, WINDOW[0] - TILE)]
    shapes += [vmem(SLOTS, CHUNK, BRICK, BRICK)]
    shapes += [vmem(4, 6, BRICK, WIDTH), vmem(4, 6, BRICK, WIDTH), vmem(2, 2, 6, BRICK, WIDTH)]
    shapes += [vmem(2, 3, 48, WIDTH), vmem(2, 2, 3, 48, WIDTH)]
    for planes, rows in ((BOX, DEEP), (DEEP // 2, ROWS[1]), (DEEP // 2, DEEP)):
        shapes += [vmem(planes, rows, WIDTH), vmem(2, planes, rows, WIDTH)]
    last = LANES[LAST]
    shapes += [vmem(2, PAIRS[LAST] + 2, last + 2, 3 * TILE, WIDTH), vmem(2, PAIRS[LAST], last, TILE, WIDTH)]
    shapes += [vmem(12, BOX, WIDTH), vmem(12, BOX, WIDTH), vmem(2, 2, 3, BOX, WIDTH), vmem(2, TILE, 2, 3, BOX, WIDTH)]
    dma = pltpu.SemaphoreType.DMA
    for shape in ((SLOTS,), (10,), (BOX,), (2, 7)):
        shapes += [dma(shape), dma(shape)]
    return shapes


def solution(mesh):
    spec = P(('batch', 'z'), 'y', 'x')

    def local_solve(source, initial_guess):
        return pl.pallas_call(
            kernel,
            out_shape=jax.ShapeDtypeStruct(source.shape, F32),
            in_specs=[pl.BlockSpec(memory_space=pl.ANY)] * 2,
            out_specs=pl.BlockSpec(memory_space=pl.ANY),
            scratch_shapes=scratch_shapes(),
            compiler_params=pltpu.CompilerParams(collective_id=0, has_side_effects=True, vmem_limit_bytes=67043328),
            name='multigrid',
        )(source, initial_guess)

    return jax.shard_map(local_solve, mesh=mesh, in_specs=(spec, spec), out_specs=spec, check_vma=False)
```

```python
import jax
import jax.numpy as jnp
from jax import lax
from jax.experimental import pallas as pl
from jax.experimental.pallas import tpu as pltpu
from jax.sharding import PartitionSpec as P

N = 192
CYCLES = 2
COARSE_SWEEPS = 24
F32 = jnp.float32
MESH = pl.DeviceIdType.MESH

ROWS = LANES = (96, 48, 48, 24, 12, 6)
PAIRS = tuple(rows // 2 for rows in ROWS)
ZO = (9, 7, 1, 1, 1, 1)
NZ = tuple(pairs + 2 * first for pairs, first in zip(PAIRS, ZO))
YO = (24, 24, 8, 8, 8, 8)
NY = tuple(-(-rows // 8) * 8 + 2 * first for rows, first in zip(ROWS, YO))
ZHALO = (8, 6, 0, 0, 0, 0)
YHALO = (16, 16, 0, 0, 0, 0)
WINDOW = tuple(-(-(rows + halo) // 8) * 8 for rows, halo in zip(ROWS, YHALO))
UNROLL = (14, 15, 24, 12, 6, 3)
CHUNK = 16
SLOTS = 4
WIDTH = 128
TILE = 8
BRICK = 96
BOX = 24
XHALO = 16
DEEP = 12
LAST = 5
HALF = 64


def iotas(shape=(TILE, WIDTH)):
    return lax.broadcasted_iota(jnp.int32, shape, 0), lax.broadcasted_iota(jnp.int32, shape, 1)


class Level:
    def __init__(self, level, zi, yi, xi, m, zhalo, yhalo, unroll):
        self.level = level
        self.unroll = unroll
        self.split = level < 2
        self.pairs, self.rows, self.lanes = PAIRS[level], ROWS[level], LANES[level]
        self.zo, self.yo = ZO[level], YO[level]
        self.planes = self.pairs + zhalo
        self.height = TILE * (-(-(self.rows + yhalo) // TILE))
        self.own_height = TILE * (-(-self.rows // TILE))
        if self.split:
            self.zs = self.zo - zhalo * zi
            self.ys = pl.multiple_of(self.yo - yhalo * yi, TILE)
            self.own_at = pl.multiple_of(yhalo * yi, TILE)
        else:
            self.zs, self.ys, self.own_at = self.zo, self.yo, 0
        self.zi = zi
        self.side = zi.astype(F32)
        self.z_at = self.zo - self.zs
        self.m = m
        self.row = pl.ds(self.ys, self.height)
        lane = lax.broadcasted_iota(jnp.int32, (TILE, WIDTH), 1)
        if self.split:
            self.valid = jnp.logical_or(lane < self.lanes + XHALO * (1 - xi), lane >= WIDTH - XHALO * xi)
            edges = (lane == (self.lanes - 1) * xi,)
        else:
            self.valid = lane < self.lanes
            edges = (lane == 0, lane == self.lanes - 1)
        self.outer = edges[0] if self.split else jnp.logical_or(*edges)
        self.w = jnp.where(self.valid, 1.0 / 6.0, 0.0).astype(F32)[None]
        sub, lane = iotas((self.height, WIDTH))
        if self.split:
            count = ones(lane == (self.lanes - 1) * xi) + ones(sub == (self.height - 1) * yi)
        else:
            count = (ones(lane == 0) + ones(lane == self.lanes - 1)
                     + ones(sub == 0) + ones(sub == self.rows - 1))
        m[...] = count.astype(F32)

    def ghosts(self):
        low, high = (self.zo - 1, self.zo), (self.zo + self.pairs, self.zo + self.pairs - 1)
        if self.split:
            return [tuple(a + (b - a) * self.zi for a, b in zip(low, high))]
        return [low, high]

    def odd(self, height, flip):
        sub, lane = iotas()
        return jnp.broadcast_to((lax.rem(sub + lane, 2) == (0 if flip else 1))[None], (height // TILE, TILE, WIDTH))

    def scaled(self, s):
        if self.rows % TILE and not self.split:
            sub, lane = iotas((self.height, WIDTH))
            inside = jnp.logical_and(sub < self.rows, lane < self.lanes)
            return s * jnp.where(inside, 1.0 / 6.0, 0.0).astype(F32)
        return flat(tiled(s) * self.w)


def turn(v, by):
    return pltpu.roll(v, by, 1)


def pick(v, idx):
    return jnp.take_along_axis(v, idx, axis=1)


def ones(where):
    return jnp.where(where, 1.0, 0.0)


def tiled(v):
    return v.reshape(v.shape[0] // TILE, TILE, WIDTH)


def flat(v):
    return v.reshape(v.shape[0] * TILE, WIDTH)


def choose(mask, a, b):
    return flat(jnp.where(mask, tiled(a), tiled(b)))


def loop(count, body):
    def step(i, carry):
        body(i)
        return carry
    lax.fori_loop(0, count, step, 0)


def unrolled(count, body):
    def step(i, carry):
        body(i)
        return carry
    if count == 1:
        body(0)
    elif count > 1:
        lax.fori_loop(0, count, step, 0, unroll=True)


def grouped(count, group, body):
    if count == group:
        unrolled(group, body)
    else:
        loop(count // group, lambda i: unrolled(group, lambda k: body(i * group + k)))


def ghost_planes(dst, src, lv):
    for to, frm in lv.ghosts():
        dst[to, lv.row, :] = -src[frm, lv.row, :]


def gather_sum(a, b, hb, z, y, height, mask, m):
    row = pl.ds(y, height)
    bc = b[z, row, :]
    s = bc + choose(mask, b[z + 1, row, :], b[z - 1, row, :])
    s = s + (b[z, pl.ds(y - 1, height), :] + b[z, pl.ds(y + 1, height), :])
    s = s + (turn(bc, 1) + turn(bc, WIDTH - 1))
    av = a[z, row, :]
    return s + (hb[z, row, :] - m * av), av


def half_sweep(a, b, hb, lv, colour, sums=None):
    ghost_planes(b, a, lv)
    mask = lv.odd(lv.height, colour)

    def plane(k):
        z = lv.zs + k
        m = lv.m[...]
        s, old = gather_sum(a, b, hb, z, lv.ys, lv.height, mask, m)
        new = lv.scaled(s)
        if sums is not None:
            new = new + lv.scaled(s - 6.0 * new)
        a[z, lv.row, :] = new
        if sums is not None:
            sums[k, 0:lv.height, :] = m * (old - new)
    grouped(lv.planes, lv.unroll, plane)
    if sums is not None:
        for n, (to, frm) in enumerate(lv.ghosts()):
            delta = -(a[frm, lv.row, :] + b[to, lv.row, :])
            up = lv.side if lv.split else float(n)
            k = frm - lv.zs
            sums[k, 0:lv.height, :] = sums[k, 0:lv.height, :] + choose(mask, delta * up, delta * (1.0 - up))


def relax(u, hb, lv, colour, sums=None):
    half_sweep(u[colour], u[1 - colour], hb[colour], lv, colour, sums)


def sweep(u, hb, lv):
    relax(u, hb, lv, 0)
    relax(u, hb, lv, 1)


def zero_start(u, hb, lv):
    def plane(k):
        u[0][lv.zs + k, lv.row, :] = lv.scaled(hb[0][lv.zs + k, lv.row, :])
    grouped(lv.planes, lv.unroll, plane)


def restrict(u, hb, lv, sums, coarse, coarse_at):
    height = lv.own_height
    own = pl.ds(lv.own_at, height)
    ghost_planes(u[1], u[0], lv)
    mask = lv.odd(height, 0)

    def plane(k):
        s, v = gather_sum(u[0], u[1], hb[0], lv.zo + k, lv.yo, height, mask, lv.m[own, :])
        sums[lv.z_at + k, own, :] = sums[lv.z_at + k, own, :] + (s - 6.0 * v)
    grouped(lv.pairs, min(12, lv.pairs), plane)

    half = lv.lanes // 2
    rows = TILE * (-(-(lv.rows // 2) // TILE))
    sub, lane = iotas((rows, WIDTH))
    even_idx = jnp.minimum(2 * lane, 126)
    odd_idx = even_idx + 1
    scale = jnp.where(iotas()[1] < half, 0.5, 0.0).astype(F32)[None]
    mask = lv.odd(rows, 0)
    zc, yc = coarse_at

    def fold(pair):
        c = []
        for s in range(2):
            z = lv.z_at + 2 * pair + s
            v = sums[z, pl.ds(lv.own_at, rows, stride=2), :] + sums[z, pl.ds(lv.own_at + 1, rows, stride=2), :]
            v = pick(v, even_idx) + pick(v, odd_idx)
            c.append(flat(tiled(v) * scale))
        coarse[0][zc + pair, pl.ds(yc, rows), :] = choose(mask, c[1], c[0])
        coarse[1][zc + pair, pl.ds(yc, rows), :] = choose(mask, c[0], c[1])
    grouped(lv.pairs // 2, min(6, lv.pairs // 2), fold)


def prolong(u, e, lv, lc, yi, xi, cx, d):
    planes = lv.planes
    crows = (lv.rows + YHALO[lv.level]) // 2
    height = TILE * (-(-crows // TILE))
    if lv.level == 0:
        zc, yc, off = lc.zo - (ZHALO[0] // 2) * lv.zi, lc.yo - (YHALO[0] // 2) * yi, 0
    elif lv.level == 1:
        zc = lc.zo + (PAIRS[2] - planes // 2) * lv.zi
        yc = lc.yo + (ROWS[2] - crows) * yi
        off = (LANES[1] // 2) * xi
    else:
        zc, yc, off = lc.zo, lc.yo, 0
    if lv.split:
        yc = pl.multiple_of(yc, TILE)
    sub, lane = iotas((height, WIDTH))
    fine_lane = jnp.where(lane < 112, lane, lane - WIDTH) if lv.split else lane
    near = lax.div(fine_lane + WIDTH, 2) - 64
    far = near + jnp.where(lax.rem(lane, 2) == 1, 1, -1)
    if lv.split:
        far = jnp.where(lane == (lv.lanes - 1) * xi, near, far)
    else:
        far = jnp.where(jnp.logical_or(lane == 0, lane == lv.lanes - 1), near, far)
    idx_near = lax.rem(near + off + WIDTH, WIDTH)
    idx_far = lax.rem(far + off + WIDTH, WIDTH)
    w_near = jnp.where(lv.valid, 0.75, 0.0).astype(F32)[None]
    w_far = jnp.where(lv.valid, jnp.where(lv.outer, -0.25, 0.25), 0.0).astype(F32)[None]
    mask = lv.odd(height, 0)

    def along_x(pair):
        r, b = e[0][zc + pair, pl.ds(yc, height), :], e[1][zc + pair, pl.ds(yc, height), :]
        for s in range(2):
            c = choose(mask, b, r) if s == 0 else choose(mask, r, b)
            c = (tiled(pick(c, idx_near)) * w_near
                 + tiled(pick(c, idx_far)) * w_far)
            cx[2 * pair + s, TILE:TILE + height, :] = flat(c)
    pairs = planes // 2
    grouped(pairs, 7 if pairs % 7 == 0 else (5 if pairs % 5 == 0 else min(6, pairs)), along_x)

    if lv.split:
        sides = ((7 + (crows + 1) * yi, TILE + (crows - 1) * yi),)
    else:
        sides = ((7, TILE), (TILE + crows, 7 + crows))

    def edge_rows(z):
        for to, frm in sides:
            cx[z, pl.ds(to, 1), :] = -cx[z, pl.ds(frm, 1), :]
    grouped(planes, 2, edge_rows)

    def along_y(z):
        mid = 0.75 * cx[z, TILE:TILE + height, :]
        d[lv.zs + z, pl.ds(lv.ys, height, stride=2), :] = mid + 0.25 * cx[z, 7:7 + height, :]
        d[lv.zs + z, pl.ds(lv.ys + 1, height, stride=2), :] = mid + 0.25 * cx[z, 9:9 + height, :]
    grouped(planes, 2, along_y)
    ghost_planes(d, d, lv)
    mask = lv.odd(lv.height, 0)

    def along_z(k):
        z = lv.zs + k
        mid = 0.75 * d[z, lv.row, :]
        up, down = 0.25 * d[z + 1, lv.row, :], 0.25 * d[z - 1, lv.row, :]
        r = u[0][z, lv.row, :] + (mid + choose(mask, up, down))
        b = u[1][z, lv.row, :] + (mid + choose(mask, down, up))
        if not lv.split and lv.rows % TILE:
            keep = iotas((lv.height, WIDTH))[0] < lv.rows
            r, b = jnp.where(keep, r, 0.0), jnp.where(keep, b, 0.0)
        u[0][z, lv.row, :] = r
        u[1][z, lv.row, :] = b
    grouped(planes, 2, along_z)


def coarsest(h, u, lv, qu, qh):
    edge = lv.lanes
    box = (edge, TILE, WIDTH)
    x, y, lane = (lax.broadcasted_iota(jnp.int32, box, d) for d in range(3))
    rows = pl.ds(TILE, TILE)
    for c in range(2):
        for k in range(lv.pairs):
            v = h[c][lv.zo + k, rows, :]
            for i in range(edge):
                qh[c, k, i] = pick(v, jnp.full((TILE, WIDTH), i, jnp.int32))
    clear_all((qu,))
    inner = ones(y < edge).astype(F32) / 6.0
    faces = (ones(x == 0) + ones(x == edge - 1) + ones(y == 0) + ones(y == edge - 1)).astype(F32)
    own = pl.ds(1, edge)

    def sweeps(_):
        for c in range(2):
            up = lax.rem(x + y + c, 2) == 1
            up_f = ones(up).astype(F32)
            for k in range(lv.pairs):
                m = faces
                if k == 0:
                    m = m + (1.0 - up_f)
                if k == lv.pairs - 1:
                    m = m + up_f
                z = k + 1
                b, a = qu.at[1 - c], qu.at[c]
                s = b[z, own, rows, :] + jnp.where(up, b[z + 1, own, rows, :], b[z - 1, own, rows, :])
                s = s + (b[z, own, pl.ds(TILE - 1, TILE), :] + b[z, own, pl.ds(TILE + 1, TILE), :])
                s = s + (b[z, pl.ds(0, edge), rows, :] + b[z, pl.ds(2, edge), rows, :])
                a[z, own, rows, :] = (s + (qh[c, k] - m * a[z, own, rows, :])) * inner
    loop(COARSE_SWEEPS, sweeps)
    for c in range(2):
        for k in range(lv.pairs):
            v = qu[c, k + 1, own, rows, :]
            total = jnp.where(lane[0] == 0, v[0], 0.0)
            for i in range(1, edge):
                total = jnp.where(lane[0] == i, v[i], total)
            u[c][lv.zo + k, rows, :] = total


def clear_all(refs):
    for ref in refs:
        def clear(i, ref=ref):
            ref[i] = jnp.zeros(ref.shape[1:], F32)
        loop(ref.shape[0], clear)


def kernel(f_hbm, u_hbm, *rest):
    outs, scratch = rest[:2], rest[2:]
    (u0r, u0b, f0r, f0b, u1r, u1b, h1r, h1b, u2r, u2b, h2r, h2b, u3r, u3b, h3r, h3b, u4r, u4b, h4r, h4b,
     u5r, u5b, h5r, h5b, d0, d1, d2, d3, d4, cx0, cx1, cx2, cx3, cx4, t0, t1, t2, t3, t4,
     m0, m1, m2, m3, m4, m5, m6, raw, xs, xr0, xr1, xs1, xr2, ys, yr, zs, zr, es, er, qu, qh, c2r, c2b, box, gbox,
     in_sem, out_sem, x_send, x_recv, send, recv, g_send, g_recv) = scratch
    zi, yi, xi = lax.axis_index('z'), lax.axis_index('y'), lax.axis_index('x')
    nx, ny, nz = 1 - xi, 1 - yi, 1 - zi
    peers = ({'x': nx}, {'y': ny}, {'z': nz}, {'z': nz, 'y': ny})

    chunks = [(src, c) for src in (u_hbm, f_hbm) for c in range(BRICK // CHUNK)]

    def load(n):
        src, c = chunks[n]
        return pltpu.make_async_copy(src.at[pl.ds(c * CHUNK, CHUNK)], raw.at[n % SLOTS], in_sem.at[n % SLOTS])
    for n in range(SLOTS):
        load(n).start()

    for ref in (u0r, u0b, f0r, f0b):
        clear_all((ref,))
    for ref in (h1r.at[0], h1b.at[0], h1r.at[1], h1b.at[1]):
        clear_all((ref,))

    barrier = pltpu.get_barrier_semaphore()
    for peer in peers:
        pl.semaphore_signal(barrier, inc=1, device_id=peer, device_id_type=MESH)

    sub, lane = iotas((BRICK, BRICK))
    odd96 = lax.rem(sub + lane, 2) == 1
    h_sq = (1.0 / N) ** 2
    half = CHUNK // 2

    def ingest(n):
        load(n).wait()
        slot = n % SLOTS
        first = n < len(chunks) // 2
        red, black = (u0r, u0b) if first else (f0r, f0b)
        start = ZO[0] + (n % (BRICK // CHUNK)) * half

        def pack(i):
            p0, p1 = raw[slot, 2 * i], raw[slot, 2 * i + 1]
            r, b = jnp.where(odd96, p1, p0), jnp.where(odd96, p0, p1)
            if not first:
                r, b = r * h_sq, b * h_sq
            red[start + i, YO[0]:YO[0] + BRICK, :BRICK] = r
            black[start + i, YO[0]:YO[0] + BRICK, :BRICK] = b
        loop(half, pack)
        if n + SLOTS < len(chunks):
            load(n + SLOTS).start()

    lvs = [Level(level, zi, yi, xi, m, ZHALO[level], YHALO[level], UNROLL[level])
           for level, m in enumerate((m0, m1, m2, m3, m4, m5))]
    near = Level(0, zi, yi, xi, m6, 4, TILE, 13)
    us = ((u0r, u0b), (u1r, u1b), (u2r, u2b), (u3r, u3b), (u4r, u4b), (u5r, u5b))
    ds_ = (d0, d1, d2, d3, d4)
    cxs = (cx0, cx1, cx2, cx3, cx4)
    ts = (t0, t1, t2, t3, t4)

    box_lane = lax.broadcasted_iota(jnp.int32, (BOX, WIDTH), 1)
    quarter = lax.div(box_lane, 32)

    class Columns:
        def __init__(self, arrays, lv, s_buf, r_buf, sem_at):
            self.arrays, self.lv, self.r_buf = arrays, lv, r_buf
            self.wide = lax.broadcasted_iota(jnp.int32, (lv.rows, WIDTH), 1)
            self.row = pl.ds(lv.yo, lv.rows)
            group = lax.div(self.wide, XHALO)
            from_lane = (lv.lanes - XHALO) * nx
            self.copies = []
            for n, a in enumerate(arrays):
                def pack_x(i, a=a, n=n):
                    acc = None
                    for k in range(TILE):
                        v = turn(a[lv.zo + TILE * i + k, self.row, :], lax.rem(XHALO * k + WIDTH - from_lane, WIDTH))
                        acc = v if k == 0 else jnp.where(group == k, v, acc)
                    s_buf[n, i] = acc
                loop(lv.pairs // TILE, pack_x)
                at = sem_at + n
                copy = pltpu.make_async_remote_copy(
                    src_ref=s_buf.at[n], dst_ref=r_buf.at[n], send_sem=x_send.at[at], recv_sem=x_recv.at[at],
                    device_id=peers[0], device_id_type=MESH)
                copy.start()
                self.copies.append(copy)

        def finish(self):
            lv, row = self.lv, self.row
            to_lane = lv.lanes + (112 - lv.lanes) * xi
            inside = jnp.logical_and(self.wide >= to_lane, self.wide < to_lane + XHALO)
            for n, a in enumerate(self.arrays):
                self.copies[n].wait()

                def unpack_x(i, a=a, n=n):
                    acc = self.r_buf[n, i]
                    for k in range(TILE):
                        z = lv.zo + TILE * i + k
                        v = turn(acc, lax.rem(to_lane + WIDTH - XHALO * k, WIDTH))
                        a[z, row, :] = jnp.where(inside, v, a[z, row, :])
                loop(lv.pairs // TILE, unpack_x)

    def send_faces(specs, lv, sem_at, start=True):
        copies = []
        def layers(first, count, size, skip, high):
            inside = first + skip + (count - size - 2 * skip) * (1 - high)
            outside = first - skip - size + (count + size + 2 * skip) * high
            return pl.ds(inside, size), pl.ds(outside, size)

        for a, zn, yn, *there in specs:
            z_skip, y_skip = there or (0, 0)
            z_own, y_own = pl.ds(lv.zo, lv.pairs), pl.ds(lv.yo, lv.rows)
            y_in, y_to = layers(lv.yo, lv.rows, yn - y_skip, y_skip, yi)
            z_in, z_to = layers(lv.zo, lv.pairs, zn - z_skip, z_skip, zi)
            y_all, z_all = layers(lv.yo, lv.rows, yn, 0, yi), layers(lv.zo, lv.pairs, zn, 0, zi)
            parts = (
                ((z_own, y_in), (z_own, y_to), peers[1]),
                ((z_in, y_own), (z_to, y_own), peers[2]),
                ((z_all[0], y_all[0]), (z_all[1], y_all[1]), peers[3]),
            )
            for src, dst, peer in parts:
                at = sem_at + len(copies)
                copy = pltpu.make_async_remote_copy(
                    src_ref=a.at[src[0], src[1]], dst_ref=a.at[dst[0], dst[1]], send_sem=send.at[at], recv_sem=recv.at[at],
                    device_id=peer, device_id_type=MESH)
                if start:
                    copy.start()
                copies.append(copy)
        return copies

    class Faces:
        def __init__(self, h, lv, cycle):
            self.h, self.cycle = h, cycle
            thick = DEEP // 2
            y_in, z_in = lv.yo + (lv.rows - DEEP) * ny, lv.zo + (lv.pairs - thick) * nz
            y_to, z_to = lv.yo + lv.rows - (lv.rows + DEEP) * yi, lv.zo + lv.pairs - (lv.pairs + thick) * zi
            self.parts = ((ys, yr, lv.zo, lv.pairs, y_in, DEEP, lv.zo, y_to),
                          (zs, zr, z_in, thick, lv.yo, lv.rows, z_to, lv.yo),
                          (es, er, z_in, thick, y_in, DEEP, z_to, y_to))
            self.copies = []
            for n, (out, into, z, planes, y, rows, _, _) in enumerate(self.parts):
                lane = lax.broadcasted_iota(jnp.int32, (rows, WIDTH), 1)

                def pack(i):
                    r, b = (colour[z + i, pl.ds(y, rows), :] for colour in h)
                    out[i] = jnp.where(lane < HALF, turn(r, XHALO * xi), turn(b, XHALO * xi + HALF))
                grouped(planes, 6, pack)
                at = 12 + n
                copy = pltpu.make_async_remote_copy(
                    src_ref=out, dst_ref=into.at[cycle], send_sem=send.at[at], recv_sem=recv.at[at],
                    device_id=peers[n + 1], device_id_type=MESH)
                copy.start()
                self.copies.append(copy)

        def finish(self):
            for copy, (_, into, _, planes, _, rows, z, y) in zip(self.copies, self.parts):
                copy.wait()
                lane = lax.broadcasted_iota(jnp.int32, (rows, WIDTH), 1)
                valid = jnp.logical_or(lane < HALF - XHALO * xi, lane >= WIDTH - XHALO * xi)

                def unpack(i):
                    v = into[self.cycle, i]
                    for c in range(2):
                        w = turn(v, lax.rem(WIDTH - HALF * c - XHALO * xi, WIDTH))
                        self.h[c][z + i, pl.ds(y, rows), :] = jnp.where(valid, w, 0.0)
                grouped(planes, 6, unpack)

    def gather_level2(cycle):
        def pack_box(i):
            for c, a in enumerate((c2r, c2b)):
                acc = a[4 * i]
                for k in range(1, 4):
                    acc = jnp.where(quarter == k, turn(a[4 * i + k], 32 * k), acc)
                box[cycle, c, i] = acc
        loop(3, pack_box)
        me = 4 * xi + 2 * zi + yi
        copies = []
        for n, peer in enumerate(peers):
            copy = pltpu.make_async_remote_copy(
                src_ref=box.at[cycle], dst_ref=gbox.at[cycle, me], send_sem=g_send.at[cycle, n], recv_sem=g_recv.at[cycle, n],
                device_id=peer, device_id_type=MESH)
            copy.start()
            copies.append(copy)
        clear_all((u2b, u3b, u4b))
        for n in range(1, len(peers)):
            dz, dy = divmod(n, 2)
            copies[n].wait_recv()
            sz, sy = zi + dz - 2 * dz * zi, yi + dy - 2 * dy * yi
            at = 4 * xi + 2 * sz + sy
            copy = pltpu.make_async_remote_copy(
                src_ref=gbox.at[cycle, at], dst_ref=gbox.at[cycle, at], send_sem=g_send.at[cycle, 3 + n],
                recv_sem=g_recv.at[cycle, 3 + n], device_id=peers[0], device_id_type=MESH)
            copy.start()
            copies.append(copy)
        copies[0].wait_recv()
        for copy in copies[:4]:
            copy.wait_send()
        for copy in copies[4:]:
            copy.wait()
        for c, a in enumerate((c2r, c2b)):
            gbox[cycle, me, c] = box[cycle, c]

        def unpack_box(i):
            for c, a in enumerate((h2r, h2b)):
                for q in range(4):
                    sz, sy = divmod(q, 2)
                    lo, hi = gbox[cycle, q, c, i], gbox[cycle, 4 + q, c, i]
                    for k in range(4):
                        lower = turn(lo, WIDTH - 32 * k) if k else lo
                        upper = turn(hi, (152 - 32 * k) % WIDTH)
                        v = jnp.where(box_lane < BOX, lower, jnp.where(box_lane < 48, upper, 0.0))
                        a[ZO[2] + 12 * sz + 4 * i + k, YO[2] + BOX * sy:YO[2] + BOX * sy + BOX, :] = v
        loop(3, unpack_box)

    l0 = lvs[0]
    count = len(chunks) // 2
    for n in range(count):
        ingest(n)
    pl.semaphore_wait(barrier, len(peers))
    x_u = Columns(us[0], l0, xs, xr0, 0)
    for n in range(count):
        ingest(count + n)
    x_u.finish()
    faces = send_faces(((u0r, 2, 4), (u0b, 3, 5)), l0, 0)
    x_f = Columns((f0r, f0b), l0, xs.at[2:4], xr0.at[2:4], 2)
    x_f.finish()
    faces += send_faces(((f0r, 2, 4),), l0, 6)
    send_faces(((f0b, 2, 3),), l0, 9)
    for ref in (u1r, u1b, u2r, u2b, h2r, h2b, u3r, u3b, h3r, h3b, u4r, u4b, h4r, h4b, u5r, u5b, h5r, h5b,
                d0, d1, d2, d3, d4, cx0, cx1, cx2, cx3, cx4, t0, t1, t2, t3, t4):
        clear_all((ref,))
    for copy in faces:
        copy.wait()

    deeper = ((f0r, 4, TILE, 2, 4), (f0b, 4, TILE, 2, 3))

    def v_cycle(cycle):
        h1 = (h1r.at[cycle], h1b.at[cycle])
        hs = ((f0r, f0b), h1, (h2r, h2b), (h3r, h3b), (h4r, h4b), (h5r, h5b))
        l1 = lvs[1]
        relax(us[0], (f0r, f0b), near, 0)

        @pl.when(cycle == 0)
        def black_source_arrived():
            for copy in send_faces(((f0b, 2, 3),), l0, 9, False):
                copy.wait()
        relax(us[0], (f0r, f0b), near, 1)
        relax(us[0], (f0r, f0b), near, 0)
        relax(us[0], (f0r, f0b), near, 1, ts[0])
        restrict(us[0], (f0r, f0b), near, ts[0], h1, (ZO[1], YO[1]))
        Columns(h1, l1, xs1, xr2.at[cycle], TILE).finish()
        faces = Faces(h1, l1, cycle)
        Columns(us[0], l0, xs, xr1.at[cycle], 4).finish()
        clear_all((u1b,))
        faces.finish()

        @pl.when(cycle == 0)
        def deeper_source():
            send_faces(deeper, l0, 0)
        for level in range(1, LAST):
            lv = lvs[level]
            zero_start(us[level], hs[level], lv)
            u, h = us[level], hs[level]
            relax(u, h, lv, 1)
            relax(u, h, lv, 0)
            relax(u, h, lv, 1, ts[level])
            if level == 1:
                restrict(u, h, lv, ts[level], (c2r, c2b), (0, 0))
                gather_level2(cycle)
                pending = send_faces(((u0r, 4, TILE), (u0b, 5, 9)), l0, 18)

            else:
                lower = level + 1
                restrict(u, h, lv, ts[level], hs[lower], (ZO[lower], YO[lower]))
        coarsest(hs[LAST], us[LAST], lvs[LAST], qu, qh)
        for level in range(4, -1, -1):
            lv = lvs[level]
            if level == 0:
                for copy in pending:
                    copy.wait()

                @pl.when(cycle == 0)
                def deeper_source_arrived():
                    for copy in send_faces(deeper, l0, 0, False):
                        copy.wait()
            prolong(us[level], us[level + 1], lv, lvs[level + 1], yi, xi, cxs[level], ds_[level])
            if level:
                loop(2, lambda i, lv=lv, level=level: sweep(us[level], hs[level], lv))

        @pl.when(cycle < CYCLES - 1)
        def wide_sweeps():
            loop(2, lambda i: sweep(us[0], (f0r, f0b), l0))

        @pl.when(cycle == CYCLES - 1)
        def last_sweeps():
            loop(2, lambda i: sweep(us[0], (f0r, f0b), near))
    loop(CYCLES, v_cycle)

    stores = []
    for n, colour in enumerate(us[0]):
        copy = pltpu.make_async_copy(colour.at[pl.ds(l0.zo, l0.pairs), pl.ds(l0.yo, l0.rows)], outs[n], out_sem.at[n])
        copy.start()
        stores.append(copy)
    for copy in stores:
        copy.wait()


def vmem(*shape):
    return pltpu.VMEM(shape, F32)


def scratch_shapes():
    arr = [vmem(NZ[level], NY[level], WIDTH) for level in range(6)]
    shapes = [arr[0]] * 4 + [arr[1]] * 2 + [vmem(2, NZ[1], NY[1], WIDTH)] * 2
    for level in range(2, 6):
        shapes += [arr[level]] * 4
    shapes += arr[:5]
    for extra in (BOX, 0):
        for level in range(LAST):
            rows = WINDOW[level] // 2 + extra if extra else -(-WINDOW[level] // XHALO) * XHALO
            shapes.append(vmem(PAIRS[level] + ZHALO[level], rows, WIDTH))
    shapes += [vmem(height, WIDTH) for height in (*WINDOW, WINDOW[0] - TILE)]
    shapes += [vmem(SLOTS, CHUNK, BRICK, BRICK)]
    shapes += [vmem(4, 6, BRICK, WIDTH), vmem(4, 6, BRICK, WIDTH), vmem(2, 2, 6, BRICK, WIDTH)]
    shapes += [vmem(2, 3, 48, WIDTH), vmem(2, 2, 3, 48, WIDTH)]
    for planes, rows in ((BOX, DEEP), (DEEP // 2, ROWS[1]), (DEEP // 2, DEEP)):
        shapes += [vmem(planes, rows, WIDTH), vmem(2, planes, rows, WIDTH)]
    last = LANES[LAST]
    shapes += [vmem(2, PAIRS[LAST] + 2, last + 2, 3 * TILE, WIDTH), vmem(2, PAIRS[LAST], last, TILE, WIDTH)]
    shapes += [vmem(12, BOX, WIDTH), vmem(12, BOX, WIDTH), vmem(2, 2, 3, BOX, WIDTH), vmem(2, TILE, 2, 3, BOX, WIDTH)]
    dma = pltpu.SemaphoreType.DMA
    for shape in ((SLOTS,), (10,), (BOX,), (2, 7)):
        shapes += [dma(shape), dma(shape)]
    return shapes


def solution(mesh):
    spec = P(('batch', 'z'), 'y', 'x')

    def local_solve(source, initial_guess):
        pairs, rows, lanes = source.shape[0] // 2, source.shape[1], source.shape[2]
        red, black = pl.pallas_call(
            kernel,
            out_shape=[jax.ShapeDtypeStruct((pairs, rows, WIDTH), F32)] * 2,
            in_specs=[pl.BlockSpec(memory_space=pl.ANY)] * 2,
            out_specs=[pl.BlockSpec(memory_space=pl.ANY)] * 2,
            scratch_shapes=scratch_shapes(),
            compiler_params=pltpu.CompilerParams(collective_id=0, has_side_effects=True, vmem_limit_bytes=67043328),
            name='multigrid',
        )(source, initial_guess)
        red, black = red[:, None, :, :lanes], black[:, None, :, :lanes]
        z, y, x = (lax.broadcasted_iota(jnp.int32, (1, 2, rows, lanes), d) for d in range(1, 4))
        return jnp.where(lax.rem(z + y + x, 2) == 0, red, black).reshape(source.shape)

    return jax.shard_map(local_solve, mesh=mesh, in_specs=(spec, spec), out_specs=spec, check_vma=False)
```

```python
import jax
import jax.numpy as jnp
from jax import lax
from jax.experimental import pallas as pl
from jax.experimental.pallas import tpu as pltpu
from jax.sharding import PartitionSpec as P

N = 192
CYCLES = 2
COARSE_SWEEPS = 24
F32 = jnp.float32
MESH = pl.DeviceIdType.MESH

ROWS = LANES = (96, 48, 48, 24, 12, 6)
PAIRS = tuple(rows // 2 for rows in ROWS)
ZO = (9, 7, 1, 1, 1, 1)
NZ = tuple(pairs + 2 * first for pairs, first in zip(PAIRS, ZO))
YO = (24, 24, 8, 8, 8, 8)
NY = tuple(-(-rows // 8) * 8 + 2 * first for rows, first in zip(ROWS, YO))
ZHALO = (8, 6, 0, 0, 0, 0)
YHALO = (16, 16, 0, 0, 0, 0)
WINDOW = tuple(-(-(rows + halo) // 8) * 8 for rows, halo in zip(ROWS, YHALO))
UNROLL = (14, 15, 24, 12, 6, 3)
CHUNK = 16
SLOTS = 4
WIDTH = 128
TILE = 8
BRICK = 96
BOX = 24
XHALO = 16
DEEP = 12
LAST = 5
HALF = 64


def iotas(shape=(TILE, WIDTH)):
    return lax.broadcasted_iota(jnp.int32, shape, 0), lax.broadcasted_iota(jnp.int32, shape, 1)


class Level:
    def __init__(self, level, zi, yi, xi, m, zhalo, yhalo, unroll):
        self.level = level
        self.unroll = unroll
        self.split = level < 2
        self.pairs, self.rows, self.lanes = PAIRS[level], ROWS[level], LANES[level]
        self.zo, self.yo = ZO[level], YO[level]
        self.planes = self.pairs + zhalo
        self.height = TILE * (-(-(self.rows + yhalo) // TILE))
        self.own_height = TILE * (-(-self.rows // TILE))
        if self.split:
            self.zs = self.zo - zhalo * zi
            self.ys = pl.multiple_of(self.yo - yhalo * yi, TILE)
            self.own_at = pl.multiple_of(yhalo * yi, TILE)
        else:
            self.zs, self.ys, self.own_at = self.zo, self.yo, 0
        self.zi = zi
        self.side = zi.astype(F32)
        self.z_at = self.zo - self.zs
        self.m = m
        self.row = pl.ds(self.ys, self.height)
        lane = lax.broadcasted_iota(jnp.int32, (TILE, WIDTH), 1)
        if self.split:
            self.valid = jnp.logical_or(lane < self.lanes + XHALO * (1 - xi), lane >= WIDTH - XHALO * xi)
            edges = (lane == (self.lanes - 1) * xi,)
        else:
            self.valid = lane < self.lanes
            edges = (lane == 0, lane == self.lanes - 1)
        self.outer = edges[0] if self.split else jnp.logical_or(*edges)
        self.w = jnp.where(self.valid, 1.0 / 6.0, 0.0).astype(F32)[None]
        sub, lane = iotas((self.height, WIDTH))
        if self.split:
            count = ones(lane == (self.lanes - 1) * xi) + ones(sub == (self.height - 1) * yi)
        else:
            count = (ones(lane == 0) + ones(lane == self.lanes - 1)
                     + ones(sub == 0) + ones(sub == self.rows - 1))
        m[...] = count.astype(F32)

    def ghosts(self):
        low, high = (self.zo - 1, self.zo), (self.zo + self.pairs, self.zo + self.pairs - 1)
        if self.split:
            return [tuple(a + (b - a) * self.zi for a, b in zip(low, high))]
        return [low, high]

    def odd(self, height, flip):
        sub, lane = iotas()
        return jnp.broadcast_to((lax.rem(sub + lane, 2) == (0 if flip else 1))[None], (height // TILE, TILE, WIDTH))

    def scaled(self, s):
        if self.rows % TILE and not self.split:
            sub, lane = iotas((self.height, WIDTH))
            inside = jnp.logical_and(sub < self.rows, lane < self.lanes)
            return s * jnp.where(inside, 1.0 / 6.0, 0.0).astype(F32)
        return flat(tiled(s) * self.w)


def turn(v, by):
    return pltpu.roll(v, by, 1)


def pick(v, idx):
    return jnp.take_along_axis(v, idx, axis=1)


def ones(where):
    return jnp.where(where, 1.0, 0.0)


def tiled(v):
    return v.reshape(v.shape[0] // TILE, TILE, WIDTH)


def flat(v):
    return v.reshape(v.shape[0] * TILE, WIDTH)


def choose(mask, a, b):
    return flat(jnp.where(mask, tiled(a), tiled(b)))


def loop(count, body):
    def step(i, carry):
        body(i)
        return carry
    lax.fori_loop(0, count, step, 0)


def unrolled(count, body):
    def step(i, carry):
        body(i)
        return carry
    if count == 1:
        body(0)
    elif count > 1:
        lax.fori_loop(0, count, step, 0, unroll=True)


def grouped(count, group, body):
    if count == group:
        unrolled(group, body)
    else:
        loop(count // group, lambda i: unrolled(group, lambda k: body(i * group + k)))


def ghost_planes(dst, src, lv):
    for to, frm in lv.ghosts():
        dst[to, lv.row, :] = -src[frm, lv.row, :]


def gather_sum(a, b, hb, z, y, height, mask, m):
    row = pl.ds(y, height)
    bc = b[z, row, :]
    s = bc + choose(mask, b[z + 1, row, :], b[z - 1, row, :])
    s = s + (b[z, pl.ds(y - 1, height), :] + b[z, pl.ds(y + 1, height), :])
    s = s + (turn(bc, 1) + turn(bc, WIDTH - 1))
    av = a[z, row, :]
    return s + (hb[z, row, :] - m * av), av


def half_sweep(a, b, hb, lv, colour, sums=None):
    ghost_planes(b, a, lv)
    mask = lv.odd(lv.height, colour)

    def plane(k):
        z = lv.zs + k
        m = lv.m[...]
        s, old = gather_sum(a, b, hb, z, lv.ys, lv.height, mask, m)
        new = lv.scaled(s)
        if sums is not None:
            new = new + lv.scaled(s - 6.0 * new)
        a[z, lv.row, :] = new
        if sums is not None:
            sums[k, 0:lv.height, :] = m * (old - new)
    grouped(lv.planes, lv.unroll, plane)
    if sums is not None:
        for n, (to, frm) in enumerate(lv.ghosts()):
            delta = -(a[frm, lv.row, :] + b[to, lv.row, :])
            up = lv.side if lv.split else float(n)
            k = frm - lv.zs
            sums[k, 0:lv.height, :] = sums[k, 0:lv.height, :] + choose(mask, delta * up, delta * (1.0 - up))


def relax(u, hb, lv, colour, sums=None):
    half_sweep(u[colour], u[1 - colour], hb[colour], lv, colour, sums)


def sweep(u, hb, lv):
    relax(u, hb, lv, 0)
    relax(u, hb, lv, 1)


def zero_start(u, hb, lv):
    def plane(k):
        u[0][lv.zs + k, lv.row, :] = lv.scaled(hb[0][lv.zs + k, lv.row, :])
    grouped(lv.planes, lv.unroll, plane)


def restrict(u, hb, lv, sums, coarse, coarse_at):
    height = lv.own_height
    own = pl.ds(lv.own_at, height)
    ghost_planes(u[1], u[0], lv)
    mask = lv.odd(height, 0)

    def plane(k):
        s, v = gather_sum(u[0], u[1], hb[0], lv.zo + k, lv.yo, height, mask, lv.m[own, :])
        sums[lv.z_at + k, own, :] = sums[lv.z_at + k, own, :] + (s - 6.0 * v)
    grouped(lv.pairs, min(12, lv.pairs), plane)

    half = lv.lanes // 2
    rows = TILE * (-(-(lv.rows // 2) // TILE))
    sub, lane = iotas((rows, WIDTH))
    even_idx = jnp.minimum(2 * lane, 126)
    odd_idx = even_idx + 1
    scale = jnp.where(iotas()[1] < half, 0.5, 0.0).astype(F32)[None]
    mask = lv.odd(rows, 0)
    zc, yc = coarse_at

    def fold(pair):
        c = []
        for s in range(2):
            z = lv.z_at + 2 * pair + s
            v = sums[z, pl.ds(lv.own_at, rows, stride=2), :] + sums[z, pl.ds(lv.own_at + 1, rows, stride=2), :]
            v = pick(v, even_idx) + pick(v, odd_idx)
            c.append(flat(tiled(v) * scale))
        coarse[0][zc + pair, pl.ds(yc, rows), :] = choose(mask, c[1], c[0])
        coarse[1][zc + pair, pl.ds(yc, rows), :] = choose(mask, c[0], c[1])
    grouped(lv.pairs // 2, min(6, lv.pairs // 2), fold)


def prolong(u, e, lv, lc, yi, xi, cx, d):
    planes = lv.planes
    crows = (lv.rows + YHALO[lv.level]) // 2
    height = TILE * (-(-crows // TILE))
    if lv.level == 0:
        zc, yc, off = lc.zo - (ZHALO[0] // 2) * lv.zi, lc.yo - (YHALO[0] // 2) * yi, 0
    elif lv.level == 1:
        zc = lc.zo + (PAIRS[2] - planes // 2) * lv.zi
        yc = lc.yo + (ROWS[2] - crows) * yi
        off = (LANES[1] // 2) * xi
    else:
        zc, yc, off = lc.zo, lc.yo, 0
    if lv.split:
        yc = pl.multiple_of(yc, TILE)
    sub, lane = iotas((height, WIDTH))
    fine_lane = jnp.where(lane < 112, lane, lane - WIDTH) if lv.split else lane
    near = lax.div(fine_lane + WIDTH, 2) - 64
    far = near + jnp.where(lax.rem(lane, 2) == 1, 1, -1)
    if lv.split:
        far = jnp.where(lane == (lv.lanes - 1) * xi, near, far)
    else:
        far = jnp.where(jnp.logical_or(lane == 0, lane == lv.lanes - 1), near, far)
    idx_near = lax.rem(near + off + WIDTH, WIDTH)
    idx_far = lax.rem(far + off + WIDTH, WIDTH)
    w_near = jnp.where(lv.valid, 0.75, 0.0).astype(F32)[None]
    w_far = jnp.where(lv.valid, jnp.where(lv.outer, -0.25, 0.25), 0.0).astype(F32)[None]
    mask = lv.odd(height, 0)

    def along_x(pair):
        r, b = e[0][zc + pair, pl.ds(yc, height), :], e[1][zc + pair, pl.ds(yc, height), :]
        for s in range(2):
            c = choose(mask, b, r) if s == 0 else choose(mask, r, b)
            c = (tiled(pick(c, idx_near)) * w_near
                 + tiled(pick(c, idx_far)) * w_far)
            cx[2 * pair + s, TILE:TILE + height, :] = flat(c)
    pairs = planes // 2
    grouped(pairs, 7 if pairs % 7 == 0 else (5 if pairs % 5 == 0 else min(6, pairs)), along_x)

    if lv.split:
        sides = ((7 + (crows + 1) * yi, TILE + (crows - 1) * yi),)
    else:
        sides = ((7, TILE), (TILE + crows, 7 + crows))

    def edge_rows(z):
        for to, frm in sides:
            cx[z, pl.ds(to, 1), :] = -cx[z, pl.ds(frm, 1), :]
    grouped(planes, 2, edge_rows)

    def along_y(z):
        mid = 0.75 * cx[z, TILE:TILE + height, :]
        d[lv.zs + z, pl.ds(lv.ys, height, stride=2), :] = mid + 0.25 * cx[z, 7:7 + height, :]
        d[lv.zs + z, pl.ds(lv.ys + 1, height, stride=2), :] = mid + 0.25 * cx[z, 9:9 + height, :]
    grouped(planes, 2, along_y)
    ghost_planes(d, d, lv)
    mask = lv.odd(lv.height, 0)

    def along_z(k):
        z = lv.zs + k
        mid = 0.75 * d[z, lv.row, :]
        up, down = 0.25 * d[z + 1, lv.row, :], 0.25 * d[z - 1, lv.row, :]
        r = u[0][z, lv.row, :] + (mid + choose(mask, up, down))
        b = u[1][z, lv.row, :] + (mid + choose(mask, down, up))
        if not lv.split and lv.rows % TILE:
            keep = iotas((lv.height, WIDTH))[0] < lv.rows
            r, b = jnp.where(keep, r, 0.0), jnp.where(keep, b, 0.0)
        u[0][z, lv.row, :] = r
        u[1][z, lv.row, :] = b
    grouped(planes, 2, along_z)


def coarsest(h, u, lv, qu, qh):
    edge = lv.lanes
    box = (edge, TILE, WIDTH)
    x, y, lane = (lax.broadcasted_iota(jnp.int32, box, d) for d in range(3))
    rows = pl.ds(TILE, TILE)
    for c in range(2):
        for k in range(lv.pairs):
            v = h[c][lv.zo + k, rows, :]
            for i in range(edge):
                qh[c, k, i] = pick(v, jnp.full((TILE, WIDTH), i, jnp.int32))
    clear_all((qu,))
    inner = ones(y < edge).astype(F32) / 6.0
    faces = (ones(x == 0) + ones(x == edge - 1) + ones(y == 0) + ones(y == edge - 1)).astype(F32)
    own = pl.ds(1, edge)

    def sweeps(_):
        for c in range(2):
            up = lax.rem(x + y + c, 2) == 1
            up_f = ones(up).astype(F32)
            for k in range(lv.pairs):
                m = faces
                if k == 0:
                    m = m + (1.0 - up_f)
                if k == lv.pairs - 1:
                    m = m + up_f
                z = k + 1
                b, a = qu.at[1 - c], qu.at[c]
                s = b[z, own, rows, :] + jnp.where(up, b[z + 1, own, rows, :], b[z - 1, own, rows, :])
                s = s + (b[z, own, pl.ds(TILE - 1, TILE), :] + b[z, own, pl.ds(TILE + 1, TILE), :])
                s = s + (b[z, pl.ds(0, edge), rows, :] + b[z, pl.ds(2, edge), rows, :])
                a[z, own, rows, :] = (s + (qh[c, k] - m * a[z, own, rows, :])) * inner
    loop(COARSE_SWEEPS, sweeps)
    for c in range(2):
        for k in range(lv.pairs):
            v = qu[c, k + 1, own, rows, :]
            total = jnp.where(lane[0] == 0, v[0], 0.0)
            for i in range(1, edge):
                total = jnp.where(lane[0] == i, v[i], total)
            u[c][lv.zo + k, rows, :] = total


def clear_all(refs):
    for ref in refs:
        def clear(i, ref=ref):
            ref[i] = jnp.zeros(ref.shape[1:], F32)
        loop(ref.shape[0], clear)


def kernel(f_hbm, u_hbm, out_hbm, *scratch):
    (u0r, u0b, f0r, f0b, u1r, u1b, h1r, h1b, u2r, u2b, h2r, h2b, u3r, u3b, h3r, h3b, u4r, u4b, h4r, h4b,
     u5r, u5b, h5r, h5b, d0, d1, d2, d3, d4, cx0, cx1, cx2, cx3, cx4, t0, t1, t2, t3, t4,
     m0, m1, m2, m3, m4, m5, m6, raw, xs, xr0, xr1, xs1, xr2, ys, yr, zs, zr, es, er, qu, qh, c2r, c2b, box, gbox,
     in_sem, out_sem, x_send, x_recv, send, recv, g_send, g_recv) = scratch
    zi, yi, xi = lax.axis_index('z'), lax.axis_index('y'), lax.axis_index('x')
    nx, ny, nz = 1 - xi, 1 - yi, 1 - zi
    peers = ({'x': nx}, {'y': ny}, {'z': nz}, {'z': nz, 'y': ny})

    chunks = [(src, c) for src in (u_hbm, f_hbm) for c in range(BRICK // CHUNK)]

    def load(n):
        src, c = chunks[n]
        return pltpu.make_async_copy(src.at[pl.ds(c * CHUNK, CHUNK)], raw.at[n % SLOTS], in_sem.at[n % SLOTS])
    for n in range(SLOTS):
        load(n).start()

    for ref in (u0r, u0b, f0r, f0b):
        clear_all((ref,))
    for ref in (h1r.at[0], h1b.at[0], h1r.at[1], h1b.at[1]):
        clear_all((ref,))

    barrier = pltpu.get_barrier_semaphore()
    for peer in peers:
        pl.semaphore_signal(barrier, inc=1, device_id=peer, device_id_type=MESH)

    sub, lane = iotas((BRICK, BRICK))
    odd96 = lax.rem(sub + lane, 2) == 1
    h_sq = (1.0 / N) ** 2
    half = CHUNK // 2

    def ingest(n):
        load(n).wait()
        slot = n % SLOTS
        first = n < len(chunks) // 2
        red, black = (u0r, u0b) if first else (f0r, f0b)
        start = ZO[0] + (n % (BRICK // CHUNK)) * half

        def pack(i):
            p0, p1 = raw[slot, 2 * i], raw[slot, 2 * i + 1]
            r, b = jnp.where(odd96, p1, p0), jnp.where(odd96, p0, p1)
            if not first:
                r, b = r * h_sq, b * h_sq
            red[start + i, YO[0]:YO[0] + BRICK, :BRICK] = r
            black[start + i, YO[0]:YO[0] + BRICK, :BRICK] = b
        loop(half, pack)
        if n + SLOTS < len(chunks):
            load(n + SLOTS).start()

    lvs = [Level(level, zi, yi, xi, m, ZHALO[level], YHALO[level], UNROLL[level])
           for level, m in enumerate((m0, m1, m2, m3, m4, m5))]
    near = Level(0, zi, yi, xi, m6, 4, TILE, 13)
    us = ((u0r, u0b), (u1r, u1b), (u2r, u2b), (u3r, u3b), (u4r, u4b), (u5r, u5b))
    ds_ = (d0, d1, d2, d3, d4)
    cxs = (cx0, cx1, cx2, cx3, cx4)
    ts = (t0, t1, t2, t3, t4)

    box_lane = lax.broadcasted_iota(jnp.int32, (BOX, WIDTH), 1)
    quarter = lax.div(box_lane, 32)

    class Columns:
        def __init__(self, arrays, lv, s_buf, r_buf, sem_at):
            self.arrays, self.lv, self.r_buf = arrays, lv, r_buf
            self.wide = lax.broadcasted_iota(jnp.int32, (lv.rows, WIDTH), 1)
            self.row = pl.ds(lv.yo, lv.rows)
            group = lax.div(self.wide, XHALO)
            from_lane = (lv.lanes - XHALO) * nx
            self.copies = []
            for n, a in enumerate(arrays):
                def pack_x(i, a=a, n=n):
                    acc = None
                    for k in range(TILE):
                        v = turn(a[lv.zo + TILE * i + k, self.row, :], lax.rem(XHALO * k + WIDTH - from_lane, WIDTH))
                        acc = v if k == 0 else jnp.where(group == k, v, acc)
                    s_buf[n, i] = acc
                loop(lv.pairs // TILE, pack_x)
                at = sem_at + n
                copy = pltpu.make_async_remote_copy(
                    src_ref=s_buf.at[n], dst_ref=r_buf.at[n], send_sem=x_send.at[at], recv_sem=x_recv.at[at],
                    device_id=peers[0], device_id_type=MESH)
                copy.start()
                self.copies.append(copy)

        def finish(self):
            lv, row = self.lv, self.row
            to_lane = lv.lanes + (112 - lv.lanes) * xi
            inside = jnp.logical_and(self.wide >= to_lane, self.wide < to_lane + XHALO)
            for n, a in enumerate(self.arrays):
                self.copies[n].wait()

                def unpack_x(i, a=a, n=n):
                    acc = self.r_buf[n, i]
                    for k in range(TILE):
                        z = lv.zo + TILE * i + k
                        v = turn(acc, lax.rem(to_lane + WIDTH - XHALO * k, WIDTH))
                        a[z, row, :] = jnp.where(inside, v, a[z, row, :])
                loop(lv.pairs // TILE, unpack_x)

    def send_faces(specs, lv, sem_at, start=True):
        copies = []
        def layers(first, count, size, skip, high):
            inside = first + skip + (count - size - 2 * skip) * (1 - high)
            outside = first - skip - size + (count + size + 2 * skip) * high
            return pl.ds(inside, size), pl.ds(outside, size)

        for a, zn, yn, *there in specs:
            z_skip, y_skip = there or (0, 0)
            z_own, y_own = pl.ds(lv.zo, lv.pairs), pl.ds(lv.yo, lv.rows)
            y_in, y_to = layers(lv.yo, lv.rows, yn - y_skip, y_skip, yi)
            z_in, z_to = layers(lv.zo, lv.pairs, zn - z_skip, z_skip, zi)
            y_all, z_all = layers(lv.yo, lv.rows, yn, 0, yi), layers(lv.zo, lv.pairs, zn, 0, zi)
            parts = (
                ((z_own, y_in), (z_own, y_to), peers[1]),
                ((z_in, y_own), (z_to, y_own), peers[2]),
                ((z_all[0], y_all[0]), (z_all[1], y_all[1]), peers[3]),
            )
            for src, dst, peer in parts:
                at = sem_at + len(copies)
                copy = pltpu.make_async_remote_copy(
                    src_ref=a.at[src[0], src[1]], dst_ref=a.at[dst[0], dst[1]], send_sem=send.at[at], recv_sem=recv.at[at],
                    device_id=peer, device_id_type=MESH)
                if start:
                    copy.start()
                copies.append(copy)
        return copies

    class Faces:
        def __init__(self, h, lv, cycle):
            self.h, self.cycle = h, cycle
            thick = DEEP // 2
            y_in, z_in = lv.yo + (lv.rows - DEEP) * ny, lv.zo + (lv.pairs - thick) * nz
            y_to, z_to = lv.yo + lv.rows - (lv.rows + DEEP) * yi, lv.zo + lv.pairs - (lv.pairs + thick) * zi
            self.parts = ((ys, yr, lv.zo, lv.pairs, y_in, DEEP, lv.zo, y_to),
                          (zs, zr, z_in, thick, lv.yo, lv.rows, z_to, lv.yo),
                          (es, er, z_in, thick, y_in, DEEP, z_to, y_to))
            self.copies = []
            for n, (out, into, z, planes, y, rows, _, _) in enumerate(self.parts):
                lane = lax.broadcasted_iota(jnp.int32, (rows, WIDTH), 1)

                def pack(i):
                    r, b = (colour[z + i, pl.ds(y, rows), :] for colour in h)
                    out[i] = jnp.where(lane < HALF, turn(r, XHALO * xi), turn(b, XHALO * xi + HALF))
                grouped(planes, 6, pack)
                at = 12 + n
                copy = pltpu.make_async_remote_copy(
                    src_ref=out, dst_ref=into.at[cycle], send_sem=send.at[at], recv_sem=recv.at[at],
                    device_id=peers[n + 1], device_id_type=MESH)
                copy.start()
                self.copies.append(copy)

        def finish(self):
            for copy, (_, into, _, planes, _, rows, z, y) in zip(self.copies, self.parts):
                copy.wait()
                lane = lax.broadcasted_iota(jnp.int32, (rows, WIDTH), 1)
                valid = jnp.logical_or(lane < HALF - XHALO * xi, lane >= WIDTH - XHALO * xi)

                def unpack(i):
                    v = into[self.cycle, i]
                    for c in range(2):
                        w = turn(v, lax.rem(WIDTH - HALF * c - XHALO * xi, WIDTH))
                        self.h[c][z + i, pl.ds(y, rows), :] = jnp.where(valid, w, 0.0)
                grouped(planes, 6, unpack)

    def gather_level2(cycle):
        def pack_box(i):
            for c, a in enumerate((c2r, c2b)):
                acc = a[4 * i]
                for k in range(1, 4):
                    acc = jnp.where(quarter == k, turn(a[4 * i + k], 32 * k), acc)
                box[cycle, c, i] = acc
        loop(3, pack_box)
        me = 4 * xi + 2 * zi + yi
        copies = []
        for n, peer in enumerate(peers):
            copy = pltpu.make_async_remote_copy(
                src_ref=box.at[cycle], dst_ref=gbox.at[cycle, me], send_sem=g_send.at[cycle, n], recv_sem=g_recv.at[cycle, n],
                device_id=peer, device_id_type=MESH)
            copy.start()
            copies.append(copy)
        clear_all((u2b, u3b, u4b))
        for n in range(1, len(peers)):
            dz, dy = divmod(n, 2)
            copies[n].wait_recv()
            sz, sy = zi + dz - 2 * dz * zi, yi + dy - 2 * dy * yi
            at = 4 * xi + 2 * sz + sy
            copy = pltpu.make_async_remote_copy(
                src_ref=gbox.at[cycle, at], dst_ref=gbox.at[cycle, at], send_sem=g_send.at[cycle, 3 + n],
                recv_sem=g_recv.at[cycle, 3 + n], device_id=peers[0], device_id_type=MESH)
            copy.start()
            copies.append(copy)
        copies[0].wait_recv()
        for copy in copies[:4]:
            copy.wait_send()
        for copy in copies[4:]:
            copy.wait()
        for c, a in enumerate((c2r, c2b)):
            gbox[cycle, me, c] = box[cycle, c]

        def unpack_box(i):
            for c, a in enumerate((h2r, h2b)):
                for q in range(4):
                    sz, sy = divmod(q, 2)
                    lo, hi = gbox[cycle, q, c, i], gbox[cycle, 4 + q, c, i]
                    for k in range(4):
                        lower = turn(lo, WIDTH - 32 * k) if k else lo
                        upper = turn(hi, (152 - 32 * k) % WIDTH)
                        v = jnp.where(box_lane < BOX, lower, jnp.where(box_lane < 48, upper, 0.0))
                        a[ZO[2] + 12 * sz + 4 * i + k, YO[2] + BOX * sy:YO[2] + BOX * sy + BOX, :] = v
        loop(3, unpack_box)

    l0 = lvs[0]
    count = len(chunks) // 2
    for n in range(count):
        ingest(n)
    pl.semaphore_wait(barrier, len(peers))
    x_u = Columns(us[0], l0, xs, xr0, 0)
    for n in range(count):
        ingest(count + n)
    x_u.finish()
    faces = send_faces(((u0r, 2, 4), (u0b, 3, 5)), l0, 0)
    x_f = Columns((f0r, f0b), l0, xs.at[2:4], xr0.at[2:4], 2)
    x_f.finish()
    faces += send_faces(((f0r, 2, 4),), l0, 6)
    send_faces(((f0b, 2, 3),), l0, 9)
    for ref in (u1r, u1b, u2r, u2b, h2r, h2b, u3r, u3b, h3r, h3b, u4r, u4b, h4r, h4b, u5r, u5b, h5r, h5b,
                d0, d1, d2, d3, d4, cx0, cx1, cx2, cx3, cx4, t0, t1, t2, t3, t4):
        clear_all((ref,))
    for copy in faces:
        copy.wait()

    deeper = ((f0r, 4, TILE, 2, 4), (f0b, 4, TILE, 2, 3))

    def v_cycle(cycle):
        h1 = (h1r.at[cycle], h1b.at[cycle])
        hs = ((f0r, f0b), h1, (h2r, h2b), (h3r, h3b), (h4r, h4b), (h5r, h5b))
        l1 = lvs[1]
        relax(us[0], (f0r, f0b), near, 0)

        @pl.when(cycle == 0)
        def black_source_arrived():
            for copy in send_faces(((f0b, 2, 3),), l0, 9, False):
                copy.wait()
        relax(us[0], (f0r, f0b), near, 1)
        relax(us[0], (f0r, f0b), near, 0)
        relax(us[0], (f0r, f0b), near, 1, ts[0])
        restrict(us[0], (f0r, f0b), near, ts[0], h1, (ZO[1], YO[1]))
        Columns(h1, l1, xs1, xr2.at[cycle], TILE).finish()
        faces = Faces(h1, l1, cycle)
        Columns(us[0], l0, xs, xr1.at[cycle], 4).finish()
        clear_all((u1b,))
        faces.finish()

        @pl.when(cycle == 0)
        def deeper_source():
            send_faces(deeper, l0, 0)
        for level in range(1, LAST):
            lv = lvs[level]
            zero_start(us[level], hs[level], lv)
            u, h = us[level], hs[level]
            relax(u, h, lv, 1)
            relax(u, h, lv, 0)
            relax(u, h, lv, 1, ts[level])
            if level == 1:
                restrict(u, h, lv, ts[level], (c2r, c2b), (0, 0))
                gather_level2(cycle)
                pending = send_faces(((u0r, 4, TILE), (u0b, 5, 9)), l0, 18)

            else:
                lower = level + 1
                restrict(u, h, lv, ts[level], hs[lower], (ZO[lower], YO[lower]))
        coarsest(hs[LAST], us[LAST], lvs[LAST], qu, qh)
        for level in range(4, -1, -1):
            lv = lvs[level]
            if level == 0:
                for copy in pending:
                    copy.wait()

                @pl.when(cycle == 0)
                def deeper_source_arrived():
                    for copy in send_faces(deeper, l0, 0, False):
                        copy.wait()
            prolong(us[level], us[level + 1], lv, lvs[level + 1], yi, xi, cxs[level], ds_[level])
            if level:
                loop(2, lambda i, lv=lv, level=level: sweep(us[level], hs[level], lv))

        @pl.when(cycle < CYCLES - 1)
        def wide_sweeps():
            loop(2, lambda i: sweep(us[0], (f0r, f0b), l0))

        @pl.when(cycle == CYCLES - 1)
        def last_sweeps():
            loop(2, lambda i: sweep(us[0], (f0r, f0b), near))
    loop(CYCLES, v_cycle)

    stores = []
    for n in range(BRICK // CHUNK):
        slot = n % SLOTS
        if n >= SLOTS:
            stores[n - SLOTS].wait()

        def unpack(i):
            z = l0.zo + n * half + i
            r, b = (colour[z, YO[0]:YO[0] + BRICK, :BRICK] for colour in us[0])
            raw[slot, 2 * i] = jnp.where(odd96, b, r)
            raw[slot, 2 * i + 1] = jnp.where(odd96, r, b)
        loop(half, unpack)
        copy = pltpu.make_async_copy(raw.at[slot], out_hbm.at[pl.ds(n * CHUNK, CHUNK)], out_sem.at[slot])
        copy.start()
        stores.append(copy)
    for copy in stores[-SLOTS:]:
        copy.wait()


def vmem(*shape):
    return pltpu.VMEM(shape, F32)


def scratch_shapes():
    arr = [vmem(NZ[level], NY[level], WIDTH) for level in range(6)]
    shapes = [arr[0]] * 4 + [arr[1]] * 2 + [vmem(2, NZ[1], NY[1], WIDTH)] * 2
    for level in range(2, 6):
        shapes += [arr[level]] * 4
    shapes += arr[:5]
    for extra in (BOX, 0):
        for level in range(LAST):
            rows = WINDOW[level] // 2 + extra if extra else -(-WINDOW[level] // XHALO) * XHALO
            shapes.append(vmem(PAIRS[level] + ZHALO[level], rows, WIDTH))
    shapes += [vmem(height, WIDTH) for height in (*WINDOW, WINDOW[0] - TILE)]
    shapes += [vmem(SLOTS, CHUNK, BRICK, BRICK)]
    shapes += [vmem(4, 6, BRICK, WIDTH), vmem(4, 6, BRICK, WIDTH), vmem(2, 2, 6, BRICK, WIDTH)]
    shapes += [vmem(2, 3, 48, WIDTH), vmem(2, 2, 3, 48, WIDTH)]
    for planes, rows in ((BOX, DEEP), (DEEP // 2, ROWS[1]), (DEEP // 2, DEEP)):
        shapes += [vmem(planes, rows, WIDTH), vmem(2, planes, rows, WIDTH)]
    last = LANES[LAST]
    shapes += [vmem(2, PAIRS[LAST] + 2, last + 2, 3 * TILE, WIDTH), vmem(2, PAIRS[LAST], last, TILE, WIDTH)]
    shapes += [vmem(12, BOX, WIDTH), vmem(12, BOX, WIDTH), vmem(2, 2, 3, BOX, WIDTH), vmem(2, TILE, 2, 3, BOX, WIDTH)]
    dma = pltpu.SemaphoreType.DMA
    for shape in ((SLOTS,), (10,), (BOX,), (2, 7)):
        shapes += [dma(shape), dma(shape)]
    return shapes


def solution(mesh):
    spec = P(('batch', 'z'), 'y', 'x')

    def local_solve(source, initial_guess):
        return pl.pallas_call(
            kernel,
            out_shape=jax.ShapeDtypeStruct(source.shape, F32),
            in_specs=[pl.BlockSpec(memory_space=pl.ANY)] * 2,
            out_specs=pl.BlockSpec(memory_space=pl.ANY),
            scratch_shapes=scratch_shapes(),
            compiler_params=pltpu.CompilerParams(collective_id=0, has_side_effects=True, vmem_limit_bytes=67043328),
            name='multigrid',
        )(source, initial_guess)

    return jax.shard_map(local_solve, mesh=mesh, in_specs=(spec, spec), out_specs=spec, check_vma=False)
```
